128 devices in a mesh: gz: 2 (over z_lo), gy: 4 (over z_hi, core), gx: 16 (over x, y).
Axes of the slice: x: 4, y: 4, z: 4 (z_hi: 2, z_lo: 2; z = z_hi * 2 + z_lo), core: 2. Of those that a mesh axis runs over, the one named last changes fastest.
Arguments:
- charges: float32 [262144], P(('gz', 'gy', 'gx')), may hold values from -2.5 to 2.5
- fractions: float32 [3, 262144], P(None, ('gz', 'gy', 'gx')), may hold values from 0 to 1
- base_cells: int32 [3, 262144], P(None, ('gz', 'gy', 'gx')), may hold values from 0 to 255, as said below
- counts: int32 [2, 4, 16], P('gz', 'gy', 'gx'), may hold values from 1024 to 2048, as said below
Outputs:
- forces: float32 [3, 262144], P(None, ('gz', 'gy', 'gx'))
The draws below stay inside these ranges and needn't reach their ends.
Inputs may be any that keep to these rules, and one draw needn't show every extreme that they name: `base_cells`: atom slots of the block at gz, gy, gx have base cells inside that block's cells: x in gx*16 to gx*16 + 15, y in gy*64 to gy*64 + 63, z in gz*128 to gz*128 + 127. The first counts[b] slots of block b hold atoms, the rest are empty; some block is full in every draw.
All inputs are finite; a program needn't handle non-finite values.
Results may differ from the reference program's by a relative error of at most 0.0003.
Values sent between devices are 32-bit elements; how exact they have to be, the bound alone decides.
A program may use at most 128 MiB of HBM per device.

```python
import jax
import jax.numpy as jnp

GRID = 256
ORDER = 4
CAP = 2048
CX = 16
CY = 64
CZ = 128
ATOMS = 262144


def draw_base_cells(key, part):
    blocks_x = GRID // CX
    blocks_y = GRID // CY
    blocks_z = GRID // CZ
    slot_index = jnp.arange(CAP * blocks_x * blocks_y * blocks_z, dtype=jnp.int32)
    block = slot_index // CAP
    block_x = block % blocks_x
    block_y = block // blocks_x % blocks_y
    block_z = block // (blocks_x * blocks_y)
    base_key = jax.random.fold_in(key, 11)
    key_x = jax.random.fold_in(base_key, 1)
    key_y = jax.random.fold_in(base_key, 2)
    key_z = jax.random.fold_in(base_key, 3)
    cell_x = block_x * CX + jax.random.randint(key_x, slot_index.shape, 0, CX, dtype=jnp.int32)
    cell_y = block_y * CY + jax.random.randint(key_y, slot_index.shape, 0, CY, dtype=jnp.int32)
    cell_z = block_z * CZ + jax.random.randint(key_z, slot_index.shape, 0, CZ, dtype=jnp.int32)
    return jnp.stack([cell_x, cell_y, cell_z]).astype(jnp.int32)


def draw_counts(key, part):
    blocks_x = GRID // CX
    blocks_y = GRID // CY
    blocks_z = GRID // CZ
    total = blocks_x * blocks_y * blocks_z
    base_key = jax.random.fold_in(key, 23)
    values = jax.random.randint(jax.random.fold_in(base_key, 1), (total,), CAP // 2, CAP + 1, dtype=jnp.int32)
    chosen = jax.random.randint(jax.random.fold_in(base_key, 2), (), 0, total, dtype=jnp.int32)
    values = jnp.where(jnp.arange(total, dtype=jnp.int32) == chosen, CAP, values)
    return values.reshape(blocks_z, blocks_y, blocks_x).astype(jnp.int32)


def block_levels(rng, dims, pieces, smallest, high):
    loudness, own = 1.0, jax.random.fold_in(rng, 6)
    for dim, blocks in pieces:
        heights = jnp.exp(jax.random.uniform(jax.random.fold_in(own, dim), (blocks,), jnp.float32, smallest / len(pieces), high / len(pieces)))
        loudness = loudness * jnp.repeat(heights, dims[dim] // blocks).reshape([-1 if axis == dim else 1 for axis in range(len(dims))])
    return loudness


def gaussian(key, shape, deviation, bound, split=(), held_as=jnp.bfloat16):
    loudness = block_levels(key, shape, split, -0.22, 0.18) if split else 1.0
    values = jax.random.normal(key, shape, jnp.float32) * deviation * loudness
    return jnp.minimum(jnp.maximum(values, -bound), bound).astype(held_as)


def setup_inputs(seed: int = 0) -> dict:
    splits = jax.random.split(jax.random.key(seed), 5)
    return {
        "charges": gaussian(splits[0], (ATOMS,), 0.4, 2.5, ((0, 128),), jnp.float32),
        "fractions": jnp.clip(1.0 * jax.random.uniform(splits[1], (3, ATOMS), jnp.float32) ** block_levels(splits[1], (3, ATOMS), ((1, 128),), -0.2, 0.2), 0.0, 1.0),
        "base_cells": draw_base_cells(jax.random.fold_in(splits[4], 71), 0),
        "counts": draw_counts(jax.random.fold_in(splits[4], 71), 0),
    }


coulomb = 332.0636
ewald = 0.7


def spline_weights(frac):
    rest = 1.0 - frac
    square = frac * frac
    cube = square * frac
    weights = jnp.stack([rest * rest * rest / 6.0, (3.0 * cube - 6.0 * square + 4.0) / 6.0,
                         (-3.0 * cube + 3.0 * square + 3.0 * frac + 1.0) / 6.0, cube / 6.0])
    slopes = jnp.stack([-0.5 * rest * rest, 1.5 * square - 2.0 * frac,
                        -1.5 * square + frac + 0.5, 0.5 * square])
    return weights, slopes


def green_factors(index, length):
    signed = jnp.where(2 * index < length, index, index - length).astype(jnp.float32)
    bspline = 36.0 / (4.0 + 2.0 * jnp.cos(index.astype(jnp.float32) * (2.0 * jnp.pi / length))) ** 2
    bspline = jnp.where(2 * index == length, 0.0, bspline)
    return signed * signed, bspline


def reference(charges, fractions, base_cells, counts):
    slot_index = jnp.arange(charges.shape[0], dtype=jnp.int32)
    live = (slot_index % CAP) < counts.reshape(-1)[slot_index // CAP]
    charge = jnp.where(live, charges, jnp.zeros_like(charges))
    weights_x, slopes_x = spline_weights(fractions[0])
    weights_y, slopes_y = spline_weights(fractions[1])
    weights_z, slopes_z = spline_weights(fractions[2])
    charge_grid = jnp.zeros((GRID, GRID, GRID), jnp.float32)
    for first in range(ORDER):
        for second in range(ORDER):
            for third in range(ORDER):
                cell_x = (base_cells[0] + first) % GRID
                cell_y = (base_cells[1] + second) % GRID
                cell_z = (base_cells[2] + third) % GRID
                charge_grid = charge_grid.at[cell_x, cell_y, cell_z].add(
                    charge * weights_x[first] * weights_y[second] * weights_z[third])
    index = jnp.arange(GRID, dtype=jnp.int32)
    square_line, spline_line = green_factors(index, GRID)
    square = square_line[:, None, None] + square_line[None, :, None] + square_line[None, None, :]
    factor = spline_line[:, None, None] * spline_line[None, :, None] * spline_line[None, None, :]
    green = jnp.where(square > 0.0,
                      coulomb * jnp.exp(square * (-(jnp.pi ** 2) / (ewald * ewald * GRID * GRID))) * factor
                      / (jnp.pi * GRID * jnp.maximum(square, 1.0)), 0.0)
    spectrum = jnp.fft.fftn(charge_grid)
    potential = jnp.real(jnp.fft.ifftn(spectrum * green)) * (GRID ** 3)
    force_x = jnp.zeros_like(charge)
    force_y = jnp.zeros_like(charge)
    force_z = jnp.zeros_like(charge)
    for first in range(ORDER):
        for second in range(ORDER):
            for third in range(ORDER):
                cell_x = (base_cells[0] + first) % GRID
                cell_y = (base_cells[1] + second) % GRID
                cell_z = (base_cells[2] + third) % GRID
                value = potential[cell_x, cell_y, cell_z]
                force_x = force_x + slopes_x[first] * weights_y[second] * weights_z[third] * value
                force_y = force_y + weights_x[first] * slopes_y[second] * weights_z[third] * value
                force_z = force_z + weights_x[first] * weights_y[second] * slopes_z[third] * value
    return -charge[None, :] * jnp.stack([force_x, force_y, force_z])
```

```python
import functools

import jax
import jax.numpy as jnp
import numpy as np
from jax import lax
from jax.experimental import pallas as pl
from jax.experimental.pallas import tpu as pltpu
from jax.sharding import PartitionSpec as P

GRID = 256
ORDER = 4
HALO = ORDER - 1
COULOMB = 332.0636
EWALD = 0.7
CX, CY, CZ = 16, 64, 128
ROWS = 72
SPAN = CX + HALO
COLUMN = 8
INTERPRET = False
F32 = jnp.float32
BF16 = jnp.bfloat16
NN = (((1,), (0,)), ((), ()))
NT = (((1,), (1,)), ((), ()))


def split_np(a):
    a = np.asarray(a, np.float32)
    high = a.astype(jnp.bfloat16)
    low = (a - high.astype(np.float32)).astype(jnp.bfloat16)
    return np.stack([high, low])


def tables():
    k = np.arange(GRID)
    half = np.arange(GRID // 2)

    def turn(first, second, length):
        angle = (first[:, None] * second[None, :] % length) * (2.0 * np.pi / length)
        return np.cos(angle), np.sin(angle)

    cos, sin = turn(k, half, GRID)
    to_kz = np.concatenate([cos, -sin], axis=1)
    twice = np.where(half > 0, 2.0, 1.0)[:, None]
    from_kz = np.concatenate([twice * cos.T, -twice * sin.T], axis=0)
    cos, sin = turn(k, k, GRID)
    real = np.concatenate([cos, sin], axis=1).reshape(64, 4, 512)
    imag = np.concatenate([-sin, cos], axis=1).reshape(64, 4, 512)
    to_ky = np.stack([real, imag], axis=1).reshape(512, 512)
    cos, sin = turn(half, half, GRID // 2)
    to_kx = np.concatenate(
        [np.concatenate([cos, sin], axis=1), np.concatenate([-sin, cos], axis=1)], axis=0
    )
    angle = half[:, None] * (2.0 * np.pi / GRID) * np.ones((1, 128))
    upper = np.arange(128)[None, :] >= 64
    twist = np.stack([np.where(upper, np.cos(angle), 1.0), np.where(upper, np.sin(angle), 0.0)])
    signed = np.where(2 * k < GRID, k, k - GRID).astype(np.float64)
    spline = 36.0 / (4.0 + 2.0 * np.cos(k * (2.0 * np.pi / GRID))) ** 2
    spline[GRID // 2] = 0.0
    decay = spline * np.exp(-np.pi**2 * signed**2 / (EWALD**2 * GRID**2))
    lanes = np.arange(128)
    kx = half[:, None] + 128 * (lanes[None, :] // 64)
    of_x = np.stack([decay[kx] * (COULOMB / (np.pi * GRID)), signed[kx] ** 2])
    kz = 64 * np.arange(2)[:, None] + lanes[None, :] % 64
    of_z = np.stack([decay[kz], signed[kz] ** 2], axis=1)
    of_y = np.stack([decay, signed**2])
    return dict(
        to_kz=split_np(to_kz),
        from_kz=split_np(from_kz),
        to_ky=split_np(to_ky),
        from_ky=split_np(to_ky.T),
        to_kx=split_np(to_kx),
        from_kx=split_np(to_kx.T),
        twist=twist.astype(np.float32),
        of_x=of_x.astype(np.float32),
        of_y=of_y.astype(np.float32),
        of_z=of_z.astype(np.float32),
    )


def halves(value):
    high = value.astype(BF16)
    return high, (value - high.astype(F32)).astype(BF16)


def dot(a, b, dims=NN):
    return lax.dot_general(a, b, dims, preferred_element_type=F32)


def dot3(a, b):
    return dot(a[0], b[0]) + (dot(a[0], b[1]) + dot(a[1], b[0]))


def spline_weights(t):
    rest = 1.0 - t
    square = t * t
    cube = square * t
    weights = (
        rest * rest * rest / 6.0,
        (3.0 * cube - 6.0 * square + 4.0) / 6.0,
        (-3.0 * cube + 3.0 * square + 3.0 * t + 1.0) / 6.0,
        cube / 6.0,
    )
    slopes = (-0.5 * rest * rest, 1.5 * square - 2.0 * t, -1.5 * square + t + 0.5, 0.5 * square)
    return weights, slopes


def place(values, lowest, rows):
    offset = lax.broadcasted_iota(jnp.int32, (rows, lowest.shape[1]), 0) - lowest
    out = jnp.where(offset == 3, values[3], 0.0)
    for i in (2, 1, 0):
        out = jnp.where(offset == i, values[i], out)
    return out


def block_index():
    return lax.axis_index("gx"), lax.axis_index("gy"), lax.axis_index("gz")


def spread_kernel(counts_ref, charges_ref, frac_ref, base_ref, out_ref, high_ref, low_ref, acc_ref, zacc_ref):
    ix, iy, iz = block_index()
    width = high_ref.shape[1]
    chunks = charges_ref.shape[1] // width
    acc_ref[...] = jnp.zeros_like(acc_ref)
    zacc_ref[...] = jnp.zeros_like(zacc_ref)

    def step(c, carry):
        at = pl.ds(pl.multiple_of(c * width, width), width)
        slot = lax.broadcasted_iota(jnp.int32, (1, width), 1) + c * width
        charge = jnp.where(slot < counts_ref[0, 0, 0], charges_ref[:, at], 0.0)
        wx, _ = spline_weights(frac_ref[0:1, at])
        wy, _ = spline_weights(frac_ref[1:2, at])
        wz, _ = spline_weights(frac_ref[2:3, at])
        wz = [w * charge for w in wz]
        low_x = base_ref[0:1, at] - ix * CX
        low_y = base_ref[1:2, at] - iy * CY
        low_z = base_ref[2:3, at] - iz * CZ
        rows_x = place(wx, low_x, 24)
        rows_y = place(wy, low_y, CZ)
        rows_z = place(wz, low_z, CZ)
        rim_z = place(wz, low_z - (CZ - HALO), 8)
        rim_row = lax.broadcasted_iota(jnp.int32, (8, 1), 0)
        rim_z = jnp.where((rim_row >= 3) & (rim_row < 6), rim_z, 0.0)
        some_y = rows_y[:ROWS]
        for x in range(SPAN):
            high, low = halves(rows_x[x : x + 1] * some_y)
            high_ref[pl.ds(x * ROWS, ROWS), :] = high
            low_ref[pl.ds(x * ROWS, ROWS), :] = low
        z_high, z_low = halves(rows_z)
        both_z = jnp.concatenate([z_high, z_low], axis=0)
        total = dot(high_ref[...], both_z, NT)
        acc_ref[...] += total[:, :CZ] + total[:, CZ:] + dot(low_ref[...], z_high, NT)
        rims = jnp.concatenate([rows_x[x : x + 1] * rim_z for x in range(SPAN)], axis=0)
        rims_high, rims_low = halves(rims)
        y_high, y_low = halves(rows_y)
        both_y = jnp.concatenate([y_high, y_low], axis=0)
        total = dot(rims_high, both_y, NT)
        zacc_ref[...] += total[:, :CZ] + total[:, CZ:] + dot(rims_low, y_high, NT)
        return carry

    lax.fori_loop(0, chunks, step, 0)
    for x in range(SPAN):
        out_ref[x, 0:64, :] = acc_ref[pl.ds(x * ROWS, 64), :]
        out_ref[x, 64:72, :] = acc_ref[pl.ds(x * ROWS + 64, 8), :] + zacc_ref[pl.ds(x * 8, 8), :]


def forward_kernel(data_ref, to_kz_ref, to_ky_ref, out_ref):
    lane = lax.broadcasted_iota(jnp.int32, (1, 128), 1)
    row = lax.broadcasted_iota(jnp.int32, (8, 128), 0)
    lower = lane < 64
    parts = []
    for x in range(2):
        planes = []
        for iz in range(2):
            pieces = []
            for iy in range(4):
                rim = jnp.where(row < HALO, data_ref[iz * 4 + (iy + 3) % 4, x, 64:72, :], 0.0)
                pieces.append(data_ref[iz * 4 + iy, x, 0:8, :] + rim)
                pieces.append(data_ref[iz * 4 + iy, x, 8:64, :])
            planes.append(jnp.concatenate(pieces, axis=0))
        rims = []
        for iz in range(2):
            tiles = [data_ref[iz * 4 + iy, x, 64:72, :] for iy in range(4)]
            turned = [pltpu.roll(tiles[1], 64, 1), pltpu.roll(tiles[3], 64, 1)]
            first = tiles[0] + jnp.where(lower, turned[1], turned[0])
            second = tiles[2] + jnp.where(lower, turned[0], turned[1])
            rims.append(jnp.concatenate([first, second], axis=1))
        rims = jnp.concatenate(rims + [jnp.zeros((112, 256), F32)], axis=0).T
        planes[1] = planes[1] + jnp.where(lane < HALO, pltpu.roll(rims, 125, 1), 0.0)
        planes[0] = planes[0] + jnp.where(lane < HALO, pltpu.roll(rims, 117, 1), 0.0)
        plane = jnp.concatenate(planes, axis=1)
        parts.append(dot3(halves(plane), (to_kz_ref[0], to_kz_ref[1])))
    rows = []
    for c in range(2):
        zero, one = (p[:, c * 128 : (c + 1) * 128] for p in parts)
        first = jnp.where(lower, zero, pltpu.roll(one, 64, 1))
        second = jnp.where(lower, pltpu.roll(zero, 64, 1), one)
        rows.append(jnp.concatenate([first, second], axis=1))
    both = jnp.concatenate(rows, axis=0)
    out = dot3((to_ky_ref[0], to_ky_ref[1]), halves(both))
    out_ref[0:64] = out[:, :128].reshape(64, 8, 128)
    out_ref[64:128] = out[:, 128:].reshape(64, 8, 128)


def middle_kernel(data_ref, to_kx_ref, from_kx_ref, twist_ref, of_x_ref, of_z_ref, of_y_ref, out_ref):
    ix, iy, iz = block_index()
    mine = ix * COLUMN + iz * 4 + iy
    half, group = mine // 64, mine % 64
    lane = lax.broadcasted_iota(jnp.int32, (1, 128), 1)
    sign = jnp.where(lane < 64, 1.0, -1.0)
    both = jnp.concatenate(
        [
            jnp.concatenate([data_ref[:, c * 4 + i, :] for i in range(4)], axis=1)
            for c in range(2)
        ],
        axis=0,
    )
    out = dot3((to_kx_ref[0], to_kx_ref[1]), halves(both))
    cos, sin = twist_ref[0], twist_ref[1]
    of_z = of_z_ref[half]
    scale_xz = of_x_ref[0] * of_z[0:1]
    square_xz = of_x_ref[1] + of_z[1:2]
    reals, imags = [], []
    for i in range(4):
        real = out[:128, i * 128 : (i + 1) * 128]
        imag = out[128:, i * 128 : (i + 1) * 128]
        real, imag = real * cos + imag * sin, imag * cos - real * sin
        real = real * sign + pltpu.roll(real, 64, 1)
        imag = imag * sign + pltpu.roll(imag, 64, 1)
        ky = group * 4 + i
        square = square_xz + of_y_ref[1, ky]
        green = jnp.where(square > 0.0, scale_xz * of_y_ref[0, ky] / jnp.maximum(square, 1.0), 0.0)
        real, imag = real * green, imag * green
        real = real * sign + pltpu.roll(real, 64, 1)
        imag = imag * sign + pltpu.roll(imag, 64, 1)
        real, imag = real * cos - imag * sin, imag * cos + real * sin
        reals.append(real)
        imags.append(imag)
    both = jnp.concatenate(
        [jnp.concatenate(reals, axis=1), jnp.concatenate(imags, axis=1)], axis=0
    )
    out = dot3((from_kx_ref[0], from_kx_ref[1]), halves(both))
    for c in range(2):
        for i in range(4):
            out_ref[:, c * 4 + i, :] = out[c * 128 : (c + 1) * 128, i * 128 : (i + 1) * 128]


def backward_kernel(data_ref, from_ky_ref, from_kz_ref, out_ref):
    lane = lax.broadcasted_iota(jnp.int32, (1, 128), 1)
    row = lax.broadcasted_iota(jnp.int32, (8, 128), 0)
    lower = lane < 64
    both = jnp.concatenate(
        [data_ref[0:64].reshape(512, 128), data_ref[64:128].reshape(512, 128)], axis=1
    )
    out = dot3((from_ky_ref[0], from_ky_ref[1]), halves(both))
    tiles = [[], []]
    for c in range(2):
        first, second = out[c * 256 : (c + 1) * 256, :128], out[c * 256 : (c + 1) * 256, 128:]
        tiles[0].append(jnp.where(lower, first, pltpu.roll(second, 64, 1)))
        tiles[1].append(jnp.where(lower, pltpu.roll(first, 64, 1), second))
    for x in range(2):
        plane = dot3(
            halves(jnp.concatenate(tiles[x], axis=1)), (from_kz_ref[0], from_kz_ref[1])
        )
        turned = [plane[:, h * 128 : (h + 1) * 128].T[:8] for h in range(2)]
        for iz in range(2):
            near = plane[:, iz * 128 : (iz + 1) * 128]
            strips = (turned[1 - iz][:, :128], turned[1 - iz][:, 128:])
            rolled = [pltpu.roll(s, 64, 1) for s in strips]
            for iy in range(4):
                after = (iy + 1) % 4
                t = iy // 2
                if iy % 2 == 0:
                    strip = strips[t]
                else:
                    strip = jnp.where(lower, rolled[t], rolled[1 - t])
                out_ref[iz * 4 + iy, x, 0:64, :] = near[iy * 64 : iy * 64 + 64]
                out_ref[iz * 4 + iy, x, 64:72, :] = jnp.where(
                    row < HALO, near[after * 64 : after * 64 + 8], pltpu.roll(strip, HALO, 0)
                )


def gather_kernel(counts_ref, charges_ref, frac_ref, base_ref, data_ref, out_ref, pot_ref, rim_ref):
    ix, iy, iz = block_index()
    width = 128
    chunks = charges_ref.shape[1] // width
    for x in range(SPAN):
        high, low = halves(data_ref[x])
        pot_ref[pl.ds(x * ROWS, ROWS), 0:128] = high
        pot_ref[pl.ds(x * ROWS, ROWS), 128:256] = low
    high, low = halves(jnp.concatenate([data_ref[x, 64:72, :] for x in range(SPAN)], axis=0))
    rim_ref[:, 0:128] = high
    rim_ref[:, 128:256] = low

    def step(c, carry):
        at = pl.ds(pl.multiple_of(c * width, width), width)
        slot = lax.broadcasted_iota(jnp.int32, (1, width), 1) + c * width
        charge = jnp.where(slot < counts_ref[0, 0, 0], charges_ref[:, at], 0.0)
        wx, sx = spline_weights(frac_ref[0:1, at])
        wy, sy = spline_weights(frac_ref[1:2, at])
        wz, sz = spline_weights(frac_ref[2:3, at])
        low_x = base_ref[0:1, at] - ix * CX
        low_y = base_ref[1:2, at] - iy * CY
        low_z = base_ref[2:3, at] - iz * CZ
        rows_x, grads_x = place(wx, low_x, 24), place(sx, low_x, 24)
        rows_y, grads_y = place(wy, low_y, CZ), place(sy, low_y, CZ)
        rows_z, grads_z = place(wz, low_z, CZ), place(sz, low_z, CZ)
        rim_row = lax.broadcasted_iota(jnp.int32, (8, 1), 0)
        inside = (rim_row >= 3) & (rim_row < 6)
        rim_low = low_z - (CZ - HALO)
        rim_rows = jnp.where(inside, place(wz, rim_low, 8), 0.0)
        rim_grads = jnp.where(inside, place(sz, rim_low, 8), 0.0)

        def folded(ref, rows, grads):
            high, low = halves(jnp.concatenate([rows, grads], axis=1))
            return dot(ref[...], jnp.concatenate([high, high], axis=0)) + dot(ref[:, 0:128], low)

        main = folded(pot_ref, rows_z, grads_z)
        rims = folded(rim_ref, rows_y, grads_y)
        force_x = jnp.zeros((8, width), F32)
        force_y = jnp.zeros((8, width), F32)
        force_z = jnp.zeros((8, width), F32)
        for x in range(SPAN):
            rim_plain = rims[x * 8 : x * 8 + 8, :width]
            rim_sloped = rims[x * 8 : x * 8 + 8, width:]
            sum_x = rim_rows * rim_plain
            sum_y = rim_rows * rim_sloped
            sum_z = rim_grads * rim_plain
            for y in range(ROWS // 8):
                low = x * ROWS + y * 8
                plain, sloped = main[low : low + 8, :width], main[low : low + 8, width:]
                near = rows_y[y * 8 : y * 8 + 8]
                sum_x += plain * near
                sum_y += plain * grads_y[y * 8 : y * 8 + 8]
                sum_z += sloped * near
            force_x += grads_x[x : x + 1] * sum_x
            force_y += rows_x[x : x + 1] * sum_y
            force_z += rows_x[x : x + 1] * sum_z
        total = [jnp.sum(f, axis=0, keepdims=True) for f in (force_x, force_y, force_z)]
        out_ref[:, at] = -charge * jnp.concatenate(total, axis=0)
        return carry

    lax.fori_loop(0, chunks, step, 0)


VMEM = pl.BlockSpec(memory_space=pltpu.VMEM)
SMEM = pl.BlockSpec(memory_space=pltpu.SMEM)


def call(kernel, shape, specs, scratch=(), limit=48 << 20):
    return pl.pallas_call(
        kernel,
        out_shape=jax.ShapeDtypeStruct(shape, F32),
        in_specs=specs,
        out_specs=VMEM,
        scratch_shapes=list(scratch),
        compiler_params=pltpu.CompilerParams(vmem_limit_bytes=limit),
        interpret=INTERPRET,
    )


def shift(value, steps):
    count = lax.axis_size("gx")
    return lax.ppermute(value, "gx", [(s, (s + steps) % count) for s in range(count)])


def per_device(charges, fractions, base_cells, counts):
    t = {name: jnp.asarray(value) for name, value in tables().items()}
    charges = charges.reshape(1, -1)
    spread = call(
        spread_kernel,
        (SPAN, ROWS, CZ),
        [SMEM, VMEM, VMEM, VMEM],
        [
            pltpu.VMEM((SPAN * ROWS, 512), BF16),
            pltpu.VMEM((SPAN * ROWS, 512), BF16),
            pltpu.VMEM((SPAN * ROWS, CZ), F32),
            pltpu.VMEM((SPAN * 8, CZ), F32),
        ],
    )
    grid = spread(counts, charges, fractions, base_cells)
    arrived = shift(grid[CX:], 1)
    grid = jnp.concatenate([grid[:HALO] + arrived, grid[HALO:CX]], axis=0)
    grid = grid.reshape(COLUMN, 2, ROWS, CZ)
    planes = lax.all_to_all(grid, ("gz", "gy"), 0, 0, tiled=True)
    forward = call(forward_kernel, (128, 8, 128), [VMEM] * 3)
    modes = forward(planes, t["to_kz"], t["to_ky"])
    modes = lax.all_to_all(modes, ("gx", "gz", "gy"), 0, 0, tiled=True)
    middle = call(middle_kernel, (128, 8, 128), [VMEM] * 6 + [SMEM])
    modes = middle(
        modes, t["to_kx"], t["from_kx"], t["twist"], t["of_x"], t["of_z"], t["of_y"]
    )
    modes = lax.all_to_all(modes, ("gx", "gz", "gy"), 0, 0, tiled=True)
    backward = call(backward_kernel, (COLUMN, 2, ROWS, CZ), [VMEM] * 3)
    planes = backward(modes, t["from_ky"], t["from_kz"])
    planes = lax.all_to_all(planes, ("gz", "gy"), 0, 0, tiled=True)
    planes = planes.reshape(CX, ROWS, CZ)
    planes = jnp.concatenate([planes, shift(planes[:HALO], -1)], axis=0)
    gather = call(
        gather_kernel,
        fractions.shape,
        [SMEM] + [VMEM] * 4,
        [pltpu.VMEM((SPAN * ROWS, 256), BF16), pltpu.VMEM((SPAN * 8, 256), BF16)],
    )
    return gather(counts, charges, fractions, base_cells, planes)


def solution(mesh):
    split = ("gz", "gy", "gx")
    return jax.shard_map(
        per_device,
        mesh=mesh,
        in_specs=(P(split), P(None, split), P(None, split), P("gz", "gy", "gx")),
        out_specs=P(None, split),
        check_vma=False,
    )
```

```python
import functools

import jax
import jax.numpy as jnp
import numpy as np
from jax import lax
from jax.experimental import pallas as pl
from jax.experimental.pallas import tpu as pltpu
from jax.sharding import PartitionSpec as P

GRID = 256
ORDER = 4
HALO = ORDER - 1
COULOMB = 332.0636
EWALD = 0.7
CX, CY, CZ = 16, 64, 128
ROWS = 72
SPAN = CX + HALO
COLUMN = 8
F32 = jnp.float32
BF16 = jnp.bfloat16
NN = (((1,), (0,)), ((), ()))
NT = (((1,), (1,)), ((), ()))


def split_np(a):
    a = np.asarray(a, np.float32)
    high = a.astype(jnp.bfloat16)
    low = (a - high.astype(np.float32)).astype(jnp.bfloat16)
    return np.stack([high, low])


def tables():
    k = np.arange(GRID)
    half = np.arange(GRID // 2)

    def turn(first, second, length):
        angle = (first[:, None] * second[None, :] % length) * (2.0 * np.pi / length)
        return np.cos(angle), np.sin(angle)

    cos, sin = turn(k, half, GRID)
    to_kz = np.concatenate([cos, -sin], axis=1)
    twice = np.where(half > 0, 2.0, 1.0)[:, None]
    from_kz = np.concatenate([twice * cos.T, -twice * sin.T], axis=0)
    cos, sin = turn(k, k, GRID)
    real = np.concatenate([cos, sin], axis=1).reshape(64, 4, 512)
    imag = np.concatenate([-sin, cos], axis=1).reshape(64, 4, 512)
    to_ky = np.stack([real, imag], axis=1).reshape(512, 512)
    cos, sin = turn(half, half, GRID // 2)
    to_kx = np.concatenate(
        [np.concatenate([cos, sin], axis=1), np.concatenate([-sin, cos], axis=1)], axis=0
    )
    angle = half[:, None] * (2.0 * np.pi / GRID) * np.ones((1, 128))
    upper = np.arange(128)[None, :] >= 64
    twist = np.stack([np.where(upper, np.cos(angle), 1.0), np.where(upper, np.sin(angle), 0.0)])
    signed = np.where(2 * k < GRID, k, k - GRID).astype(np.float64)
    spline = 36.0 / (4.0 + 2.0 * np.cos(k * (2.0 * np.pi / GRID))) ** 2
    spline[GRID // 2] = 0.0
    decay = spline * np.exp(-np.pi**2 * signed**2 / (EWALD**2 * GRID**2))
    lanes = np.arange(128)
    kx = half[:, None] + 128 * (lanes[None, :] // 64)
    of_x = np.stack([decay[kx] * (COULOMB / (np.pi * GRID)), signed[kx] ** 2])
    kz = 64 * np.arange(2)[:, None] + lanes[None, :] % 64
    of_z = np.stack([decay[kz], signed[kz] ** 2], axis=1)
    of_y = np.stack([decay, signed**2])
    return dict(
        to_kz=split_np(to_kz),
        from_kz=split_np(from_kz),
        to_ky=split_np(to_ky),
        from_ky=split_np(to_ky.T),
        to_kx=split_np(to_kx),
        from_kx=split_np(to_kx.T),
        twist=twist.astype(np.float32),
        of_x=of_x.astype(np.float32),
        of_y=of_y.astype(np.float32),
        of_z=of_z.astype(np.float32),
    )


def halves(value):
    high = value.astype(BF16)
    return high, (value - high.astype(F32)).astype(BF16)


def dot(a, b, dims=NN):
    return lax.dot_general(a, b, dims, preferred_element_type=F32)


def dot3(a, b):
    return dot(a[0], b[0]) + (dot(a[0], b[1]) + dot(a[1], b[0]))


def spline_weights(t):
    rest = 1.0 - t
    square = t * t
    cube = square * t
    weights = (
        rest * rest * rest / 6.0,
        (3.0 * cube - 6.0 * square + 4.0) / 6.0,
        (-3.0 * cube + 3.0 * square + 3.0 * t + 1.0) / 6.0,
        cube / 6.0,
    )
    slopes = (-0.5 * rest * rest, 1.5 * square - 2.0 * t, -1.5 * square + t + 0.5, 0.5 * square)
    return weights, slopes


def place(values, lowest, rows):
    offset = lax.broadcasted_iota(jnp.int32, (rows, lowest.shape[1]), 0) - lowest
    out = jnp.where(offset == 3, values[3], 0.0)
    for i in (2, 1, 0):
        out = jnp.where(offset == i, values[i], out)
    return out


def block_index():
    return lax.axis_index("gx"), lax.axis_index("gy"), lax.axis_index("gz")


def spread_kernel(counts_ref, charges_ref, frac_ref, base_ref, out_ref, high_ref, low_ref, acc_ref, zacc_ref):
    ix, iy, iz = block_index()
    width = high_ref.shape[1]
    chunks = charges_ref.shape[1] // width
    acc_ref[...] = jnp.zeros_like(acc_ref)
    zacc_ref[...] = jnp.zeros_like(zacc_ref)

    def step(c, carry):
        at = pl.ds(pl.multiple_of(c * width, width), width)
        slot = lax.broadcasted_iota(jnp.int32, (1, width), 1) + c * width
        charge = jnp.where(slot < counts_ref[0, 0, 0], charges_ref[:, at], 0.0)
        wx, _ = spline_weights(frac_ref[0:1, at])
        wy, _ = spline_weights(frac_ref[1:2, at])
        wz, _ = spline_weights(frac_ref[2:3, at])
        wz = [w * charge for w in wz]
        low_x = base_ref[0:1, at] - ix * CX
        low_y = base_ref[1:2, at] - iy * CY
        low_z = base_ref[2:3, at] - iz * CZ
        rows_x = place(wx, low_x, 24)
        rows_y = place(wy, low_y, CZ)
        rows_z = place(wz, low_z, CZ)
        rim_z = place(wz, low_z - (CZ - HALO), 8)
        rim_row = lax.broadcasted_iota(jnp.int32, (8, 1), 0)
        rim_z = jnp.where((rim_row >= 3) & (rim_row < 6), rim_z, 0.0)
        some_y = rows_y[:ROWS]
        for x in range(SPAN):
            high, low = halves(rows_x[x : x + 1] * some_y)
            high_ref[pl.ds(x * ROWS, ROWS), :] = high
            low_ref[pl.ds(x * ROWS, ROWS), :] = low
        z_high, z_low = halves(rows_z)
        both_z = jnp.concatenate([z_high, z_low], axis=0)
        total = dot(high_ref[...], both_z, NT)
        acc_ref[...] += total[:, :CZ] + total[:, CZ:] + dot(low_ref[...], z_high, NT)
        rims = jnp.concatenate([rows_x[x : x + 1] * rim_z for x in range(SPAN)], axis=0)
        rims_high, rims_low = halves(rims)
        y_high, y_low = halves(rows_y)
        both_y = jnp.concatenate([y_high, y_low], axis=0)
        total = dot(rims_high, both_y, NT)
        zacc_ref[...] += total[:, :CZ] + total[:, CZ:] + dot(rims_low, y_high, NT)
        return carry

    lax.fori_loop(0, chunks, step, 0)
    for x in range(SPAN):
        out_ref[x, 0:64, :] = acc_ref[pl.ds(x * ROWS, 64), :]
        out_ref[x, 64:72, :] = acc_ref[pl.ds(x * ROWS + 64, 8), :] + zacc_ref[pl.ds(x * 8, 8), :]


def forward_kernel(data_ref, to_kz_ref, to_ky_ref, out_ref):
    lane = lax.broadcasted_iota(jnp.int32, (1, 128), 1)
    row = lax.broadcasted_iota(jnp.int32, (8, 128), 0)
    lower = lane < 64
    parts = []
    for x in range(2):
        planes = []
        for iz in range(2):
            pieces = []
            for iy in range(4):
                rim = jnp.where(row < HALO, data_ref[iz * 4 + (iy + 3) % 4, x, 64:72, :], 0.0)
                pieces.append(data_ref[iz * 4 + iy, x, 0:8, :] + rim)
                pieces.append(data_ref[iz * 4 + iy, x, 8:64, :])
            planes.append(jnp.concatenate(pieces, axis=0))
        rims = []
        for iz in range(2):
            tiles = [data_ref[iz * 4 + iy, x, 64:72, :] for iy in range(4)]
            turned = [pltpu.roll(tiles[1], 64, 1), pltpu.roll(tiles[3], 64, 1)]
            first = tiles[0] + jnp.where(lower, turned[1], turned[0])
            second = tiles[2] + jnp.where(lower, turned[0], turned[1])
            rims.append(jnp.concatenate([first, second], axis=1))
        rims = jnp.concatenate(rims + [jnp.zeros((112, 256), F32)], axis=0).T
        planes[1] = planes[1] + jnp.where(lane < HALO, pltpu.roll(rims, 125, 1), 0.0)
        planes[0] = planes[0] + jnp.where(lane < HALO, pltpu.roll(rims, 117, 1), 0.0)
        plane = jnp.concatenate(planes, axis=1)
        parts.append(dot3(halves(plane), (to_kz_ref[0], to_kz_ref[1])))
    rows = []
    for c in range(2):
        zero, one = (p[:, c * 128 : (c + 1) * 128] for p in parts)
        first = jnp.where(lower, zero, pltpu.roll(one, 64, 1))
        second = jnp.where(lower, pltpu.roll(zero, 64, 1), one)
        rows.append(jnp.concatenate([first, second], axis=1))
    both = jnp.concatenate(rows, axis=0)
    out = dot3((to_ky_ref[0], to_ky_ref[1]), halves(both))
    out_ref[0:64] = out[:, :128].reshape(64, 8, 128)
    out_ref[64:128] = out[:, 128:].reshape(64, 8, 128)


def middle_kernel(data_ref, to_kx_ref, from_kx_ref, twist_ref, of_x_ref, of_z_ref, of_y_ref, out_ref):
    ix, iy, iz = block_index()
    mine = ix * COLUMN + iz * 4 + iy
    half, group = mine // 64, mine % 64
    lane = lax.broadcasted_iota(jnp.int32, (1, 128), 1)
    sign = jnp.where(lane < 64, 1.0, -1.0)
    both = jnp.concatenate(
        [
            jnp.concatenate([data_ref[:, c * 4 + i, :] for i in range(4)], axis=1)
            for c in range(2)
        ],
        axis=0,
    )
    out = dot3((to_kx_ref[0], to_kx_ref[1]), halves(both))
    cos, sin = twist_ref[0], twist_ref[1]
    of_z = of_z_ref[half]
    scale_xz = of_x_ref[0] * of_z[0:1]
    square_xz = of_x_ref[1] + of_z[1:2]
    reals, imags = [], []
    for i in range(4):
        real = out[:128, i * 128 : (i + 1) * 128]
        imag = out[128:, i * 128 : (i + 1) * 128]
        real, imag = real * cos + imag * sin, imag * cos - real * sin
        real = real * sign + pltpu.roll(real, 64, 1)
        imag = imag * sign + pltpu.roll(imag, 64, 1)
        ky = group * 4 + i
        square = square_xz + of_y_ref[1, ky]
        green = jnp.where(square > 0.0, scale_xz * of_y_ref[0, ky] / jnp.maximum(square, 1.0), 0.0)
        real, imag = real * green, imag * green
        real = real * sign + pltpu.roll(real, 64, 1)
        imag = imag * sign + pltpu.roll(imag, 64, 1)
        real, imag = real * cos - imag * sin, imag * cos + real * sin
        reals.append(real)
        imags.append(imag)
    both = jnp.concatenate(
        [jnp.concatenate(reals, axis=1), jnp.concatenate(imags, axis=1)], axis=0
    )
    out = dot3((from_kx_ref[0], from_kx_ref[1]), halves(both))
    for c in range(2):
        for i in range(4):
            out_ref[:, c * 4 + i, :] = out[c * 128 : (c + 1) * 128, i * 128 : (i + 1) * 128]


def backward_kernel(data_ref, from_ky_ref, from_kz_ref, out_ref):
    lane = lax.broadcasted_iota(jnp.int32, (1, 128), 1)
    row = lax.broadcasted_iota(jnp.int32, (8, 128), 0)
    lower = lane < 64
    both = jnp.concatenate(
        [data_ref[0:64].reshape(512, 128), data_ref[64:128].reshape(512, 128)], axis=1
    )
    out = dot3((from_ky_ref[0], from_ky_ref[1]), halves(both))
    tiles = [[], []]
    for c in range(2):
        first, second = out[c * 256 : (c + 1) * 256, :128], out[c * 256 : (c + 1) * 256, 128:]
        tiles[0].append(jnp.where(lower, first, pltpu.roll(second, 64, 1)))
        tiles[1].append(jnp.where(lower, pltpu.roll(first, 64, 1), second))
    for x in range(2):
        plane = dot3(
            halves(jnp.concatenate(tiles[x], axis=1)), (from_kz_ref[0], from_kz_ref[1])
        )
        turned = [plane[:, h * 128 : (h + 1) * 128].T[:8] for h in range(2)]
        for iz in range(2):
            near = plane[:, iz * 128 : (iz + 1) * 128]
            strips = (turned[1 - iz][:, :128], turned[1 - iz][:, 128:])
            rolled = [pltpu.roll(s, 64, 1) for s in strips]
            for iy in range(4):
                after = (iy + 1) % 4
                t = iy // 2
                if iy % 2 == 0:
                    strip = strips[t]
                else:
                    strip = jnp.where(lower, rolled[t], rolled[1 - t])
                out_ref[iz * 4 + iy, x, 0:64, :] = near[iy * 64 : iy * 64 + 64]
                out_ref[iz * 4 + iy, x, 64:72, :] = jnp.where(
                    row < HALO, near[after * 64 : after * 64 + 8], pltpu.roll(strip, HALO, 0)
                )


def gather_kernel(counts_ref, charges_ref, frac_ref, base_ref, data_ref, out_ref, pot_ref, rim_ref):
    ix, iy, iz = block_index()
    width = 128
    chunks = charges_ref.shape[1] // width
    for x in range(SPAN):
        high, low = halves(data_ref[x])
        pot_ref[pl.ds(x * ROWS, ROWS), 0:128] = high
        pot_ref[pl.ds(x * ROWS, ROWS), 128:256] = low
    high, low = halves(jnp.concatenate([data_ref[x, 64:72, :] for x in range(SPAN)], axis=0))
    rim_ref[:, 0:128] = high
    rim_ref[:, 128:256] = low

    def step(c, carry):
        at = pl.ds(pl.multiple_of(c * width, width), width)
        slot = lax.broadcasted_iota(jnp.int32, (1, width), 1) + c * width
        charge = jnp.where(slot < counts_ref[0, 0, 0], charges_ref[:, at], 0.0)
        wx, sx = spline_weights(frac_ref[0:1, at])
        wy, sy = spline_weights(frac_ref[1:2, at])
        wz, sz = spline_weights(frac_ref[2:3, at])
        low_x = base_ref[0:1, at] - ix * CX
        low_y = base_ref[1:2, at] - iy * CY
        low_z = base_ref[2:3, at] - iz * CZ
        rows_x, grads_x = place(wx, low_x, 24), place(sx, low_x, 24)
        rows_y, grads_y = place(wy, low_y, CZ), place(sy, low_y, CZ)
        rows_z, grads_z = place(wz, low_z, CZ), place(sz, low_z, CZ)
        rim_row = lax.broadcasted_iota(jnp.int32, (8, 1), 0)
        inside = (rim_row >= 3) & (rim_row < 6)
        rim_low = low_z - (CZ - HALO)
        rim_rows = jnp.where(inside, place(wz, rim_low, 8), 0.0)
        rim_grads = jnp.where(inside, place(sz, rim_low, 8), 0.0)

        def folded(ref, rows, grads):
            high, low = halves(jnp.concatenate([rows, grads], axis=1))
            return dot(ref[...], jnp.concatenate([high, high], axis=0)) + dot(ref[:, 0:128], low)

        main = folded(pot_ref, rows_z, grads_z)
        rims = folded(rim_ref, rows_y, grads_y)
        force_x = jnp.zeros((8, width), F32)
        force_y = jnp.zeros((8, width), F32)
        force_z = jnp.zeros((8, width), F32)
        for x in range(SPAN):
            rim_plain = rims[x * 8 : x * 8 + 8, :width]
            rim_sloped = rims[x * 8 : x * 8 + 8, width:]
            sum_x = rim_rows * rim_plain
            sum_y = rim_rows * rim_sloped
            sum_z = rim_grads * rim_plain
            for y in range(ROWS // 8):
                low = x * ROWS + y * 8
                plain, sloped = main[low : low + 8, :width], main[low : low + 8, width:]
                near = rows_y[y * 8 : y * 8 + 8]
                sum_x += plain * near
                sum_y += plain * grads_y[y * 8 : y * 8 + 8]
                sum_z += sloped * near
            force_x += grads_x[x : x + 1] * sum_x
            force_y += rows_x[x : x + 1] * sum_y
            force_z += rows_x[x : x + 1] * sum_z
        total = [jnp.sum(f, axis=0, keepdims=True) for f in (force_x, force_y, force_z)]
        out_ref[:, at] = -charge * jnp.concatenate(total, axis=0)
        return carry

    lax.fori_loop(0, chunks, step, 0)


MESH = pl.DeviceIdType.MESH
INPUTS = ("charges", "fractions", "base_cells")
NAMES = ("to_kz", "to_ky", "to_kx", "twist", "of_x", "of_z", "from_kx", "from_ky", "from_kz")


def fused_kernel(counts_ref, of_y_ref, *refs):
    total = len(INPUTS) + len(NAMES)
    hbm, out_ref, refs = refs[:total], refs[total], refs[total + 1 :]
    local, refs = refs[:total], refs[total:]
    (high_ref, low_ref, acc_ref, zacc_ref, grid_ref, rim_in_ref, planes_ref, send_ref, modes_ref,
     send2_ref, modes2_ref, blocks_ref, near_ref, pot_ref, rim_ref,
     load_sem, rim_send, rim_recv, a_send, a_recv, c_send, c_recv, d_send, d_recv,
     b_send, b_recv, e_send, e_recv) = refs
    loads = [pltpu.make_async_copy(h, v, load_sem.at[i]) for i, (h, v) in enumerate(zip(hbm, local))]
    for load in loads:
        load.start()
    charges_ref, frac_ref, base_ref = local[: len(INPUTS)]
    t = dict(zip(NAMES, local[len(INPUTS) :]))
    ix, iy, iz = block_index()
    count_x = lax.axis_size("gx")
    j = iz * 4 + iy
    mine = ix * COLUMN + j
    after = {"gx": lax.rem(ix + 1, count_x)}
    before = {"gx": lax.rem(ix + count_x - 1, count_x)}

    def device(index):
        low = lax.rem(index, COLUMN)
        return {"gx": lax.div(index, COLUMN), "gz": lax.div(low, 4), "gy": lax.rem(low, 4)}

    barrier = pltpu.get_barrier_semaphore()

    def greet(o, carry):
        pl.semaphore_signal(
            barrier, inc=1, device_id=device(lax.rem(mine + o, 128)), device_id_type=MESH
        )
        return carry

    lax.fori_loop(1, 128, greet, 0)
    for load in loads[: len(INPUTS)]:
        load.wait()
    spread_kernel(counts_ref, charges_ref, frac_ref, base_ref, grid_ref, high_ref, low_ref, acc_ref, zacc_ref)
    pl.semaphore_wait(barrier, 127)

    rim = pltpu.make_async_remote_copy(
        src_ref=grid_ref.at[pl.ds(CX, HALO)], dst_ref=rim_in_ref, send_sem=rim_send, recv_sem=rim_recv,
        device_id=after, device_id_type=MESH,
    )
    rim.start()

    def column(o):
        to = lax.rem(j + o, COLUMN)
        return to, {"gz": lax.div(to, 4), "gy": lax.rem(to, 4)}

    copies = []
    for o in range(1, COLUMN):
        to, where = column(o)
        copies.append((to, pltpu.make_async_remote_copy(
            src_ref=grid_ref.at[pl.ds(2 * to, 2)], dst_ref=planes_ref.at[j],
            send_sem=a_send.at[o], recv_sem=a_recv.at[o], device_id=where, device_id_type=MESH,
        )))
    for to, copy in copies:
        pl.when(to >= 2)(copy.start)
    rim.wait()
    grid_ref[0:HALO] += rim_in_ref[...]
    for to, copy in copies:
        pl.when(to < 2)(copy.start)
    planes_ref[pl.ds(j, 1)] = grid_ref[pl.ds(2 * j, 2)].reshape(1, 2, ROWS, CZ)
    for load in loads[len(INPUTS) :]:
        load.wait()
    for _, copy in copies:
        copy.wait()

    def spray(source, target, send_sem, recv_sem):
        def one(o, carry):
            to = lax.rem(mine + o, 128)
            pltpu.make_async_remote_copy(
                src_ref=source.at[to], dst_ref=target.at[mine], send_sem=send_sem, recv_sem=recv_sem,
                device_id=device(to), device_id_type=MESH,
            ).start()
            return carry

        lax.fori_loop(1, 128, one, 0)
        target[pl.ds(mine, 1)] = source[pl.ds(mine, 1)]
        sent = source.at[pl.ds(0, 127)]
        pltpu.make_async_copy(sent, sent, send_sem).wait()
        got = target.at[pl.ds(0, 127)]
        pltpu.make_async_copy(got, got, recv_sem).wait()

    forward_kernel(planes_ref, t["to_kz"], t["to_ky"], send_ref)
    spray(send_ref, modes_ref, c_send, c_recv)
    middle_kernel(modes_ref, t["to_kx"], t["from_kx"], t["twist"], t["of_x"], t["of_z"], of_y_ref, send2_ref)
    spray(send2_ref, modes2_ref, d_send, d_recv)
    backward_kernel(modes2_ref, t["from_ky"], t["from_kz"], blocks_ref)

    copies = []
    for o in range(1, COLUMN):
        to, where = column(o)
        copies.append(pltpu.make_async_remote_copy(
            src_ref=blocks_ref.at[to], dst_ref=near_ref.at[pl.ds(2 * j, 2)],
            send_sem=b_send.at[o], recv_sem=b_recv.at[o], device_id=where, device_id_type=MESH,
        ))
    for copy in copies:
        copy.start()
    near_ref[pl.ds(2 * j, 2)] = blocks_ref[pl.ds(j, 1)].reshape(2, ROWS, CZ)
    for copy in copies:
        copy.wait()
    rim = pltpu.make_async_remote_copy(
        src_ref=near_ref.at[pl.ds(0, HALO)], dst_ref=near_ref.at[pl.ds(CX, HALO)],
        send_sem=e_send, recv_sem=e_recv, device_id=before, device_id_type=MESH,
    )
    rim.start()
    rim.wait()
    gather_kernel(counts_ref, charges_ref, frac_ref, base_ref, near_ref, out_ref, pot_ref, rim_ref)


def per_device(charges, fractions, base_cells, counts):
    t = {name: jnp.asarray(value) for name, value in tables().items()}
    arrays = [charges.reshape(1, -1), fractions, base_cells] + [t[name] for name in NAMES]
    smem = pl.BlockSpec(memory_space=pltpu.SMEM)
    dma = pltpu.SemaphoreType.DMA
    scratch = [pltpu.VMEM(a.shape, a.dtype) for a in arrays]
    scratch += [
        pltpu.VMEM((SPAN * ROWS, 512), BF16),
        pltpu.VMEM((SPAN * ROWS, 512), BF16),
        pltpu.VMEM((SPAN * ROWS, CZ), F32),
        pltpu.VMEM((SPAN * 8, CZ), F32),
        pltpu.VMEM((SPAN, ROWS, CZ), F32),
        pltpu.VMEM((HALO, ROWS, CZ), F32),
        pltpu.VMEM((COLUMN, 2, ROWS, CZ), F32),
        pltpu.VMEM((128, 8, 128), F32),
        pltpu.VMEM((128, 8, 128), F32),
        pltpu.VMEM((128, 8, 128), F32),
        pltpu.VMEM((128, 8, 128), F32),
        pltpu.VMEM((COLUMN, 2, ROWS, CZ), F32),
        pltpu.VMEM((SPAN, ROWS, CZ), F32),
        pltpu.VMEM((SPAN * ROWS, 256), BF16),
        pltpu.VMEM((SPAN * 8, 256), BF16),
        dma((len(arrays),)), dma, dma, dma((COLUMN,)), dma((COLUMN,)), dma, dma, dma, dma,
        dma((COLUMN,)), dma((COLUMN,)), dma, dma,
    ]
    return pl.pallas_call(
        fused_kernel,
        out_shape=jax.ShapeDtypeStruct(fractions.shape, F32),
        in_specs=[smem, smem] + [pl.BlockSpec(memory_space=pl.ANY)] * len(arrays),
        out_specs=pl.BlockSpec(memory_space=pltpu.VMEM),
        scratch_shapes=scratch,
        compiler_params=pltpu.CompilerParams(
            collective_id=0, has_side_effects=True, vmem_limit_bytes=48 << 20
        ),
    )(counts, t["of_y"], *arrays)


def solution(mesh):
    split = ("gz", "gy", "gx")
    return jax.shard_map(
        per_device,
        mesh=mesh,
        in_specs=(P(split), P(None, split), P(None, split), P("gz", "gy", "gx")),
        out_specs=P(None, split),
        check_vma=False,
    )
```

```python
import functools

import jax
import jax.numpy as jnp
import numpy as np
from jax import lax
from jax.experimental import pallas as pl
from jax.experimental.pallas import tpu as pltpu
from jax.sharding import PartitionSpec as P

GRID = 256
ORDER = 4
HALO = ORDER - 1
COULOMB = 332.0636
EWALD = 0.7
CX, CY, CZ = 16, 64, 128
ROWS = 72
SPAN = CX + HALO
COLUMN = 8
F32 = jnp.float32
BF16 = jnp.bfloat16
NN = (((1,), (0,)), ((), ()))
NT = (((1,), (1,)), ((), ()))


def split_np(a):
    a = np.asarray(a, np.float32)
    high = a.astype(jnp.bfloat16)
    low = (a - high.astype(np.float32)).astype(jnp.bfloat16)
    return np.stack([high, low])


def tables():
    k = np.arange(GRID)
    half = np.arange(GRID // 2)

    def turn(first, second, length):
        angle = (first[:, None] * second[None, :] % length) * (2.0 * np.pi / length)
        return np.cos(angle), np.sin(angle)

    cos, sin = turn(k, half, GRID)
    to_kz = np.concatenate([cos, -sin], axis=1)
    cos, sin = turn(k, k, GRID)
    real = np.concatenate([cos, sin], axis=1).reshape(64, 4, 512)
    imag = np.concatenate([-sin, cos], axis=1).reshape(64, 4, 512)
    to_ky = np.stack([real, imag], axis=1).reshape(512, 512)
    cos, sin = turn(half, half, GRID // 2)
    to_kx = np.concatenate(
        [np.concatenate([cos, sin], axis=1), np.concatenate([-sin, cos], axis=1)], axis=0
    )
    angle = half[:, None] * (2.0 * np.pi / GRID) * np.ones((1, 128))
    upper = np.arange(128)[None, :] >= 64
    twist = np.stack([np.where(upper, np.cos(angle), 1.0), np.where(upper, np.sin(angle), 0.0)])
    signed = np.where(2 * k < GRID, k, k - GRID).astype(np.float64)
    spline = 36.0 / (4.0 + 2.0 * np.cos(k * (2.0 * np.pi / GRID))) ** 2
    spline[GRID // 2] = 0.0
    decay = spline * np.exp(-np.pi**2 * signed**2 / (EWALD**2 * GRID**2))
    lanes = np.arange(128)
    kx = half[:, None] + 128 * (lanes[None, :] // 64)
    of_x = np.stack([decay[kx] * (COULOMB / (np.pi * GRID)), signed[kx] ** 2])
    kz = 64 * np.arange(2)[:, None] + lanes[None, :] % 64
    of_z = np.stack([decay[kz], signed[kz] ** 2], axis=1)
    of_y = np.stack([decay, signed**2])
    return dict(
        to_kz=split_np(to_kz),
        to_ky=split_np(to_ky),
        to_kx=split_np(to_kx),
        twist=twist.astype(np.float32),
        of_x=of_x.astype(np.float32),
        of_y=of_y.astype(np.float32),
        of_z=of_z.astype(np.float32),
    )


def halves(value):
    high = value.astype(BF16)
    return high, (value - high.astype(F32)).astype(BF16)


def dot(a, b, dims=NN):
    return lax.dot_general(a, b, dims, preferred_element_type=F32)


def dot3(a, b):
    return dot(
        jnp.concatenate([a[0], a[1], a[0]], axis=1), jnp.concatenate([b[0], b[0], b[1]], axis=0)
    )


def spline_weights(t):
    rest = 1.0 - t
    square = t * t
    cube = square * t
    weights = (
        rest * rest * rest / 6.0,
        (3.0 * cube - 6.0 * square + 4.0) / 6.0,
        (-3.0 * cube + 3.0 * square + 3.0 * t + 1.0) / 6.0,
        cube / 6.0,
    )
    slopes = (-0.5 * rest * rest, 1.5 * square - 2.0 * t, -1.5 * square + t + 0.5, 0.5 * square)
    return weights, slopes


def place(values, lowest, rows):
    offset = lax.broadcasted_iota(jnp.int32, (rows, lowest.shape[1]), 0) - lowest
    out = jnp.where(offset == 3, values[3], 0.0)
    for i in (2, 1, 0):
        out = jnp.where(offset == i, values[i], out)
    return out


def block_index():
    return lax.axis_index("gx"), lax.axis_index("gy"), lax.axis_index("gz")


def plane_of(iz, iy):
    return lax.rem(iy, 2) * 4 + lax.div(iy, 2) * 2 + iz


def holder_of(plane):
    return {"gz": lax.rem(plane, 2), "gy": lax.rem(lax.div(plane, 2), 2) * 2 + lax.div(plane, 4)}


def spread_rows(counts_ref, charges_ref, frac_ref, base_ref, rows_x_ref, rows_y_ref, both_z_ref, strips_ref):
    ix, iy, iz = block_index()
    slot = lax.broadcasted_iota(jnp.int32, charges_ref.shape, 1)
    charge = jnp.where(slot < counts_ref[0, 0, 0], charges_ref[...], 0.0)
    wx, _ = spline_weights(frac_ref[0:1])
    wy, _ = spline_weights(frac_ref[1:2])
    wz, _ = spline_weights(frac_ref[2:3])
    wz = [w * charge for w in wz]
    low_x = base_ref[0:1] - ix * CX
    low_y = base_ref[1:2] - iy * CY
    low_z = base_ref[2:3] - iz * CZ
    rows_x = place(wx, low_x, 24)
    rows_x_ref[...] = rows_x
    rows_y = place(wy, low_y, CZ)
    rows_y_ref[...] = rows_y[:ROWS]
    high, low = halves(place(wz, low_z, CZ))
    both_z_ref[0:CZ] = high
    both_z_ref[CZ : 2 * CZ] = low
    rim_z = place(wz, low_z - (CZ - HALO), 8)
    rim_row = lax.broadcasted_iota(jnp.int32, (8, 1), 0)
    rim_z = jnp.where((rim_row >= 3) & (rim_row < 6), rim_z, 0.0)
    rims = halves(jnp.concatenate([rows_x[x : x + 1] * rim_z for x in range(20)], axis=0))
    y_high, y_low = halves(rows_y)
    total = dot(rims[0], jnp.concatenate([y_high, y_low], axis=0), NT)
    strips_ref[...] = total[:, :CZ] + total[:, CZ:] + dot(rims[1], y_high, NT)


def spread_group(group, rows_x_ref, rows_y_ref, both_z_ref, strips_ref, high_ref, low_ref, out_ref):
    for i in range(4):
        high, low = halves(rows_x_ref[pl.ds(group * 4 + i, 1), :] * rows_y_ref[...])
        high_ref[pl.ds(i * ROWS, ROWS), :] = high
        low_ref[pl.ds(i * ROWS, ROWS), :] = low
    total = dot(high_ref[...], both_z_ref[...], NT)
    total = total[:, :CZ] + total[:, CZ:] + dot(low_ref[...], both_z_ref[0:CZ], NT)
    for i in range(4):
        x = group * 4 + i
        strip = strips_ref[pl.ds(pl.multiple_of(x * 8, 8), 8), :]
        out_ref[x, 0:64, :] = total[i * ROWS : i * ROWS + 64]
        out_ref[x, 64:72, :] = total[i * ROWS + 64 : i * ROWS + 72] + strip


def forward_kernel(data_ref, to_kz_ref, to_ky_ref, out_ref):
    lane = lax.broadcasted_iota(jnp.int32, (1, 128), 1)
    row = lax.broadcasted_iota(jnp.int32, (8, 128), 0)
    lower = lane < 64
    parts = []
    for x in range(2):
        planes = []
        for iz in range(2):
            pieces = []
            for iy in range(4):
                rim = jnp.where(row < HALO, data_ref[iz * 4 + (iy + 3) % 4, x, 64:72, :], 0.0)
                pieces.append(data_ref[iz * 4 + iy, x, 0:8, :] + rim)
                pieces.append(data_ref[iz * 4 + iy, x, 8:64, :])
            planes.append(jnp.concatenate(pieces, axis=0))
        rims = []
        for iz in range(2):
            tiles = [data_ref[iz * 4 + iy, x, 64:72, :] for iy in range(4)]
            turned = [pltpu.roll(tiles[1], 64, 1), pltpu.roll(tiles[3], 64, 1)]
            first = tiles[0] + jnp.where(lower, turned[1], turned[0])
            second = tiles[2] + jnp.where(lower, turned[0], turned[1])
            rims.append(jnp.concatenate([first, second], axis=1))
        rims = jnp.concatenate(rims + [jnp.zeros((112, 256), F32)], axis=0).T
        planes[1] = planes[1] + jnp.where(lane < HALO, pltpu.roll(rims, 125, 1), 0.0)
        planes[0] = planes[0] + jnp.where(lane < HALO, pltpu.roll(rims, 117, 1), 0.0)
        plane = jnp.concatenate(planes, axis=1)
        parts.append(dot3(halves(plane), (to_kz_ref[0], to_kz_ref[1])))
    rows = []
    for c in range(2):
        zero, one = (p[:, c * 128 : (c + 1) * 128] for p in parts)
        first = jnp.where(lower, zero, pltpu.roll(one, 64, 1))
        second = jnp.where(lower, pltpu.roll(zero, 64, 1), one)
        rows.append(jnp.concatenate([first, second], axis=1))
    both = jnp.concatenate(rows, axis=0)
    out = dot3((to_ky_ref[0], to_ky_ref[1]), halves(both))
    out_ref[0:64] = out[:, :128].reshape(64, 8, 128)
    out_ref[64:128] = out[:, 128:].reshape(64, 8, 128)


def middle_kernel(data_ref, to_kx_ref, from_kx_ref, twist_ref, of_x_ref, of_z_ref, of_y_ref, out_ref):
    ix, iy, iz = block_index()
    mine = ix * COLUMN + plane_of(iz, iy)
    half, group = mine // 64, mine % 64
    lane = lax.broadcasted_iota(jnp.int32, (1, 128), 1)
    sign = jnp.where(lane < 64, 1.0, -1.0)
    both = jnp.concatenate(
        [
            jnp.concatenate([data_ref[:, c * 4 + i, :] for i in range(4)], axis=1)
            for c in range(2)
        ],
        axis=0,
    )
    out = dot3((to_kx_ref[0], to_kx_ref[1]), halves(both))
    cos, sin = twist_ref[0], twist_ref[1]
    of_z = of_z_ref[half]
    scale_xz = of_x_ref[0] * of_z[0:1]
    square_xz = of_x_ref[1] + of_z[1:2]
    reals, imags = [], []
    for i in range(4):
        real = out[:128, i * 128 : (i + 1) * 128]
        imag = out[128:, i * 128 : (i + 1) * 128]
        real, imag = real * cos + imag * sin, imag * cos - real * sin
        real = real * sign + pltpu.roll(real, 64, 1)
        imag = imag * sign + pltpu.roll(imag, 64, 1)
        ky = group * 4 + i
        square = square_xz + of_y_ref[1, ky]
        green = jnp.where(square > 0.0, scale_xz * of_y_ref[0, ky] / jnp.maximum(square, 1.0), 0.0)
        real, imag = real * green, imag * green
        real = real * sign + pltpu.roll(real, 64, 1)
        imag = imag * sign + pltpu.roll(imag, 64, 1)
        real, imag = real * cos - imag * sin, imag * cos + real * sin
        reals.append(real)
        imags.append(imag)
    both = jnp.concatenate(
        [jnp.concatenate(reals, axis=1), jnp.concatenate(imags, axis=1)], axis=0
    )
    out = dot3((from_kx_ref[0], from_kx_ref[1]), halves(both))
    for c in range(2):
        for i in range(4):
            out_ref[:, c * 4 + i, :] = out[c * 128 : (c + 1) * 128, i * 128 : (i + 1) * 128]


def backward_kernel(data_ref, from_ky_ref, from_kz_ref, out_ref):
    lane = lax.broadcasted_iota(jnp.int32, (1, 128), 1)
    row = lax.broadcasted_iota(jnp.int32, (8, 128), 0)
    lower = lane < 64
    both = jnp.concatenate(
        [data_ref[0:64].reshape(512, 128), data_ref[64:128].reshape(512, 128)], axis=1
    )
    out = dot3((from_ky_ref[0], from_ky_ref[1]), halves(both))
    tiles = [[], []]
    for c in range(2):
        first, second = out[c * 256 : (c + 1) * 256, :128], out[c * 256 : (c + 1) * 256, 128:]
        tiles[0].append(jnp.where(lower, first, pltpu.roll(second, 64, 1)))
        tiles[1].append(jnp.where(lower, pltpu.roll(first, 64, 1), second))
    for x in range(2):
        plane = dot3(
            halves(jnp.concatenate(tiles[x], axis=1)), (from_kz_ref[0], from_kz_ref[1])
        )
        turned = [plane[:, h * 128 : (h + 1) * 128].T[:8] for h in range(2)]
        for iz in range(2):
            near = plane[:, iz * 128 : (iz + 1) * 128]
            strips = (turned[1 - iz][:, :128], turned[1 - iz][:, 128:])
            rolled = [pltpu.roll(s, 64, 1) for s in strips]
            for iy in range(4):
                after = (iy + 1) % 4
                t = iy // 2
                if iy % 2 == 0:
                    strip = strips[t]
                else:
                    strip = jnp.where(lower, rolled[t], rolled[1 - t])
                out_ref[iz * 4 + iy, x, 0:64, :] = near[iy * 64 : iy * 64 + 64]
                out_ref[iz * 4 + iy, x, 64:72, :] = jnp.where(
                    row < HALO, near[after * 64 : after * 64 + 8], pltpu.roll(strip, HALO, 0)
                )


WIDTH = 128


def gather_rows(frac_ref, base_ref, grads_x_ref, grads_y_ref, fold_z_ref, fold_y_ref, strip_ref, rows_y_ref):
    ix, iy, iz = block_index()

    def folded(rows, grads):
        high, low = halves(jnp.concatenate([rows, grads], axis=1))
        return jnp.concatenate([high, high, low], axis=0)

    def step(c, carry):
        at = pl.ds(pl.multiple_of(c * WIDTH, WIDTH), WIDTH)
        _, sx = spline_weights(frac_ref[0:1, at])
        _, sy = spline_weights(frac_ref[1:2, at])
        wz, sz = spline_weights(frac_ref[2:3, at])
        low_x = base_ref[0:1, at] - ix * CX
        low_y = base_ref[1:2, at] - iy * CY
        low_z = base_ref[2:3, at] - iz * CZ
        grads_x_ref[:, at] = place(sx, low_x, 24)
        grads_y = place(sy, low_y, ROWS)
        grads_y_ref[:, at] = grads_y
        rim_row = lax.broadcasted_iota(jnp.int32, (8, 1), 0)
        inside = (rim_row >= 3) & (rim_row < 6)
        rim_low = low_z - (CZ - HALO)
        strip_ref[0:8, at] = jnp.where(inside, place(wz, rim_low, 8), 0.0)
        strip_ref[8:16, at] = jnp.where(inside, place(sz, rim_low, 8), 0.0)
        fold_z_ref[c] = folded(place(wz, low_z, CZ), place(sz, low_z, CZ))
        pad = jnp.zeros((CZ - ROWS, WIDTH), F32)
        fold_y_ref[c] = folded(
            jnp.concatenate([rows_y_ref[:, at], pad], axis=0), jnp.concatenate([grads_y, pad], axis=0)
        )
        return carry

    lax.fori_loop(0, frac_ref.shape[1] // WIDTH, step, 0)


def gather_kernel(
    counts_ref, charges_ref, rows_x_ref, grads_x_ref, rows_y_ref, grads_y_ref, fold_z_ref, fold_y_ref,
    strip_ref, data_ref, out_ref, pot_ref, rim_ref,
):
    def spread_out(ref, at, value):
        high, low = halves(value)
        ref[at, 0:128] = high
        ref[at, 128:256] = low
        ref[at, 256:384] = high

    for x in range(SPAN):
        spread_out(pot_ref, pl.ds(x * ROWS, ROWS), data_ref[x])
    spread_out(
        rim_ref, slice(None), jnp.concatenate([data_ref[x, 64:72, :] for x in range(SPAN)], axis=0)
    )

    def step(c, carry):
        at = pl.ds(pl.multiple_of(c * WIDTH, WIDTH), WIDTH)
        slot = lax.broadcasted_iota(jnp.int32, (1, WIDTH), 1) + c * WIDTH
        charge = jnp.where(slot < counts_ref[0, 0, 0], charges_ref[:, at], 0.0)
        rows_x, grads_x = rows_x_ref[:, at], grads_x_ref[:, at]
        rows_y, grads_y = rows_y_ref[:, at], grads_y_ref[:, at]
        rim_rows, rim_grads = strip_ref[0:8, at], strip_ref[8:16, at]
        rims = dot(rim_ref[...], fold_y_ref[c])
        main = dot(pot_ref[...], fold_z_ref[c])
        force_x = jnp.zeros((8, WIDTH), F32)
        force_y = jnp.zeros((8, WIDTH), F32)
        force_z = jnp.zeros((8, WIDTH), F32)
        for x in range(SPAN):
            rim_plain = rims[x * 8 : x * 8 + 8, :WIDTH]
            rim_sloped = rims[x * 8 : x * 8 + 8, WIDTH:]
            sum_x = rim_rows * rim_plain
            sum_y = rim_rows * rim_sloped
            sum_z = rim_grads * rim_plain
            for y in range(ROWS // 8):
                low = x * ROWS + y * 8
                plain, sloped = main[low : low + 8, :WIDTH], main[low : low + 8, WIDTH:]
                near = rows_y[y * 8 : y * 8 + 8]
                sum_x += plain * near
                sum_y += plain * grads_y[y * 8 : y * 8 + 8]
                sum_z += sloped * near
            force_x += grads_x[x : x + 1] * sum_x
            force_y += rows_x[x : x + 1] * sum_y
            force_z += rows_x[x : x + 1] * sum_z
        total = [jnp.sum(f, axis=0, keepdims=True) for f in (force_x, force_y, force_z)]
        out_ref[:, at] = -charge * jnp.concatenate(total, axis=0)
        return carry

    lax.fori_loop(0, charges_ref.shape[1] // WIDTH, step, 0)


def turn_tables(to_kz_ref, to_ky_ref, to_kx_ref, from_kz_ref, from_ky_ref, from_kx_ref):
    row = lax.broadcasted_iota(jnp.int32, (GRID, 1), 0)
    twice = jnp.where(lax.rem(row, GRID // 2) == 0, 1.0, 2.0)
    for part in range(2):
        from_kz_ref[part] = (to_kz_ref[part].T.astype(F32) * twice).astype(BF16)
        from_ky_ref[part] = to_ky_ref[part].T
        from_kx_ref[part] = to_kx_ref[part].T


MESH = pl.DeviceIdType.MESH
INPUTS = ("charges", "fractions", "base_cells")
SMALL = ("counts", "of_y")
NAMES = ("to_kz", "to_ky", "to_kx", "twist", "of_x", "of_z")


FAR = sorted(
    ((a, b) for a in range(4) for b in range(4) if a or b),
    key=lambda o: -(min(o[0], 4 - o[0]) + min(o[1], 4 - o[1])),
)


def drain(ref, sem):
    pltpu.make_async_copy(ref, ref, sem).wait()


def fused_kernel(*refs):
    total = len(INPUTS) + len(SMALL) + len(NAMES)
    hbm, out_ref, refs = refs[:total], refs[total], refs[total + 1 :]
    local, refs = refs[:total], refs[total:]
    (rows_x_ref, rows_y_ref, both_z_ref, strips_ref, high_ref, low_ref, grid_ref, rim_in_ref, planes_ref,
     send_ref, modes_ref, send2_ref, modes2_ref, blocks_ref, near_ref, pot_ref, rim_ref,
     grads_x_ref, grads_y_ref, fold_z_ref, fold_y_ref, strip_ref, from_kz_ref, from_ky_ref, from_kx_ref,
     load_sem, rim_send, rim_recv, a_send, a_recv, c_send, c_recv, d_send, d_recv,
     b_send, b_recv, e_send, e_recv) = refs
    loads = [pltpu.make_async_copy(h, v, load_sem.at[i]) for i, (h, v) in enumerate(zip(hbm, local))]
    first = len(INPUTS) + len(SMALL)
    for load in loads[:first]:
        load.start()
    charges_ref, frac_ref, base_ref, counts_ref, of_y_ref = local[:first]
    t = dict(zip(NAMES, local[first:]))
    ix, iy, iz = block_index()
    count_x = lax.axis_size("gx")
    block = iz * 4 + iy
    plane = plane_of(iz, iy)
    mine = ix * COLUMN + plane
    after = {"gx": lax.rem(ix + 1, count_x)}
    before = {"gx": lax.rem(ix + count_x - 1, count_x)}
    core, height = lax.rem(iy, 2), lax.div(iy, 2) * 2 + iz
    others = []
    for up, flip in ((2, 0), (2, 1), (1, 0), (1, 1), (3, 0), (3, 1), (0, 1), (0, 0)):
        to = lax.rem(core + flip, 2) * 4 + lax.rem(height + up, 4)
        others.append((to, holder_of(to)))

    barrier = pltpu.get_barrier_semaphore()

    def everyone(action):
        def row(_, steps):
            along, across = lax.rem(steps, 4), lax.rem(lax.div(steps, 4), 4)
            to_x = lax.rem(lax.div(ix, 4) + along, 4) * 4 + lax.rem(lax.rem(ix, 4) + across, 4)
            for to, where in others:
                action(to_x * COLUMN + to, {"gx": to_x, **where})
            return lax.div(steps, 16)

        for part in (FAR[:7], FAR[7:]):
            steps = sum((a + 4 * b) << (4 * i) for i, (a, b) in enumerate(part))
            lax.fori_loop(0, len(part), row, jnp.int32(steps))
        for to, where in others[:-1]:
            action(ix * COLUMN + to, where)

    def greet(to, where):
        pl.semaphore_signal(barrier, inc=1, device_id=where, device_id_type=MESH)

    with jax.named_scope("greet"):
        everyone(greet)
    with jax.named_scope("load"):
        for load in loads[:first]:
            load.wait()
        for load in loads[first:]:
            load.start()
    spread = (rows_x_ref, rows_y_ref, both_z_ref, strips_ref)
    with jax.named_scope("rows"):
        spread_rows(counts_ref, charges_ref, frac_ref, base_ref, *spread)
    with jax.named_scope("spread4"):
        spread_group(4, *spread, high_ref, low_ref, grid_ref)
    with jax.named_scope("barwait"):
        pl.semaphore_wait(barrier, 127)
    rim = pltpu.make_async_remote_copy(
        src_ref=grid_ref.at[pl.ds(CX, HALO)], dst_ref=rim_in_ref, send_sem=rim_send, recv_sem=rim_recv,
        device_id=after, device_id_type=MESH,
    )
    rim.start()

    def give(to):
        @pl.when(to != plane)
        def _():
            pltpu.make_async_remote_copy(
                src_ref=grid_ref.at[pl.ds(2 * to, 2)], dst_ref=planes_ref.at[block],
                send_sem=a_send.at[to], recv_sem=a_recv.at[block],
                device_id=holder_of(to), device_id_type=MESH,
            ).start()

    def some(i, carry):
        group = 1 + lax.rem(i + plane, 3)
        spread_group(group, *spread, high_ref, low_ref, grid_ref)
        give(2 * group)
        give(2 * group + 1)
        return carry

    with jax.named_scope("spread123"):
        lax.fori_loop(0, 3, some, 0)
    with jax.named_scope("spread0"):
        spread_group(0, *spread, high_ref, low_ref, grid_ref)
    with jax.named_scope("rimwait"):
        rim.wait_recv()
    grid_ref[0:HALO] += rim_in_ref[...]
    give(0)
    give(1)
    planes_ref[pl.ds(block, 1)] = grid_ref[pl.ds(2 * plane, 2)].reshape(1, 2, ROWS, CZ)
    with jax.named_scope("await"):
        for load in loads[first:]:
            load.wait()
        for b in range(COLUMN):
            pl.when(b != block)(functools.partial(drain, planes_ref.at[b], a_recv.at[b]))

    def spray(source, target, send_sem, recv_sem, meanwhile):
        def one(to, where):
            pltpu.make_async_remote_copy(
                src_ref=source.at[to], dst_ref=target.at[mine], send_sem=send_sem, recv_sem=recv_sem,
                device_id=where, device_id_type=MESH,
            ).start()

        with jax.named_scope("csend"):
            everyone(one)
        target[pl.ds(mine, 1)] = source[pl.ds(mine, 1)]
        meanwhile()
        with jax.named_scope("cwait"):
            drain(target.at[pl.ds(0, 127)], recv_sem)

    with jax.named_scope("forward"):
        forward_kernel(planes_ref, t["to_kz"], t["to_ky"], send_ref)

    def prepare_back():
        with jax.named_scope("turn"):
            turn_tables(t["to_kz"], t["to_ky"], t["to_kx"], from_kz_ref, from_ky_ref, from_kx_ref)

    def prepare_gather():
        with jax.named_scope("gather_rows"):
            gather_rows(
                frac_ref, base_ref, grads_x_ref, grads_y_ref, fold_z_ref, fold_y_ref, strip_ref, rows_y_ref
            )

    spray(send_ref, modes_ref, c_send, c_recv, prepare_back)
    with jax.named_scope("middle"):
        middle_kernel(modes_ref, t["to_kx"], from_kx_ref, t["twist"], t["of_x"], t["of_z"], of_y_ref, send2_ref)
    spray(send2_ref, modes2_ref, d_send, d_recv, prepare_gather)
    with jax.named_scope("backward"):
        backward_kernel(modes2_ref, from_ky_ref, from_kz_ref, blocks_ref)

    for to, where in others[:-1]:
        to_block = where["gz"] * 4 + where["gy"]
        pltpu.make_async_remote_copy(
            src_ref=blocks_ref.at[to_block], dst_ref=near_ref.at[pl.ds(2 * plane, 2)],
            send_sem=b_send.at[to], recv_sem=b_recv.at[plane], device_id=where, device_id_type=MESH,
        ).start()
    near_ref[pl.ds(2 * plane, 2)] = blocks_ref[pl.ds(block, 1)].reshape(2, ROWS, CZ)
    rim_back = pltpu.make_async_remote_copy(
        src_ref=near_ref.at[pl.ds(0, HALO)], dst_ref=near_ref.at[pl.ds(CX, HALO)],
        send_sem=e_send, recv_sem=e_recv, device_id=before, device_id_type=MESH,
    )
    with jax.named_scope("bwait"):
        for b in range(COLUMN):
            pl.when(b != plane)(functools.partial(drain, near_ref.at[pl.ds(2 * b, 2)], b_recv.at[b]))
            if b == 1:
                rim_back.start()
    with jax.named_scope("sendwait"):
        rim.wait_send()
        rim_back.wait_send()
        for o in range(COLUMN):
            @pl.when(o != plane)
            def _():
                drain(grid_ref.at[pl.ds(2 * o, 2)], a_send.at[o])
                drain(blocks_ref.at[o], b_send.at[o])

        drain(send_ref.at[pl.ds(0, 127)], c_send)
        drain(send2_ref.at[pl.ds(0, 127)], d_send)
    with jax.named_scope("ewait"):
        rim_back.wait_recv()
    with jax.named_scope("gather"):
        gather_kernel(
            counts_ref, charges_ref, rows_x_ref, grads_x_ref, rows_y_ref, grads_y_ref, fold_z_ref,
            fold_y_ref, strip_ref, near_ref, out_ref, pot_ref, rim_ref,
        )


def per_device(charges, fractions, base_cells, counts):
    t = {name: jnp.asarray(value) for name, value in tables().items()}
    arrays = [charges.reshape(1, -1), fractions, base_cells, counts, t["of_y"]]
    arrays += [t[name] for name in NAMES]
    small = len(INPUTS) + len(SMALL)
    atoms = fractions.shape[1]
    dma = pltpu.SemaphoreType.DMA
    scratch = [
        (pltpu.SMEM if len(INPUTS) <= i < small else pltpu.VMEM)(a.shape, a.dtype)
        for i, a in enumerate(arrays)
    ]
    scratch += [
        pltpu.VMEM((24, atoms), F32),
        pltpu.VMEM((ROWS, atoms), F32),
        pltpu.VMEM((2 * CZ, atoms), BF16),
        pltpu.VMEM((160, CZ), F32),
        pltpu.VMEM((4 * ROWS, atoms), BF16),
        pltpu.VMEM((4 * ROWS, atoms), BF16),
        pltpu.VMEM((20, ROWS, CZ), F32),
        pltpu.VMEM((HALO, ROWS, CZ), F32),
        pltpu.VMEM((COLUMN, 2, ROWS, CZ), F32),
        pltpu.VMEM((128, 8, 128), F32),
        pltpu.VMEM((128, 8, 128), F32),
        pltpu.VMEM((128, 8, 128), F32),
        pltpu.VMEM((128, 8, 128), F32),
        pltpu.VMEM((COLUMN, 2, ROWS, CZ), F32),
        pltpu.VMEM((SPAN, ROWS, CZ), F32),
        pltpu.VMEM((SPAN * ROWS, 384), BF16),
        pltpu.VMEM((SPAN * 8, 384), BF16),
        pltpu.VMEM((24, atoms), F32),
        pltpu.VMEM((ROWS, atoms), F32),
        pltpu.VMEM((atoms // WIDTH, 384, 2 * WIDTH), BF16),
        pltpu.VMEM((atoms // WIDTH, 384, 2 * WIDTH), BF16),
        pltpu.VMEM((16, atoms), F32),
        pltpu.VMEM(t["to_kz"].shape, BF16),
        pltpu.VMEM(t["to_ky"].shape, BF16),
        pltpu.VMEM(t["to_kx"].shape, BF16),
        dma((len(arrays),)), dma, dma, dma((COLUMN,)), dma((COLUMN,)), dma, dma, dma, dma,
        dma((COLUMN,)), dma((COLUMN,)), dma, dma,
    ]
    return pl.pallas_call(
        fused_kernel,
        out_shape=jax.ShapeDtypeStruct(fractions.shape, F32),
        in_specs=[pl.BlockSpec(memory_space=pltpu.HBM)] * len(arrays),
        out_specs=pl.BlockSpec(memory_space=pltpu.VMEM),
        scratch_shapes=scratch,
        compiler_params=pltpu.CompilerParams(
            collective_id=0, has_side_effects=True, vmem_limit_bytes=62 << 20
        ),
    )(*arrays)


def solution(mesh):
    split = ("gz", "gy", "gx")
    return jax.shard_map(
        per_device,
        mesh=mesh,
        in_specs=(P(split), P(None, split), P(None, split), P("gz", "gy", "gx")),
        out_specs=P(None, split),
        check_vma=False,
    )
```

```python
import functools

import jax
import jax.numpy as jnp
import numpy as np
from jax import lax
from jax.experimental import pallas as pl
from jax.experimental.pallas import tpu as pltpu
from jax.sharding import PartitionSpec as P

GRID = 256
ORDER = 4
HALO = ORDER - 1
COULOMB = 332.0636
EWALD = 0.7
CX, CY, CZ = 16, 64, 128
ROWS = 72
SPAN = CX + HALO
COLUMN = 8
F32 = jnp.float32
BF16 = jnp.bfloat16
NN = (((1,), (0,)), ((), ()))
NT = (((1,), (1,)), ((), ()))


def split_np(a):
    a = np.asarray(a, np.float32)
    high = a.astype(jnp.bfloat16)
    low = (a - high.astype(np.float32)).astype(jnp.bfloat16)
    return np.stack([high, low])


def tables():
    k = np.arange(GRID)
    half = np.arange(GRID // 2)

    def turn(first, second, length):
        angle = (first[:, None] * second[None, :] % length) * (2.0 * np.pi / length)
        return np.cos(angle), np.sin(angle)

    cos, sin = turn(k, half, GRID)
    to_kz = np.concatenate([cos, -sin], axis=1)
    cos, sin = turn(k, k, GRID)
    real = np.concatenate([cos, sin], axis=1).reshape(64, 2, 2, 512)
    imag = np.concatenate([-sin, cos], axis=1).reshape(64, 2, 2, 512)
    to_ky = np.stack([real, imag], axis=2).swapaxes(0, 1).reshape(512, 512)
    cos, sin = turn(half, half, GRID // 2)
    to_kx = np.concatenate(
        [np.concatenate([cos, sin], axis=1), np.concatenate([-sin, cos], axis=1)], axis=0
    )
    angle = half[:, None] * (2.0 * np.pi / GRID) * np.ones((1, 128))
    upper = np.arange(128)[None, :] >= 64
    twist = np.stack([np.where(upper, np.cos(angle), 1.0), np.where(upper, np.sin(angle), 0.0)])
    signed = np.where(2 * k < GRID, k, k - GRID).astype(np.float64)
    spline = 36.0 / (4.0 + 2.0 * np.cos(k * (2.0 * np.pi / GRID))) ** 2
    spline[GRID // 2] = 0.0
    decay = spline * np.exp(-np.pi**2 * signed**2 / (EWALD**2 * GRID**2))
    lanes = np.arange(128)
    kx = half[:, None] + 128 * (lanes[None, :] // 64)
    of_x = np.stack([decay[kx] * (COULOMB / (np.pi * GRID)), signed[kx] ** 2])
    kz = 64 * np.arange(2)[:, None] + lanes[None, :] % 64
    of_z = np.stack([decay[kz], signed[kz] ** 2], axis=1)
    of_y = np.stack([decay, signed**2])
    return dict(
        to_kz=split_np(to_kz),
        to_ky=split_np(to_ky),
        to_kx=split_np(to_kx),
        twist=twist.astype(np.float32),
        of_x=of_x.astype(np.float32),
        of_y=of_y.astype(np.float32),
        of_z=of_z.astype(np.float32),
    )


def halves(value):
    high = value.astype(BF16)
    return high, (value - high.astype(F32)).astype(BF16)


def dot(a, b, dims=NN):
    return lax.dot_general(a, b, dims, preferred_element_type=F32)


def dot3(a, b):
    return dot(
        jnp.concatenate([a[0], a[1], a[0]], axis=1), jnp.concatenate([b[0], b[0], b[1]], axis=0)
    )


def part_of(ref, *at):
    return ref[(0, *at)], ref[(1, *at)]


def spline_weights(t):
    rest = 1.0 - t
    square = t * t
    cube = square * t
    weights = (
        rest * rest * rest / 6.0,
        (3.0 * cube - 6.0 * square + 4.0) / 6.0,
        (-3.0 * cube + 3.0 * square + 3.0 * t + 1.0) / 6.0,
        cube / 6.0,
    )
    slopes = (-0.5 * rest * rest, 1.5 * square - 2.0 * t, -1.5 * square + t + 0.5, 0.5 * square)
    return weights, slopes


def place(values, lowest, rows):
    offset = lax.broadcasted_iota(jnp.int32, (rows, lowest.shape[1]), 0) - lowest
    out = jnp.where(offset == 3, values[3], 0.0)
    for i in (2, 1, 0):
        out = jnp.where(offset == i, values[i], out)
    return out


def block_index():
    return lax.axis_index("gx"), lax.axis_index("gy"), lax.axis_index("gz")


def plane_of(iz, iy):
    return lax.rem(iy, 2) * 4 + lax.div(iy, 2) * 2 + iz


def holder_of(plane):
    return {"gz": lax.rem(plane, 2), "gy": lax.rem(lax.div(plane, 2), 2) * 2 + lax.div(plane, 4)}


def spread_rows(counts_ref, charges_ref, frac_ref, base_ref, rows_x_ref, rows_y_ref, both_z_ref, strips_ref):
    ix, iy, iz = block_index()
    slot = lax.broadcasted_iota(jnp.int32, charges_ref.shape, 1)
    charge = jnp.where(slot < counts_ref[0, 0, 0], charges_ref[...], 0.0)
    wx, _ = spline_weights(frac_ref[0:1])
    wy, _ = spline_weights(frac_ref[1:2])
    wz, _ = spline_weights(frac_ref[2:3])
    wz = [w * charge for w in wz]
    low_x = base_ref[0:1] - ix * CX
    low_y = base_ref[1:2] - iy * CY
    low_z = base_ref[2:3] - iz * CZ
    rows_x = place(wx, low_x, 24)
    rows_x_ref[...] = rows_x
    rows_y = place(wy, low_y, ROWS)
    rows_y_ref[...] = rows_y
    high, low = halves(place(wz, low_z, CZ))
    both_z_ref[0:CZ] = high
    both_z_ref[CZ : 2 * CZ] = low
    rim_z = place(wz, low_z - (CZ - HALO), 8)
    rim_row = lax.broadcasted_iota(jnp.int32, (8, 1), 0)
    rim_z = jnp.where((rim_row >= 3) & (rim_row < 6), rim_z, 0.0)
    rims = halves(jnp.concatenate([rows_x[x : x + 1] * rim_z for x in range(20)], axis=0))
    rows_y = jnp.concatenate([rows_y, jnp.zeros((CZ - ROWS, rows_y.shape[1]), F32)], axis=0)
    y_high, y_low = halves(rows_y)
    total = dot(rims[0], jnp.concatenate([y_high, y_low], axis=0), NT)
    strips_ref[...] = total[:, :CZ] + total[:, CZ:] + dot(rims[1], y_high, NT)


def spread_group(group, rows_x_ref, rows_y_ref, both_z_ref, strips_ref, high_ref, low_ref, out_ref):
    for i in range(4):
        high, low = halves(rows_x_ref[pl.ds(group * 4 + i, 1), :] * rows_y_ref[...])
        high_ref[pl.ds(i * ROWS, ROWS), :] = high
        low_ref[pl.ds(i * ROWS, ROWS), :] = low
    total = dot(high_ref[...], both_z_ref[...], NT)
    total = total[:, :CZ] + total[:, CZ:] + dot(low_ref[...], both_z_ref[0:CZ], NT)
    for i in range(4):
        x = group * 4 + i
        strip = strips_ref[pl.ds(pl.multiple_of(x * 8, 8), 8), :]
        out_ref[x, 0:64, :] = total[i * ROWS : i * ROWS + 64]
        out_ref[x, 64:72, :] = total[i * ROWS + 64 : i * ROWS + 72] + strip


def forward_kernel(data_ref, to_kz_ref, to_ky_ref, out_ref, leave):
    lane = lax.broadcasted_iota(jnp.int32, (1, 128), 1)
    row = lax.broadcasted_iota(jnp.int32, (8, 128), 0)
    lower = lane < 64
    parts = []
    for x in range(2):
        planes = []
        for iz in range(2):
            pieces = []
            for iy in range(4):
                rim = jnp.where(row < HALO, data_ref[iz * 4 + (iy + 3) % 4, x, 64:72, :], 0.0)
                pieces.append(data_ref[iz * 4 + iy, x, 0:8, :] + rim)
                pieces.append(data_ref[iz * 4 + iy, x, 8:64, :])
            planes.append(jnp.concatenate(pieces, axis=0))
        rims = []
        for iz in range(2):
            tiles = [data_ref[iz * 4 + iy, x, 64:72, :] for iy in range(4)]
            turned = [pltpu.roll(tiles[1], 64, 1), pltpu.roll(tiles[3], 64, 1)]
            first = tiles[0] + jnp.where(lower, turned[1], turned[0])
            second = tiles[2] + jnp.where(lower, turned[0], turned[1])
            rims.append(jnp.concatenate([first, second], axis=1))
        rims = jnp.concatenate(rims + [jnp.zeros((112, 256), F32)], axis=0).T
        planes[1] = planes[1] + jnp.where(lane < HALO, pltpu.roll(rims, 125, 1), 0.0)
        planes[0] = planes[0] + jnp.where(lane < HALO, pltpu.roll(rims, 117, 1), 0.0)
        plane = jnp.concatenate(planes, axis=1)
        parts.append(dot3(halves(plane), (to_kz_ref[0], to_kz_ref[1])))
    rows = []
    for c in range(2):
        zero, one = (p[:, c * 128 : (c + 1) * 128] for p in parts)
        first = jnp.where(lower, zero, pltpu.roll(one, 64, 1))
        second = jnp.where(lower, pltpu.roll(zero, 64, 1), one)
        rows.append(jnp.concatenate([first, second], axis=1))
    both = halves(jnp.concatenate(rows, axis=0))
    for half in range(2):
        out = dot3(part_of(to_ky_ref, slice(half * 256, half * 256 + 256)), both)
        out_ref[half, 0:64] = out[:, :128].reshape(64, 4, 128)
        out_ref[half, 64:128] = out[:, 128:].reshape(64, 4, 128)
        leave(half)


def middle_kernel(part, data_ref, to_kx_ref, from_kx_ref, twist_ref, of_x_ref, of_z_ref, of_y_ref, out_ref):
    ix, iy, iz = block_index()
    mine = ix * COLUMN + plane_of(iz, iy)
    half, group = mine // 64, mine % 64
    lane = lax.broadcasted_iota(jnp.int32, (1, 128), 1)
    sign = jnp.where(lane < 64, 1.0, -1.0)
    both = jnp.concatenate(
        [
            jnp.concatenate([data_ref[part, :, c * 2 + i, :] for i in range(2)], axis=1)
            for c in range(2)
        ],
        axis=0,
    )
    out = dot3(part_of(to_kx_ref), halves(both))
    cos, sin = twist_ref[0], twist_ref[1]
    of_z = of_z_ref[half]
    scale_xz = of_x_ref[0] * of_z[0:1]
    square_xz = of_x_ref[1] + of_z[1:2]
    reals, imags = [], []
    for i in range(2):
        real = out[:128, i * 128 : (i + 1) * 128]
        imag = out[128:, i * 128 : (i + 1) * 128]
        real, imag = real * cos + imag * sin, imag * cos - real * sin
        real = real * sign + pltpu.roll(real, 64, 1)
        imag = imag * sign + pltpu.roll(imag, 64, 1)
        ky = group * 4 + part * 2 + i
        square = square_xz + of_y_ref[1, ky]
        green = jnp.where(square > 0.0, scale_xz * of_y_ref[0, ky] / jnp.maximum(square, 1.0), 0.0)
        real, imag = real * green, imag * green
        real = real * sign + pltpu.roll(real, 64, 1)
        imag = imag * sign + pltpu.roll(imag, 64, 1)
        real, imag = real * cos - imag * sin, imag * cos + real * sin
        reals.append(real)
        imags.append(imag)
    both = jnp.concatenate(
        [jnp.concatenate(reals, axis=1), jnp.concatenate(imags, axis=1)], axis=0
    )
    out = dot3(part_of(from_kx_ref), halves(both))
    for c in range(2):
        for i in range(2):
            out_ref[part, :, c * 2 + i, :] = out[c * 128 : (c + 1) * 128, i * 128 : (i + 1) * 128]


def backward_kernel(data_ref, from_ky_ref, from_kz_ref, out_ref, arrive):
    lane = lax.broadcasted_iota(jnp.int32, (1, 128), 1)
    row = lax.broadcasted_iota(jnp.int32, (8, 128), 0)
    lower = lane < 64
    out = 0.0
    for half in range(2):
        arrive(half)
        both = jnp.concatenate(
            [data_ref[half, 0:64].reshape(256, 128), data_ref[half, 64:128].reshape(256, 128)], axis=1
        )
        out = out + dot3(
            part_of(from_ky_ref, slice(None), slice(half * 256, half * 256 + 256)), halves(both)
        )
    tiles = [[], []]
    for c in range(2):
        first, second = out[c * 256 : (c + 1) * 256, :128], out[c * 256 : (c + 1) * 256, 128:]
        tiles[0].append(jnp.where(lower, first, pltpu.roll(second, 64, 1)))
        tiles[1].append(jnp.where(lower, pltpu.roll(first, 64, 1), second))
    for x in range(2):
        plane = dot3(halves(jnp.concatenate(tiles[x], axis=1)), part_of(from_kz_ref))
        turned = [plane[:, h * 128 : (h + 1) * 128].T[:8] for h in range(2)]
        for iz in range(2):
            near = plane[:, iz * 128 : (iz + 1) * 128]
            strips = (turned[1 - iz][:, :128], turned[1 - iz][:, 128:])
            rolled = [pltpu.roll(s, 64, 1) for s in strips]
            for iy in range(4):
                after = (iy + 1) % 4
                t = iy // 2
                if iy % 2 == 0:
                    strip = strips[t]
                else:
                    strip = jnp.where(lower, rolled[t], rolled[1 - t])
                out_ref[iz * 4 + iy, x, 0:64, :] = near[iy * 64 : iy * 64 + 64]
                out_ref[iz * 4 + iy, x, 64:72, :] = jnp.where(
                    row < HALO, near[after * 64 : after * 64 + 8], pltpu.roll(strip, HALO, 0)
                )


WIDTH = 128
UNROLL = 4
ORDER_UP = ((0, 0), (0, 1), (1, 0), (1, 1), (3, 0), (3, 1), (2, 0), (2, 1))
EARLY = 6


def gather_rows(
    frac_ref, base_ref, rows_x_ref, both_x_ref, grads_y_ref, fold_z_ref, fold_y_ref, strip_ref, rows_y_ref
):
    ix, iy, iz = block_index()

    def folded(rows, grads):
        high, low = halves(jnp.concatenate([rows, grads], axis=1))
        return jnp.concatenate([high, high, low], axis=0)

    def step(c, carry):
        at = pl.ds(pl.multiple_of(c * WIDTH, WIDTH), WIDTH)
        _, sx = spline_weights(frac_ref[0:1, at])
        _, sy = spline_weights(frac_ref[1:2, at])
        wz, sz = spline_weights(frac_ref[2:3, at])
        low_x = base_ref[0:1, at] - ix * CX
        low_y = base_ref[1:2, at] - iy * CY
        low_z = base_ref[2:3, at] - iz * CZ
        both_x_ref[c, 0:24] = rows_x_ref[:, at]
        both_x_ref[c, 24:48] = place(sx, low_x, 24)
        grads_y = place(sy, low_y, ROWS)
        grads_y_ref[:, at] = grads_y
        rim_row = lax.broadcasted_iota(jnp.int32, (8, 1), 0)
        inside = (rim_row >= 3) & (rim_row < 6)
        rim_low = low_z - (CZ - HALO)
        strip_ref[0:8, at] = jnp.where(inside, place(wz, rim_low, 8), 0.0)
        strip_ref[8:16, at] = jnp.where(inside, place(sz, rim_low, 8), 0.0)
        fold_z_ref[c] = folded(place(wz, low_z, CZ), place(sz, low_z, CZ))
        pad = jnp.zeros((CZ - ROWS, WIDTH), F32)
        fold_y_ref[c] = folded(
            jnp.concatenate([rows_y_ref[:, at], pad], axis=0), jnp.concatenate([grads_y, pad], axis=0)
        )
        return carry

    lax.fori_loop(0, frac_ref.shape[1] // WIDTH, step, 0)


def stage(pot_ref, rim_ref, layers):
    for i, layer in enumerate(layers):
        high, low = halves(layer)
        at = pl.ds(i * ROWS, ROWS)
        pot_ref[at, 0:128] = high
        pot_ref[at, 128:256] = low
        pot_ref[at, 256:384] = high
        at = pl.ds(i * 8, 8)
        rim_ref[at, 0:128] = layer[64:72]
    count = len(layers) * 8
    high, low = halves(rim_ref[0:count, 0:128])
    return jnp.concatenate([high, low, high], axis=1)


def gather_part(first, last, cells, pot_ref, strips_ref, both_x_ref, rows_y_ref, grads_y_ref,
                fold_z_ref, fold_y_ref, strip_ref, finish):
    def one(c):
        at = pl.ds(pl.multiple_of(c * WIDTH, WIDTH), WIDTH)
        rows_y, grads_y = rows_y_ref[:, at], grads_y_ref[:, at]
        rim_rows, rim_grads = strip_ref[0:8, at], strip_ref[8:16, at]
        rims = dot(strips_ref[0 : len(cells) * 8], fold_y_ref[c])
        main = dot(pot_ref[0 : len(cells) * ROWS], fold_z_ref[c])
        force_x = jnp.zeros((8, WIDTH), F32)
        force_y = jnp.zeros((8, WIDTH), F32)
        force_z = jnp.zeros((8, WIDTH), F32)
        for i, x in enumerate(cells):
            rim_plain = rims[i * 8 : i * 8 + 8, :WIDTH]
            rim_sloped = rims[i * 8 : i * 8 + 8, WIDTH:]
            sum_x = rim_rows * rim_plain
            sum_y = rim_rows * rim_sloped
            sum_z = rim_grads * rim_plain
            for y in range(ROWS // 8):
                low = i * ROWS + y * 8
                plain, sloped = main[low : low + 8, :WIDTH], main[low : low + 8, WIDTH:]
                near = rows_y[y * 8 : y * 8 + 8]
                sum_x += plain * near
                sum_y += plain * grads_y[y * 8 : y * 8 + 8]
                sum_z += sloped * near
            rows_x, grads_x = both_x_ref[c, pl.ds(x, 1), :], both_x_ref[c, pl.ds(x + 24, 1), :]
            force_x += grads_x * sum_x
            force_y += rows_x * sum_y
            force_z += rows_x * sum_z
        finish(c, at, force_x, force_y, force_z)

    def step(i, carry):
        for u in range(UNROLL):
            one(i * UNROLL + u)
        return carry

    lax.fori_loop(first // UNROLL, last // UNROLL, step, 0)


def turn_tables(to_kz_ref, to_ky_ref, to_kx_ref, from_kz_ref, from_ky_ref, from_kx_ref):
    row = lax.broadcasted_iota(jnp.int32, (GRID, 1), 0)
    twice = jnp.where(lax.rem(row, GRID // 2) == 0, 1.0, 2.0)
    for part in range(2):
        from_kz_ref[part] = (to_kz_ref[part].T.astype(F32) * twice).astype(BF16)
        from_ky_ref[part] = to_ky_ref[part].T
        from_kx_ref[part] = to_kx_ref[part].T


MESH = pl.DeviceIdType.MESH
INPUTS = ("charges", "fractions", "base_cells")
SMALL = ("counts", "of_y")
NAMES = ("to_kz", "to_ky", "to_kx", "twist", "of_x", "of_z")


FAR = sorted(
    ((a, b) for a in range(4) for b in range(4) if a or b),
    key=lambda o: -(min(o[0], 4 - o[0]) + min(o[1], 4 - o[1])),
)


def drain(ref, sem):
    pltpu.make_async_copy(ref, ref, sem).wait()


def fused_kernel(*refs):
    total = len(INPUTS) + len(SMALL) + len(NAMES)
    hbm, out_ref, refs = refs[:total], refs[total], refs[total + 1 :]
    local, refs = refs[:total], refs[total:]
    (rows_x_ref, rows_y_ref, both_z_ref, strips_ref, high_ref, low_ref, grid_ref, rim_in_ref, planes_ref,
     send_ref, modes_ref, send2_ref, modes2_ref, blocks_ref, near_ref, far_ref, part_ref, pot_ref, rim_ref, strips2_ref,
     both_x_ref, grads_y_ref, fold_z_ref, fold_y_ref, strip_ref, from_kz_ref, from_ky_ref, from_kx_ref,
     load_sem, rim_send, rim_recv, a_send, a_recv, c_send, c_recv, d_send, d_recv,
     b_send, b_recv, e_send, e_recv) = refs
    loads = [pltpu.make_async_copy(h, v, load_sem.at[i]) for i, (h, v) in enumerate(zip(hbm, local))]
    first = len(INPUTS) + len(SMALL)
    for load in loads[:first]:
        load.start()
    charges_ref, frac_ref, base_ref, counts_ref, of_y_ref = local[:first]
    t = dict(zip(NAMES, local[first:]))
    ix, iy, iz = block_index()
    count_x = lax.axis_size("gx")
    block = iz * 4 + iy
    plane = plane_of(iz, iy)
    mine = ix * COLUMN + plane
    after = {"gx": lax.rem(ix + 1, count_x)}
    before = {"gx": lax.rem(ix + count_x - 1, count_x)}
    core, height = lax.rem(iy, 2), lax.div(iy, 2) * 2 + iz
    others = []
    for up, flip in ((2, 0), (2, 1), (1, 0), (1, 1), (3, 0), (3, 1), (0, 1), (0, 0)):
        to = lax.rem(core + flip, 2) * 4 + lax.rem(height + up, 4)
        others.append((to, holder_of(to)))

    barrier = pltpu.get_barrier_semaphore()

    def everyone(action):
        def row(_, steps):
            along, across = lax.rem(steps, 4), lax.rem(lax.div(steps, 4), 4)
            to_x = lax.rem(lax.div(ix, 4) + along, 4) * 4 + lax.rem(lax.rem(ix, 4) + across, 4)
            for to, where in others:
                action(to_x * COLUMN + to, {"gx": to_x, **where})
            return lax.div(steps, 16)

        for part in (FAR[:7], FAR[7:]):
            steps = sum((a + 4 * b) << (4 * i) for i, (a, b) in enumerate(part))
            lax.fori_loop(0, len(part), row, jnp.int32(steps))
        for to, where in others[:-1]:
            action(ix * COLUMN + to, where)

    def greet(to, where):
        pl.semaphore_signal(barrier, inc=1, device_id=where, device_id_type=MESH)

    with jax.named_scope("greet"):
        everyone(greet)
    with jax.named_scope("load"):
        for load in loads[:first]:
            load.wait()
        for load in loads[first:]:
            load.start()
    spread = (rows_x_ref, rows_y_ref, both_z_ref, strips_ref)
    with jax.named_scope("rows"):
        spread_rows(counts_ref, charges_ref, frac_ref, base_ref, *spread)
    with jax.named_scope("spread4"):
        spread_group(4, *spread, high_ref, low_ref, grid_ref)
    def give(to):
        @pl.when(to != plane)
        def _():
            pltpu.make_async_remote_copy(
                src_ref=grid_ref.at[pl.ds(2 * to, 2)], dst_ref=planes_ref.at[block],
                send_sem=a_send.at[to], recv_sem=a_recv.at[block],
                device_id=holder_of(to), device_id_type=MESH,
            ).start()

    def group_at(i):
        return 1 + lax.rem(i + plane, 3)

    with jax.named_scope("spread1"):
        spread_group(group_at(0), *spread, high_ref, low_ref, grid_ref)
    with jax.named_scope("barwait"):
        pl.semaphore_wait(barrier, 127)
    rim = pltpu.make_async_remote_copy(
        src_ref=grid_ref.at[pl.ds(CX, HALO)], dst_ref=rim_in_ref, send_sem=rim_send, recv_sem=rim_recv,
        device_id=after, device_id_type=MESH,
    )
    rim.start()
    give(2 * group_at(0))
    give(2 * group_at(0) + 1)

    def some(i, carry):
        group = group_at(i)
        spread_group(group, *spread, high_ref, low_ref, grid_ref)
        give(2 * group)
        give(2 * group + 1)
        return carry

    with jax.named_scope("spread23"):
        lax.fori_loop(1, 3, some, 0)
    with jax.named_scope("spread0"):
        spread_group(0, *spread, high_ref, low_ref, grid_ref)
    with jax.named_scope("rimwait"):
        rim.wait_recv()
    grid_ref[0:HALO] += rim_in_ref[...]
    give(0)
    give(1)
    planes_ref[pl.ds(block, 1)] = grid_ref[pl.ds(2 * plane, 2)].reshape(1, 2, ROWS, CZ)
    with jax.named_scope("await"):
        for load in loads[first:]:
            load.wait()
        for b in range(COLUMN):
            pl.when(b != block)(functools.partial(drain, planes_ref.at[b], a_recv.at[b]))

    def spray(source, target, send_sem, recv_sem, half):
        def one(to, where):
            pltpu.make_async_remote_copy(
                src_ref=source.at[half, to], dst_ref=target.at[half, mine], send_sem=send_sem.at[half],
                recv_sem=recv_sem.at[half], device_id=where, device_id_type=MESH,
            ).start()

        with jax.named_scope("send"):
            everyone(one)
        target[half, pl.ds(mine, 1)] = source[half, pl.ds(mine, 1)]

    def arrive(target, recv_sem, half):
        with jax.named_scope("arrive"):
            drain(target.at[half, pl.ds(0, 127)], recv_sem.at[half])

    forward_kernel(
        planes_ref, t["to_kz"], t["to_ky"], send_ref,
        functools.partial(spray, send_ref, modes_ref, c_send, c_recv),
    )
    with jax.named_scope("turn"):
        turn_tables(t["to_kz"], t["to_ky"], t["to_kx"], from_kz_ref, from_ky_ref, from_kx_ref)
    for half in range(2):
        arrive(modes_ref, c_recv, half)
        with jax.named_scope("middle"):
            middle_kernel(
                half, modes_ref, t["to_kx"], from_kx_ref, t["twist"], t["of_x"], t["of_z"], of_y_ref, send2_ref
            )
        spray(send2_ref, modes2_ref, d_send, d_recv, half)
    with jax.named_scope("gather_rows"):
        gather_rows(
            frac_ref, base_ref, rows_x_ref, both_x_ref, grads_y_ref, fold_z_ref, fold_y_ref, strip_ref, rows_y_ref
        )
    backward_kernel(
        modes2_ref, from_ky_ref, from_kz_ref, blocks_ref, functools.partial(arrive, modes2_ref, d_recv)
    )

    sends = []
    for slot in range(1, COLUMN):
        up, flip = ORDER_UP[slot]
        to = lax.rem(core + flip, 2) * 4 + lax.rem(height + up, 4)
        where = holder_of(to)
        theirs = ORDER_UP.index(((4 - up) % 4, flip))
        copy = pltpu.make_async_remote_copy(
            src_ref=blocks_ref.at[where["gz"] * 4 + where["gy"]], dst_ref=near_ref.at[theirs],
            send_sem=b_send.at[slot], recv_sem=b_recv.at[theirs], device_id=where, device_id_type=MESH,
        )
        copy.start()
        sends.append(copy)
    near_ref[0] = blocks_ref[block]
    slot_cells = []
    for up, flip in ORDER_UP:
        x = 2 * (lax.rem(core + flip, 2) * 4 + lax.rem(height + up, 4))
        slot_cells += [x, x + 1]

    def slot_of(low_plane):
        up = lax.rem(low_plane - height + 4, 4)
        return jnp.where(up < 2, 2 * up, 10 - 2 * up) + core

    rims_back = []
    for low_plane, layers in ((0, 2), (1, 1)):
        slot = slot_of(low_plane)
        rims_back.append((slot, pltpu.make_async_remote_copy(
            src_ref=near_ref.at[slot, pl.ds(0, layers)], dst_ref=far_ref.at[pl.ds(2 * low_plane, layers)],
            send_sem=e_send.at[low_plane], recv_sem=e_recv.at[low_plane],
            device_id=before, device_id_type=MESH,
        )))
    tools = (both_x_ref, rows_y_ref, grads_y_ref, fold_z_ref, fold_y_ref, strip_ref)
    chunks = charges_ref.shape[1] // WIDTH

    def keep(c, at, force_x, force_y, force_z):
        part_ref[0, :, at] = force_x
        part_ref[1, :, at] = force_y
        part_ref[2, :, at] = force_z

    def finish(c, at, *forces):
        slot = lax.broadcasted_iota(jnp.int32, (1, WIDTH), 1) + c * WIDTH
        charge = jnp.where(slot < counts_ref[0, 0, 0], charges_ref[:, at], 0.0)
        total = [
            jnp.sum(part_ref[d, :, at] + force, axis=0, keepdims=True) for d, force in enumerate(forces)
        ]
        out_ref[:, at] = -charge * jnp.concatenate(total, axis=0)

    with jax.named_scope("bwait"):
        for slot in range(1, EARLY):
            drain(near_ref.at[slot], b_recv.at[slot])
        for slot, copy in rims_back:
            pl.when(slot < EARLY)(copy.start)
    with jax.named_scope("stage1"):
        strips2_ref[0 : EARLY * 16] = stage(
            pot_ref, rim_ref, [near_ref[slot, i] for slot in range(EARLY) for i in range(2)]
        )
    with jax.named_scope("gather1"):
        gather_part(0, chunks // 2, slot_cells[: 2 * EARLY], pot_ref, strips2_ref, *tools, keep)
    with jax.named_scope("bwait2"):
        for slot in range(EARLY, COLUMN):
            drain(near_ref.at[slot], b_recv.at[slot])
        for slot, copy in rims_back:
            pl.when(slot >= EARLY)(copy.start)
    with jax.named_scope("gather2"):
        gather_part(chunks // 2, chunks, slot_cells[: 2 * EARLY], pot_ref, strips2_ref, *tools, keep)
    with jax.named_scope("sendwait"):
        rim.wait_send()
        for o in range(COLUMN):
            @pl.when(o != plane)
            def _():
                drain(grid_ref.at[pl.ds(2 * o, 2)], a_send.at[o])

        for half in range(2):
            drain(send_ref.at[half, pl.ds(0, 127)], c_send.at[half])
            drain(send2_ref.at[half, pl.ds(0, 127)], d_send.at[half])
        for copy in sends:
            copy.wait_send()
    with jax.named_scope("ewait"):
        for _, copy in rims_back:
            copy.wait_send()
            copy.wait_recv()
    with jax.named_scope("stage3"):
        late = [near_ref[slot, i] for slot in range(EARLY, COLUMN) for i in range(2)]
        late += [far_ref[i] for i in range(HALO)]
        strips2_ref[0 : len(late) * 8] = stage(pot_ref, rim_ref, late)
    with jax.named_scope("gather3"):
        cells = slot_cells[2 * EARLY :] + [CX, CX + 1, CX + 2]
        gather_part(0, chunks, cells, pot_ref, strips2_ref, *tools, finish)


def per_device(charges, fractions, base_cells, counts):
    t = {name: jnp.asarray(value) for name, value in tables().items()}
    arrays = [charges.reshape(1, -1), fractions, base_cells, counts, t["of_y"]]
    arrays += [t[name] for name in NAMES]
    small = len(INPUTS) + len(SMALL)
    atoms = fractions.shape[1]
    dma = pltpu.SemaphoreType.DMA
    scratch = [
        (pltpu.SMEM if len(INPUTS) <= i < small else pltpu.VMEM)(a.shape, a.dtype)
        for i, a in enumerate(arrays)
    ]
    scratch += [
        pltpu.VMEM((24, atoms), F32),
        pltpu.VMEM((ROWS, atoms), F32),
        pltpu.VMEM((2 * CZ, atoms), BF16),
        pltpu.VMEM((160, CZ), F32),
        pltpu.VMEM((4 * ROWS, atoms), BF16),
        pltpu.VMEM((4 * ROWS, atoms), BF16),
        pltpu.VMEM((20, ROWS, CZ), F32),
        pltpu.VMEM((HALO, ROWS, CZ), F32),
        pltpu.VMEM((COLUMN, 2, ROWS, CZ), F32),
        pltpu.VMEM((2, 128, 4, 128), F32),
        pltpu.VMEM((2, 128, 4, 128), F32),
        pltpu.VMEM((2, 128, 4, 128), F32),
        pltpu.VMEM((2, 128, 4, 128), F32),
        pltpu.VMEM((COLUMN, 2, ROWS, CZ), F32),
        pltpu.VMEM((COLUMN, 2, ROWS, CZ), F32),
        pltpu.VMEM((HALO, ROWS, CZ), F32),
        pltpu.VMEM((3, 8, atoms), F32),
        pltpu.VMEM((2 * EARLY * ROWS, 384), BF16),
        pltpu.VMEM((2 * EARLY * 8, 128), F32),
        pltpu.VMEM((2 * EARLY * 8, 384), BF16),
        pltpu.VMEM((atoms // WIDTH, 48, WIDTH), F32),
        pltpu.VMEM((ROWS, atoms), F32),
        pltpu.VMEM((atoms // WIDTH, 384, 2 * WIDTH), BF16),
        pltpu.VMEM((atoms // WIDTH, 384, 2 * WIDTH), BF16),
        pltpu.VMEM((16, atoms), F32),
        pltpu.VMEM(t["to_kz"].shape, BF16),
        pltpu.VMEM(t["to_ky"].shape, BF16),
        pltpu.VMEM(t["to_kx"].shape, BF16),
        dma((len(arrays),)), dma, dma, dma((COLUMN,)), dma((COLUMN,)), dma((2,)), dma((2,)), dma((2,)), dma((2,)),
        dma((COLUMN,)), dma((COLUMN,)), dma((2,)), dma((2,)),
    ]
    return pl.pallas_call(
        fused_kernel,
        out_shape=jax.ShapeDtypeStruct(fractions.shape, F32),
        in_specs=[pl.BlockSpec(memory_space=pltpu.HBM)] * len(arrays),
        out_specs=pl.BlockSpec(memory_space=pltpu.VMEM),
        scratch_shapes=scratch,
        compiler_params=pltpu.CompilerParams(
            collective_id=0, has_side_effects=True, vmem_limit_bytes=62 << 20
        ),
    )(*arrays)


def solution(mesh):
    split = ("gz", "gy", "gx")
    return jax.shard_map(
        per_device,
        mesh=mesh,
        in_specs=(P(split), P(None, split), P(None, split), P("gz", "gy", "gx")),
        out_specs=P(None, split),
        check_vma=False,
    )
```

```python
import functools

import jax
import jax.numpy as jnp
import numpy as np
from jax import lax
from jax.experimental import pallas as pl
from jax.experimental.pallas import tpu as pltpu
from jax.sharding import PartitionSpec as P

GRID = 256
ORDER = 4
HALO = ORDER - 1
COULOMB = 332.0636
EWALD = 0.7
CX, CY, CZ = 16, 64, 128
ROWS = 72
SPAN = CX + HALO
COLUMN = 8
F32 = jnp.float32
BF16 = jnp.bfloat16
NN = (((1,), (0,)), ((), ()))
NT = (((1,), (1,)), ((), ()))


def split_np(a):
    a = np.asarray(a, np.float32)
    high = a.astype(jnp.bfloat16)
    low = (a - high.astype(np.float32)).astype(jnp.bfloat16)
    return np.stack([high, low])


def tables():
    k = np.arange(GRID)
    half = np.arange(GRID // 2)

    def turn(first, second, length):
        angle = (first[:, None] * second[None, :] % length) * (2.0 * np.pi / length)
        return np.cos(angle), np.sin(angle)

    cos, sin = turn(k, half, GRID)
    to_kz = np.concatenate([cos, -sin], axis=1)
    cos, sin = turn(k, k, GRID)
    real = np.concatenate([cos, sin], axis=1).reshape(64, 2, 2, 512)
    imag = np.concatenate([-sin, cos], axis=1).reshape(64, 2, 2, 512)
    to_ky = np.stack([real, imag], axis=2).swapaxes(0, 1).reshape(512, 512)
    cos, sin = turn(half, half, GRID // 2)
    to_kx = np.concatenate(
        [np.concatenate([cos, sin], axis=1), np.concatenate([-sin, cos], axis=1)], axis=0
    )
    angle = half[:, None] * (2.0 * np.pi / GRID) * np.ones((1, 128))
    upper = np.arange(128)[None, :] >= 64
    twist = np.stack([np.where(upper, np.cos(angle), 1.0), np.where(upper, np.sin(angle), 0.0)])
    signed = np.where(2 * k < GRID, k, k - GRID).astype(np.float64)
    spline = 36.0 / (4.0 + 2.0 * np.cos(k * (2.0 * np.pi / GRID))) ** 2
    spline[GRID // 2] = 0.0
    decay = spline * np.exp(-np.pi**2 * signed**2 / (EWALD**2 * GRID**2))
    lanes = np.arange(128)
    kx = half[:, None] + 128 * (lanes[None, :] // 64)
    of_x = np.stack([decay[kx] * (COULOMB / (np.pi * GRID)), signed[kx] ** 2])
    kz = 64 * np.arange(2)[:, None] + lanes[None, :] % 64
    of_z = np.stack([decay[kz], signed[kz] ** 2], axis=1)
    of_y = np.stack([decay, signed**2])
    return dict(
        to_kz=split_np(to_kz),
        to_ky=split_np(to_ky),
        to_kx=split_np(to_kx),
        twist=twist.astype(np.float32),
        of_x=of_x.astype(np.float32),
        of_y=of_y.astype(np.float32),
        of_z=of_z.astype(np.float32),
    )


def halves(value):
    high = value.astype(BF16)
    return high, (value - high.astype(F32)).astype(BF16)


def dot(a, b, dims=NN):
    return lax.dot_general(a, b, dims, preferred_element_type=F32)


def dot3(a, b):
    return dot(
        jnp.concatenate([a[0], a[1], a[0]], axis=1), jnp.concatenate([b[0], b[0], b[1]], axis=0)
    )


def part_of(ref, *at):
    return ref[(0, *at)], ref[(1, *at)]


def spline_weights(t):
    rest = 1.0 - t
    square = t * t
    cube = square * t
    weights = (
        rest * rest * rest / 6.0,
        (3.0 * cube - 6.0 * square + 4.0) / 6.0,
        (-3.0 * cube + 3.0 * square + 3.0 * t + 1.0) / 6.0,
        cube / 6.0,
    )
    slopes = (-0.5 * rest * rest, 1.5 * square - 2.0 * t, -1.5 * square + t + 0.5, 0.5 * square)
    return weights, slopes


def place(values, lowest, rows):
    offset = lax.broadcasted_iota(jnp.int32, (rows, lowest.shape[1]), 0) - lowest
    out = jnp.where(offset == 3, values[3], 0.0)
    for i in (2, 1, 0):
        out = jnp.where(offset == i, values[i], out)
    return out


def block_index():
    return lax.axis_index("gx"), lax.axis_index("gy"), lax.axis_index("gz")


def plane_of(iz, iy):
    return lax.rem(iy, 2) * 4 + lax.div(iy, 2) * 2 + iz


def holder_of(plane):
    return {"gz": lax.rem(plane, 2), "gy": lax.rem(lax.div(plane, 2), 2) * 2 + lax.div(plane, 4)}


def spread_rows(counts_ref, charges_ref, frac_ref, base_ref, rows_x_ref, rows_y_ref, both_z_ref, strips_ref,
                both_y_ref, high_ref, low_ref):
    ix, iy, iz = block_index()
    width = 512
    rim_row = lax.broadcasted_iota(jnp.int32, (8, 1), 0)
    inside = (rim_row >= 3) & (rim_row < 6)

    for c in range(charges_ref.shape[1] // width):
        at = pl.ds(c * width, width)
        slot = lax.broadcasted_iota(jnp.int32, (1, width), 1) + c * width
        charge = jnp.where(slot < counts_ref[0, 0, 0], charges_ref[:, at], 0.0)
        wx, _ = spline_weights(frac_ref[0:1, at])
        wy, _ = spline_weights(frac_ref[1:2, at])
        wz, _ = spline_weights(frac_ref[2:3, at])
        wz = [w * charge for w in wz]
        low_z = base_ref[2:3, at] - iz * CZ
        rows_x = place(wx, base_ref[0:1, at] - ix * CX, 24)
        rows_x_ref[:, at] = rows_x
        rows_y = place(wy, base_ref[1:2, at] - iy * CY, ROWS)
        rows_y_ref[:, at] = rows_y
        high, low = halves(rows_y)
        both_y_ref[0:ROWS, at] = high
        both_y_ref[ROWS : 2 * ROWS, at] = low
        high, low = halves(place(wz, low_z, CZ))
        both_z_ref[0:CZ, at] = high
        both_z_ref[CZ : 2 * CZ, at] = low
        rim_z = jnp.where(inside, place(wz, low_z - (CZ - HALO), 8), 0.0)
        high, low = halves(jnp.concatenate([rows_x[x : x + 1] * rim_z for x in range(20)], axis=0))
        high_ref[0:160, at] = high
        low_ref[0:160, at] = low
    pad = jnp.zeros((256 - 2 * ROWS, both_y_ref.shape[1]), BF16)
    total = dot(high_ref[0:160], jnp.concatenate([both_y_ref[...], pad], axis=0), NT)
    pad = jnp.zeros((CZ - ROWS, both_y_ref.shape[1]), BF16)
    more = dot(low_ref[0:160], jnp.concatenate([both_y_ref[0:ROWS], pad], axis=0), NT)
    strips_ref[...] = jnp.concatenate(
        [total[:, :ROWS] + total[:, ROWS : 2 * ROWS], jnp.zeros((160, CZ - ROWS), F32)], axis=1
    ) + more


def spread_group(group, rows_x_ref, rows_y_ref, both_z_ref, strips_ref, high_ref, low_ref, out_ref):
    for i in range(4):
        high, low = halves(rows_x_ref[pl.ds(group * 4 + i, 1), :] * rows_y_ref[...])
        high_ref[pl.ds(i * ROWS, ROWS), :] = high
        low_ref[pl.ds(i * ROWS, ROWS), :] = low
    total = dot(high_ref[...], both_z_ref[...], NT)
    total = total[:, :CZ] + total[:, CZ:] + dot(low_ref[...], both_z_ref[0:CZ], NT)
    for i in range(4):
        x = group * 4 + i
        strip = strips_ref[pl.ds(pl.multiple_of(x * 8, 8), 8), :]
        out_ref[x, 0:64, :] = total[i * ROWS : i * ROWS + 64]
        out_ref[x, 64:72, :] = total[i * ROWS + 64 : i * ROWS + 72] + strip


def forward_kernel(data_ref, to_kz_ref, to_ky_ref, out_ref, leave):
    lane = lax.broadcasted_iota(jnp.int32, (1, 128), 1)
    row = lax.broadcasted_iota(jnp.int32, (8, 128), 0)
    lower = lane < 64
    parts = []
    for x in range(2):
        planes = []
        for iz in range(2):
            pieces = []
            for iy in range(4):
                rim = jnp.where(row < HALO, data_ref[iz * 4 + (iy + 3) % 4, x, 64:72, :], 0.0)
                pieces.append(data_ref[iz * 4 + iy, x, 0:8, :] + rim)
                pieces.append(data_ref[iz * 4 + iy, x, 8:64, :])
            planes.append(jnp.concatenate(pieces, axis=0))
        rims = []
        for iz in range(2):
            tiles = [data_ref[iz * 4 + iy, x, 64:72, :] for iy in range(4)]
            turned = [pltpu.roll(tiles[1], 64, 1), pltpu.roll(tiles[3], 64, 1)]
            first = tiles[0] + jnp.where(lower, turned[1], turned[0])
            second = tiles[2] + jnp.where(lower, turned[0], turned[1])
            rims.append(jnp.concatenate([first, second], axis=1))
        rims = jnp.concatenate(rims + [jnp.zeros((112, 256), F32)], axis=0).T
        planes[1] = planes[1] + jnp.where(lane < HALO, pltpu.roll(rims, 125, 1), 0.0)
        planes[0] = planes[0] + jnp.where(lane < HALO, pltpu.roll(rims, 117, 1), 0.0)
        plane = jnp.concatenate(planes, axis=1)
        parts.append(dot3(halves(plane), (to_kz_ref[0], to_kz_ref[1])))
    rows = []
    for c in range(2):
        zero, one = (p[:, c * 128 : (c + 1) * 128] for p in parts)
        first = jnp.where(lower, zero, pltpu.roll(one, 64, 1))
        second = jnp.where(lower, pltpu.roll(zero, 64, 1), one)
        rows.append(jnp.concatenate([first, second], axis=1))
    both = halves(jnp.concatenate(rows, axis=0))
    for half in range(2):
        out = dot3(part_of(to_ky_ref, slice(half * 256, half * 256 + 256)), both)
        flat = out_ref.reshape(2, 512, 128)
        flat[half, 0:256] = out[:, :128]
        flat[half, 256:512] = out[:, 128:]
        leave(half)


def middle_kernel(part, data_ref, to_kx_ref, from_kx_ref, twist_ref, of_x_ref, of_z_ref, of_y_ref, out_ref):
    ix, iy, iz = block_index()
    mine = ix * COLUMN + plane_of(iz, iy)
    half, group = mine // 64, mine % 64
    lane = lax.broadcasted_iota(jnp.int32, (1, 128), 1)
    sign = jnp.where(lane < 64, 1.0, -1.0)
    flat = data_ref.reshape(2, 512, 128)
    both = jnp.concatenate(
        [
            jnp.concatenate([flat[part, pl.ds(c * 2 + i, 128, stride=4), :] for i in range(2)], axis=1)
            for c in range(2)
        ],
        axis=0,
    )
    out = dot3(part_of(to_kx_ref), halves(both))
    cos, sin = twist_ref[0], twist_ref[1]
    of_z = of_z_ref[half]
    scale_xz = of_x_ref[0] * of_z[0:1]
    square_xz = of_x_ref[1] + of_z[1:2]
    reals, imags = [], []
    for i in range(2):
        real = out[:128, i * 128 : (i + 1) * 128]
        imag = out[128:, i * 128 : (i + 1) * 128]
        real, imag = real * cos + imag * sin, imag * cos - real * sin
        real = real * sign + pltpu.roll(real, 64, 1)
        imag = imag * sign + pltpu.roll(imag, 64, 1)
        ky = group * 4 + part * 2 + i
        square = square_xz + of_y_ref[1, ky]
        green = jnp.where(square > 0.0, scale_xz * of_y_ref[0, ky] / jnp.maximum(square, 1.0), 0.0)
        real, imag = real * green, imag * green
        real = real * sign + pltpu.roll(real, 64, 1)
        imag = imag * sign + pltpu.roll(imag, 64, 1)
        real, imag = real * cos - imag * sin, imag * cos + real * sin
        reals.append(real)
        imags.append(imag)
    both = jnp.concatenate(
        [jnp.concatenate(reals, axis=1), jnp.concatenate(imags, axis=1)], axis=0
    )
    out = dot3(part_of(from_kx_ref), halves(both))
    flat = out_ref.reshape(2, 512, 128)
    for c in range(2):
        for i in range(2):
            flat[part, pl.ds(c * 2 + i, 128, stride=4), :] = out[c * 128 : (c + 1) * 128, i * 128 : (i + 1) * 128]


def backward_kernel(data_ref, from_ky_ref, from_kz_ref, out_ref, arrive):
    lane = lax.broadcasted_iota(jnp.int32, (1, 128), 1)
    row = lax.broadcasted_iota(jnp.int32, (8, 128), 0)
    lower = lane < 64
    out = 0.0
    for half in range(2):
        arrive(half)
        flat = data_ref.reshape(2, 512, 128)
        both = jnp.concatenate([flat[half, 0:256], flat[half, 256:512]], axis=1)
        out = out + dot3(
            part_of(from_ky_ref, slice(None), slice(half * 256, half * 256 + 256)), halves(both)
        )
    tiles = [[], []]
    for c in range(2):
        first, second = out[c * 256 : (c + 1) * 256, :128], out[c * 256 : (c + 1) * 256, 128:]
        tiles[0].append(jnp.where(lower, first, pltpu.roll(second, 64, 1)))
        tiles[1].append(jnp.where(lower, pltpu.roll(first, 64, 1), second))
    for x in range(2):
        plane = dot3(halves(jnp.concatenate(tiles[x], axis=1)), part_of(from_kz_ref))
        turned = [plane[:, h * 128 : (h + 1) * 128].T[:8] for h in range(2)]
        for iz in range(2):
            near = plane[:, iz * 128 : (iz + 1) * 128]
            strips = (turned[1 - iz][:, :128], turned[1 - iz][:, 128:])
            rolled = [pltpu.roll(s, 64, 1) for s in strips]
            for iy in range(4):
                after = (iy + 1) % 4
                t = iy // 2
                if iy % 2 == 0:
                    strip = strips[t]
                else:
                    strip = jnp.where(lower, rolled[t], rolled[1 - t])
                out_ref[iz * 4 + iy, x, 0:64, :] = near[iy * 64 : iy * 64 + 64]
                out_ref[iz * 4 + iy, x, 64:72, :] = jnp.where(
                    row < HALO, near[after * 64 : after * 64 + 8], pltpu.roll(strip, HALO, 0)
                )


WIDTH = 128
UNROLL = 4
ORDER_UP = ((0, 0), (0, 1), (1, 0), (1, 1), (3, 0), (3, 1), (2, 0), (2, 1))
EARLY = 6


def gather_rows(frac_ref, base_ref, rows_x_ref, both_x_ref, grads_y_ref, fold_z_ref):
    ix, iy, iz = block_index()
    rim_row = lax.broadcasted_iota(jnp.int32, (8, 1), 0)
    inside = (rim_row >= 3) & (rim_row < 6)

    def step(c, carry):
        at = pl.ds(pl.multiple_of(c * WIDTH, WIDTH), WIDTH)
        _, sx = spline_weights(frac_ref[0:1, at])
        _, sy = spline_weights(frac_ref[1:2, at])
        wz, sz = spline_weights(frac_ref[2:3, at])
        low_z = base_ref[2:3, at] - iz * CZ
        both_x_ref[c, 0:24] = rows_x_ref[:, at]
        both_x_ref[c, 24:48] = place(sx, base_ref[0:1, at] - ix * CX, 24)
        grads_y_ref[:, at] = place(sy, base_ref[1:2, at] - iy * CY, ROWS)
        high, low = halves(jnp.concatenate([place(wz, low_z, CZ), place(sz, low_z, CZ)], axis=1))
        fold_z_ref[c, 0:128] = high
        fold_z_ref[c, 128:256] = high
        fold_z_ref[c, 256:384] = low
        rim_low = low_z - (CZ - HALO)
        rims = jnp.concatenate([place(wz, rim_low, 8), place(sz, rim_low, 8)], axis=1)
        rims = jnp.where(inside, rims, 0.0)
        rest = rims - rims.astype(BF16).astype(F32)
        zeros = jnp.zeros((104, 2 * WIDTH), F32)
        fold_z_ref[c, 384:512] = jnp.concatenate([rims, rims, rest, zeros], axis=0).astype(BF16)
        return carry

    lax.fori_loop(0, frac_ref.shape[1] // WIDTH, step, 0)


def stage(pot_ref, layers):
    lane = lax.broadcasted_iota(jnp.int32, (1, 128), 1)
    strips = [layer[64:72] for layer in layers]
    blank = [jnp.zeros((128 - 8 * len(layers), 128), F32)] if len(layers) < 16 else []
    turned = jnp.concatenate(strips + blank, axis=0).T[:ROWS]
    for i, layer in enumerate(layers):
        high, low = halves(layer)
        at = pl.ds(i * ROWS, ROWS)
        pot_ref[at, 0:128] = high
        pot_ref[at, 128:256] = low
        pot_ref[at, 256:384] = high
        first, second, third = (pltpu.roll(turned, (128 + 8 * k - 8 * i) % 128, 1) for k in range(3))
        value = jnp.where(lane < 8, first, jnp.where(lane < 16, second, third))
        value = jnp.where(lane < 24, value, 0.0)
        rounded = value.astype(BF16).astype(F32)
        value = jnp.where((lane >= 8) & (lane < 16), value - rounded, rounded)
        pot_ref[at, 384:512] = value.astype(BF16)


def gather_part(cells, pot_ref, both_x_ref, rows_y_ref, grads_y_ref, fold_z_ref, finish):
    def one(c):
        at = pl.ds(pl.multiple_of(c * WIDTH, WIDTH), WIDTH)
        rows_y, grads_y = rows_y_ref[:, at], grads_y_ref[:, at]
        main = dot(pot_ref[0 : len(cells) * ROWS], fold_z_ref[c])
        force_x = force_y = force_z = 0.0
        for i, x in enumerate(cells):
            sum_x = sum_y = sum_z = 0.0
            for y in range(ROWS // 8):
                low = i * ROWS + y * 8
                plain, sloped = main[low : low + 8, :WIDTH], main[low : low + 8, WIDTH:]
                near = rows_y[y * 8 : y * 8 + 8]
                sum_x += plain * near
                sum_y += plain * grads_y[y * 8 : y * 8 + 8]
                sum_z += sloped * near
            rows_x, grads_x = both_x_ref[c, pl.ds(x, 1), :], both_x_ref[c, pl.ds(x + 24, 1), :]
            force_x += grads_x * sum_x
            force_y += rows_x * sum_y
            force_z += rows_x * sum_z
        finish(c, at, force_x, force_y, force_z)

    def step(i, carry):
        for u in range(UNROLL):
            one(i * UNROLL + u)
        return carry

    lax.fori_loop(0, fold_z_ref.shape[0] // UNROLL, step, 0)


def turn_tables(to_kz_ref, to_ky_ref, to_kx_ref, from_kz_ref, from_ky_ref, from_kx_ref):
    row = lax.broadcasted_iota(jnp.int32, (GRID, 1), 0)
    twice = jnp.where(lax.rem(row, GRID // 2) == 0, 1.0, 2.0)
    for part in range(2):
        from_kz_ref[part] = (to_kz_ref[part].T.astype(F32) * twice).astype(BF16)
        from_ky_ref[part] = to_ky_ref[part].T
        from_kx_ref[part] = to_kx_ref[part].T


MESH = pl.DeviceIdType.MESH
INPUTS = ("charges", "fractions", "base_cells")
SMALL = ("counts", "of_y")
NAMES = ("to_kz", "to_ky", "to_kx", "twist", "of_x", "of_z")


FAR = sorted(
    ((a, b) for a in range(4) for b in range(4) if a or b),
    key=lambda o: -(min(o[0], 4 - o[0]) + min(o[1], 4 - o[1])),
)


def drain(ref, sem):
    pltpu.make_async_copy(ref, ref, sem).wait()


def fused_kernel(*refs):
    total = len(INPUTS) + len(SMALL) + len(NAMES)
    hbm, out_ref, refs = refs[:total], refs[total], refs[total + 1 :]
    local, refs = refs[:total], refs[total:]
    (rows_x_ref, rows_y_ref, both_z_ref, strips_ref, both_y_ref, high_ref, low_ref, grid_ref, rim_in_ref, planes_ref,
     send_ref, modes_ref, send2_ref, modes2_ref, blocks_ref, near_ref, far_ref, part_ref, pot_ref,
     both_x_ref, grads_y_ref, fold_z_ref, from_kz_ref, from_ky_ref, from_kx_ref,
     load_sem, rim_send, rim_recv, a_send, a_recv, c_send, c_recv, d_send, d_recv,
     b_send, b_recv, e_send, e_recv) = refs
    loads = [pltpu.make_async_copy(h, v, load_sem.at[i]) for i, (h, v) in enumerate(zip(hbm, local))]
    first = len(INPUTS) + len(SMALL)
    for load in loads[:first]:
        load.start()
    charges_ref, frac_ref, base_ref, counts_ref, of_y_ref = local[:first]
    t = dict(zip(NAMES, local[first:]))
    ix, iy, iz = block_index()
    count_x = lax.axis_size("gx")
    block = iz * 4 + iy
    plane = plane_of(iz, iy)
    mine = ix * COLUMN + plane
    after = {"gx": lax.rem(ix + 1, count_x)}
    before = {"gx": lax.rem(ix + count_x - 1, count_x)}
    core, height = lax.rem(iy, 2), lax.div(iy, 2) * 2 + iz
    others = []
    for up, flip in ((2, 0), (2, 1), (1, 0), (1, 1), (3, 0), (3, 1), (0, 1), (0, 0)):
        to = lax.rem(core + flip, 2) * 4 + lax.rem(height + up, 4)
        others.append((to, holder_of(to)))

    barrier = pltpu.get_barrier_semaphore()

    def everyone(action):
        def row(_, steps):
            along, across = lax.rem(steps, 4), lax.rem(lax.div(steps, 4), 4)
            to_x = lax.rem(lax.div(ix, 4) + along, 4) * 4 + lax.rem(lax.rem(ix, 4) + across, 4)
            for to, where in others:
                action(to_x * COLUMN + to, {"gx": to_x, **where})
            return lax.div(steps, 16)

        for part in (FAR[:7], FAR[7:]):
            steps = sum((a + 4 * b) << (4 * i) for i, (a, b) in enumerate(part))
            lax.fori_loop(0, len(part), row, jnp.int32(steps))
        for to, where in others[:-1]:
            action(ix * COLUMN + to, where)

    def greet(to, where):
        pl.semaphore_signal(barrier, inc=1, device_id=where, device_id_type=MESH)

    with jax.named_scope("greet"):
        everyone(greet)
    with jax.named_scope("load"):
        for load in loads[:first]:
            load.wait()
        for load in loads[first:]:
            load.start()
    spread = (rows_x_ref, rows_y_ref, both_z_ref, strips_ref)
    with jax.named_scope("rows"):
        spread_rows(
            counts_ref, charges_ref, frac_ref, base_ref, *spread, both_y_ref, high_ref, low_ref
        )
    with jax.named_scope("spread4"):
        spread_group(4, *spread, high_ref, low_ref, grid_ref)
    def give(to):
        @pl.when(to != plane)
        def _():
            pltpu.make_async_remote_copy(
                src_ref=grid_ref.at[pl.ds(2 * to, 2)], dst_ref=planes_ref.at[block],
                send_sem=a_send.at[to], recv_sem=a_recv.at[block],
                device_id=holder_of(to), device_id_type=MESH,
            ).start()

    def group_at(i):
        return 1 + lax.rem(i + plane, 3)

    with jax.named_scope("spread1"):
        spread_group(group_at(0), *spread, high_ref, low_ref, grid_ref)
    with jax.named_scope("barwait"):
        pl.semaphore_wait(barrier, 127)
    rim = pltpu.make_async_remote_copy(
        src_ref=grid_ref.at[pl.ds(CX, HALO)], dst_ref=rim_in_ref, send_sem=rim_send, recv_sem=rim_recv,
        device_id=after, device_id_type=MESH,
    )
    rim.start()
    give(2 * group_at(0))
    give(2 * group_at(0) + 1)

    def some(i, carry):
        group = group_at(i)
        spread_group(group, *spread, high_ref, low_ref, grid_ref)
        give(2 * group)
        give(2 * group + 1)
        return carry

    with jax.named_scope("spread23"):
        lax.fori_loop(1, 3, some, 0)
    with jax.named_scope("spread0"):
        spread_group(0, *spread, high_ref, low_ref, grid_ref)
    with jax.named_scope("rimwait"):
        rim.wait_recv()
    grid_ref[0:HALO] += rim_in_ref[...]
    give(0)
    give(1)
    planes_ref[pl.ds(block, 1)] = grid_ref[pl.ds(2 * plane, 2)].reshape(1, 2, ROWS, CZ)
    with jax.named_scope("await"):
        for load in loads[first:]:
            load.wait()
        for b in range(COLUMN):
            pl.when(b != block)(functools.partial(drain, planes_ref.at[b], a_recv.at[b]))

    def spray(source, target, send_sem, recv_sem, half):
        def one(to, where):
            pltpu.make_async_remote_copy(
                src_ref=source.at[half, to], dst_ref=target.at[half, mine], send_sem=send_sem.at[half],
                recv_sem=recv_sem.at[half], device_id=where, device_id_type=MESH,
            ).start()

        with jax.named_scope("send"):
            everyone(one)
        target[half, pl.ds(mine, 1)] = source[half, pl.ds(mine, 1)]

    def arrive(target, recv_sem, half):
        with jax.named_scope("arrive"):
            drain(target.at[half, pl.ds(0, 127)], recv_sem.at[half])

    forward_kernel(
        planes_ref, t["to_kz"], t["to_ky"], send_ref,
        functools.partial(spray, send_ref, modes_ref, c_send, c_recv),
    )
    with jax.named_scope("turn"):
        turn_tables(t["to_kz"], t["to_ky"], t["to_kx"], from_kz_ref, from_ky_ref, from_kx_ref)
    for half in range(2):
        arrive(modes_ref, c_recv, half)
        with jax.named_scope("middle"):
            middle_kernel(
                half, modes_ref, t["to_kx"], from_kx_ref, t["twist"], t["of_x"], t["of_z"], of_y_ref, send2_ref
            )
        spray(send2_ref, modes2_ref, d_send, d_recv, half)
    with jax.named_scope("gather_rows"):
        gather_rows(frac_ref, base_ref, rows_x_ref, both_x_ref, grads_y_ref, fold_z_ref)
    backward_kernel(
        modes2_ref, from_ky_ref, from_kz_ref, blocks_ref, functools.partial(arrive, modes2_ref, d_recv)
    )

    sends = []
    for slot in range(1, COLUMN):
        up, flip = ORDER_UP[slot]
        to = lax.rem(core + flip, 2) * 4 + lax.rem(height + up, 4)
        where = holder_of(to)
        theirs = ORDER_UP.index(((4 - up) % 4, flip))
        sends.append(pltpu.make_async_remote_copy(
            src_ref=blocks_ref.at[where["gz"] * 4 + where["gy"]], dst_ref=near_ref.at[theirs],
            send_sem=b_send.at[slot], recv_sem=b_recv.at[theirs], device_id=where, device_id_type=MESH,
        ))

    for copy in sends:
        copy.start()
    near_ref[0] = blocks_ref[block]
    slot_cells = []
    for up, flip in ORDER_UP:
        x = 2 * (lax.rem(core + flip, 2) * 4 + lax.rem(height + up, 4))
        slot_cells += [x, x + 1]

    def slot_of(low_plane):
        up = lax.rem(low_plane - height + 4, 4)
        return jnp.where(up < 2, 2 * up, 10 - 2 * up) + core

    rims_back = []
    for low_plane, layers in ((0, 2), (1, 1)):
        slot = slot_of(low_plane)
        rims_back.append((slot, pltpu.make_async_remote_copy(
            src_ref=near_ref.at[slot, pl.ds(0, layers)], dst_ref=far_ref.at[pl.ds(2 * low_plane, layers)],
            send_sem=e_send.at[low_plane], recv_sem=e_recv.at[low_plane],
            device_id=before, device_id_type=MESH,
        )))
    tools = (both_x_ref, rows_y_ref, grads_y_ref, fold_z_ref)

    def keep(c, at, *forces):
        for d, force in enumerate(forces):
            part_ref[d, :, at] = force

    def add(c, at, *forces):
        for d, force in enumerate(forces):
            part_ref[d, :, at] += force

    def finish(c, at, *forces):
        slot = lax.broadcasted_iota(jnp.int32, (1, WIDTH), 1) + c * WIDTH
        charge = jnp.where(slot < counts_ref[0, 0, 0], charges_ref[:, at], 0.0)
        total = [
            jnp.sum(part_ref[d, :, at] + force, axis=0, keepdims=True) for d, force in enumerate(forces)
        ]
        out_ref[:, at] = -charge * jnp.concatenate(total, axis=0)

    def gather_slots(first, last, more, done):
        layers = [near_ref[slot, i] for slot in range(first, last) for i in range(2)]
        layers += [far_ref[i] for i in range(more)]
        stage(pot_ref, layers)
        cells = slot_cells[2 * first : 2 * last] + [CX + i for i in range(more)]
        gather_part(cells, pot_ref, *tools, done)

    with jax.named_scope("bwait1"):
        drain(near_ref.at[1], b_recv.at[1])
    with jax.named_scope("gather1"):
        gather_slots(0, 2, 0, keep)
    with jax.named_scope("bwait2"):
        for slot in range(2, EARLY):
            drain(near_ref.at[slot], b_recv.at[slot])
        for slot, copy in rims_back:
            pl.when(slot < EARLY)(copy.start)
    with jax.named_scope("gather2"):
        gather_slots(2, EARLY, 0, add)
    with jax.named_scope("bwait3"):
        for slot in range(EARLY, COLUMN):
            drain(near_ref.at[slot], b_recv.at[slot])
        for slot, copy in rims_back:
            pl.when(slot >= EARLY)(copy.start)
    with jax.named_scope("gather3"):
        gather_slots(EARLY, COLUMN, 0, add)
    with jax.named_scope("sendwait"):
        rim.wait_send()
        for o in range(COLUMN):
            @pl.when(o != plane)
            def _():
                drain(grid_ref.at[pl.ds(2 * o, 2)], a_send.at[o])

        for half in range(2):
            drain(send_ref.at[half, pl.ds(0, 127)], c_send.at[half])
            drain(send2_ref.at[half, pl.ds(0, 127)], d_send.at[half])
        for copy in sends:
            copy.wait_send()
    with jax.named_scope("ewait"):
        for _, copy in rims_back:
            copy.wait_send()
            copy.wait_recv()
    with jax.named_scope("gather4"):
        gather_slots(0, 0, HALO, finish)


def per_device(charges, fractions, base_cells, counts):
    t = {name: jnp.asarray(value) for name, value in tables().items()}
    arrays = [charges.reshape(1, -1), fractions, base_cells, counts, t["of_y"]]
    arrays += [t[name] for name in NAMES]
    small = len(INPUTS) + len(SMALL)
    atoms = fractions.shape[1]
    dma = pltpu.SemaphoreType.DMA
    scratch = [
        (pltpu.SMEM if len(INPUTS) <= i < small else pltpu.VMEM)(a.shape, a.dtype)
        for i, a in enumerate(arrays)
    ]
    scratch += [
        pltpu.VMEM((24, atoms), F32),
        pltpu.VMEM((ROWS, atoms), F32),
        pltpu.VMEM((2 * CZ, atoms), BF16),
        pltpu.VMEM((160, CZ), F32),
        pltpu.VMEM((2 * ROWS, atoms), BF16),
        pltpu.VMEM((4 * ROWS, atoms), BF16),
        pltpu.VMEM((4 * ROWS, atoms), BF16),
        pltpu.VMEM((20, ROWS, CZ), F32),
        pltpu.VMEM((HALO, ROWS, CZ), F32),
        pltpu.VMEM((COLUMN, 2, ROWS, CZ), F32),
        pltpu.VMEM((2, 128, 4, 128), F32),
        pltpu.VMEM((2, 128, 4, 128), F32),
        pltpu.VMEM((2, 128, 4, 128), F32),
        pltpu.VMEM((2, 128, 4, 128), F32),
        pltpu.VMEM((COLUMN, 2, ROWS, CZ), F32),
        pltpu.VMEM((COLUMN, 2, ROWS, CZ), F32),
        pltpu.VMEM((HALO, ROWS, CZ), F32),
        pltpu.VMEM((3, 8, atoms), F32),
        pltpu.VMEM((2 * EARLY * ROWS, 512), BF16),
        pltpu.VMEM((atoms // WIDTH, 48, WIDTH), F32),
        pltpu.VMEM((ROWS, atoms), F32),
        pltpu.VMEM((atoms // WIDTH, 512, 2 * WIDTH), BF16),
        pltpu.VMEM(t["to_kz"].shape, BF16),
        pltpu.VMEM(t["to_ky"].shape, BF16),
        pltpu.VMEM(t["to_kx"].shape, BF16),
        dma((len(arrays),)), dma, dma, dma((COLUMN,)), dma((COLUMN,)), dma((2,)), dma((2,)), dma((2,)), dma((2,)),
        dma((COLUMN,)), dma((COLUMN,)), dma((2,)), dma((2,)),
    ]
    return pl.pallas_call(
        fused_kernel,
        out_shape=jax.ShapeDtypeStruct(fractions.shape, F32),
        in_specs=[pl.BlockSpec(memory_space=pltpu.HBM)] * len(arrays),
        out_specs=pl.BlockSpec(memory_space=pltpu.VMEM),
        scratch_shapes=scratch,
        compiler_params=pltpu.CompilerParams(
            collective_id=0, has_side_effects=True, vmem_limit_bytes=62 << 20
        ),
    )(*arrays)


def solution(mesh):
    split = ("gz", "gy", "gx")
    return jax.shard_map(
        per_device,
        mesh=mesh,
        in_specs=(P(split), P(None, split), P(None, split), P("gz", "gy", "gx")),
        out_specs=P(None, split),
        check_vma=False,
    )
```

```python
import functools

import jax
import jax.numpy as jnp
import numpy as np
from jax import lax
from jax.experimental import pallas as pl
from jax.experimental.pallas import tpu as pltpu
from jax.sharding import PartitionSpec as P

GRID = 256
ORDER = 4
HALO = ORDER - 1
COULOMB = 332.0636
EWALD = 0.7
CX, CY, CZ = 16, 64, 128
ROWS = 72
SPAN = CX + HALO
COLUMN = 8
F32 = jnp.float32
BF16 = jnp.bfloat16
NN = (((1,), (0,)), ((), ()))
NT = (((1,), (1,)), ((), ()))


def split_np(a):
    a = np.asarray(a, np.float32)
    high = a.astype(jnp.bfloat16)
    low = (a - high.astype(np.float32)).astype(jnp.bfloat16)
    return np.stack([high, low])


def tables():
    k = np.arange(GRID)
    half = np.arange(GRID // 2)

    def turn(first, second, length):
        angle = (first[:, None] * second[None, :] % length) * (2.0 * np.pi / length)
        return np.cos(angle), np.sin(angle)

    cos, sin = turn(k, half, GRID)
    to_kz = np.concatenate([cos, -sin], axis=1)
    cos, sin = turn(k, k, GRID)
    real = np.concatenate([cos, sin], axis=1).reshape(64, 2, 2, 512)
    imag = np.concatenate([-sin, cos], axis=1).reshape(64, 2, 2, 512)
    to_ky = np.stack([real, imag], axis=2).swapaxes(0, 1).reshape(512, 512)
    cos, sin = turn(half, half, GRID // 2)
    to_kx = np.concatenate(
        [np.concatenate([cos, sin], axis=1), np.concatenate([-sin, cos], axis=1)], axis=0
    )
    angle = half[:, None] * (2.0 * np.pi / GRID) * np.ones((1, 128))
    upper = np.arange(128)[None, :] >= 64
    twist = np.stack([np.where(upper, np.cos(angle), 1.0), np.where(upper, np.sin(angle), 0.0)])
    signed = np.where(2 * k < GRID, k, k - GRID).astype(np.float64)
    spline = 36.0 / (4.0 + 2.0 * np.cos(k * (2.0 * np.pi / GRID))) ** 2
    spline[GRID // 2] = 0.0
    decay = spline * np.exp(-np.pi**2 * signed**2 / (EWALD**2 * GRID**2))
    lanes = np.arange(128)
    kx = half[:, None] + 128 * (lanes[None, :] // 64)
    of_x = np.stack([decay[kx] * (COULOMB / (np.pi * GRID)), signed[kx] ** 2])
    kz = 64 * np.arange(2)[:, None] + lanes[None, :] % 64
    of_z = np.stack([decay[kz], signed[kz] ** 2], axis=1)
    of_y = np.stack([decay, signed**2])
    return dict(
        to_kz=split_np(to_kz),
        to_ky=split_np(to_ky),
        to_kx=split_np(to_kx),
        twist=twist.astype(np.float32),
        of_x=of_x.astype(np.float32),
        of_y=of_y.astype(np.float32),
        of_z=of_z.astype(np.float32),
    )


def halves(value):
    high = value.astype(BF16)
    return high, (value - high.astype(F32)).astype(BF16)


def dot(a, b, dims=NN):
    return lax.dot_general(a, b, dims, preferred_element_type=F32)


def dot3(a, b):
    return dot(
        jnp.concatenate([a[0], a[1], a[0]], axis=1), jnp.concatenate([b[0], b[0], b[1]], axis=0)
    )


def part_of(ref, *at):
    return ref[(0, *at)], ref[(1, *at)]


def spline_weights(t):
    rest = 1.0 - t
    square = t * t
    cube = square * t
    weights = (
        rest * rest * rest / 6.0,
        (3.0 * cube - 6.0 * square + 4.0) / 6.0,
        (-3.0 * cube + 3.0 * square + 3.0 * t + 1.0) / 6.0,
        cube / 6.0,
    )
    slopes = (-0.5 * rest * rest, 1.5 * square - 2.0 * t, -1.5 * square + t + 0.5, 0.5 * square)
    return weights, slopes


def place(values, lowest, rows):
    offset = lax.broadcasted_iota(jnp.int32, (rows, lowest.shape[1]), 0) - lowest
    out = jnp.where(offset == 3, values[3], 0.0)
    for i in (2, 1, 0):
        out = jnp.where(offset == i, values[i], out)
    return out


def block_index():
    return lax.axis_index("gx"), lax.axis_index("gy"), lax.axis_index("gz")


def plane_of(iz, iy):
    return lax.rem(iy, 2) * 4 + lax.div(iy, 2) * 2 + iz


def holder_of(plane):
    return {"gz": lax.rem(plane, 2), "gy": lax.rem(lax.div(plane, 2), 2) * 2 + lax.div(plane, 4)}


def spread_rows(counts_ref, charges_ref, frac_ref, base_ref, rows_x_ref, rows_y_ref, both_z_ref, strips_ref,
                both_y_ref, high_ref, low_ref):
    ix, iy, iz = block_index()
    width = 512
    rim_row = lax.broadcasted_iota(jnp.int32, (8, 1), 0)
    inside = (rim_row >= 3) & (rim_row < 6)

    for c in range(charges_ref.shape[1] // width):
        at = pl.ds(c * width, width)
        slot = lax.broadcasted_iota(jnp.int32, (1, width), 1) + c * width
        charge = jnp.where(slot < counts_ref[0, 0, 0], charges_ref[:, at], 0.0)
        wx, _ = spline_weights(frac_ref[0:1, at])
        wy, _ = spline_weights(frac_ref[1:2, at])
        wz, _ = spline_weights(frac_ref[2:3, at])
        wz = [w * charge for w in wz]
        low_z = base_ref[2:3, at] - iz * CZ
        rows_x = place(wx, base_ref[0:1, at] - ix * CX, 24)
        rows_x_ref[:, at] = rows_x
        rows_y = place(wy, base_ref[1:2, at] - iy * CY, ROWS)
        rows_y_ref[:, at] = rows_y
        high, low = halves(rows_y)
        both_y_ref[0:ROWS, at] = high
        both_y_ref[ROWS : 2 * ROWS, at] = low
        high, low = halves(place(wz, low_z, CZ))
        both_z_ref[0:CZ, at] = high
        both_z_ref[CZ : 2 * CZ, at] = low
        rim_z = jnp.where(inside, place(wz, low_z - (CZ - HALO), 8), 0.0)
        high, low = halves(jnp.concatenate([rows_x[x : x + 1] * rim_z for x in range(20)], axis=0))
        high_ref[0:160, at] = high
        low_ref[0:160, at] = low
    pad = jnp.zeros((256 - 2 * ROWS, both_y_ref.shape[1]), BF16)
    total = dot(high_ref[0:160], jnp.concatenate([both_y_ref[...], pad], axis=0), NT)
    pad = jnp.zeros((CZ - ROWS, both_y_ref.shape[1]), BF16)
    more = dot(low_ref[0:160], jnp.concatenate([both_y_ref[0:ROWS], pad], axis=0), NT)
    strips_ref[...] = jnp.concatenate(
        [total[:, :ROWS] + total[:, ROWS : 2 * ROWS], jnp.zeros((160, CZ - ROWS), F32)], axis=1
    ) + more


def spread_group(group, rows_x_ref, rows_y_ref, both_z_ref, strips_ref, high_ref, low_ref, out_ref):
    for i in range(4):
        high, low = halves(rows_x_ref[pl.ds(group * 4 + i, 1), :] * rows_y_ref[...])
        high_ref[pl.ds(i * ROWS, ROWS), :] = high
        low_ref[pl.ds(i * ROWS, ROWS), :] = low
    total = dot(high_ref[...], both_z_ref[...], NT)
    total = total[:, :CZ] + total[:, CZ:] + dot(low_ref[...], both_z_ref[0:CZ], NT)
    for i in range(4):
        x = group * 4 + i
        strip = strips_ref[pl.ds(pl.multiple_of(x * 8, 8), 8), :]
        out_ref[x, 0:64, :] = total[i * ROWS : i * ROWS + 64]
        out_ref[x, 64:72, :] = total[i * ROWS + 64 : i * ROWS + 72] + strip


def forward_kernel(data_ref, to_kz_ref, to_ky_ref, out_ref, leave):
    lane = lax.broadcasted_iota(jnp.int32, (1, 128), 1)
    row = lax.broadcasted_iota(jnp.int32, (8, 128), 0)
    lower = lane < 64
    parts = []
    for x in range(2):
        planes = []
        for iz in range(2):
            pieces = []
            for iy in range(4):
                rim = jnp.where(row < HALO, data_ref[iz * 4 + (iy + 3) % 4, x, 64:72, :], 0.0)
                pieces.append(data_ref[iz * 4 + iy, x, 0:8, :] + rim)
                pieces.append(data_ref[iz * 4 + iy, x, 8:64, :])
            planes.append(jnp.concatenate(pieces, axis=0))
        rims = []
        for iz in range(2):
            tiles = [data_ref[iz * 4 + iy, x, 64:72, :] for iy in range(4)]
            turned = [pltpu.roll(tiles[1], 64, 1), pltpu.roll(tiles[3], 64, 1)]
            first = tiles[0] + jnp.where(lower, turned[1], turned[0])
            second = tiles[2] + jnp.where(lower, turned[0], turned[1])
            rims.append(jnp.concatenate([first, second], axis=1))
        rims = jnp.concatenate(rims + [jnp.zeros((112, 256), F32)], axis=0).T
        planes[1] = planes[1] + jnp.where(lane < HALO, pltpu.roll(rims, 125, 1), 0.0)
        planes[0] = planes[0] + jnp.where(lane < HALO, pltpu.roll(rims, 117, 1), 0.0)
        plane = jnp.concatenate(planes, axis=1)
        parts.append(dot3(halves(plane), (to_kz_ref[0], to_kz_ref[1])))
    rows = []
    for c in range(2):
        zero, one = (p[:, c * 128 : (c + 1) * 128] for p in parts)
        first = jnp.where(lower, zero, pltpu.roll(one, 64, 1))
        second = jnp.where(lower, pltpu.roll(zero, 64, 1), one)
        rows.append(jnp.concatenate([first, second], axis=1))
    both = halves(jnp.concatenate(rows, axis=0))
    for half in range(2):
        out = dot3(part_of(to_ky_ref, slice(half * 256, half * 256 + 256)), both)
        flat = out_ref.reshape(2, 512, 128)
        flat[half, 0:256] = out[:, :128]
        flat[half, 256:512] = out[:, 128:]
        leave(half)


def fill_green(of_x_ref, of_z_ref, of_y_ref, green_ref):
    ix, iy, iz = block_index()
    mine = ix * COLUMN + plane_of(iz, iy)
    half, group = mine // 64, mine % 64
    of_z = of_z_ref[half]
    scale_xz = of_x_ref[0] * of_z[0:1]
    square_xz = of_x_ref[1] + of_z[1:2]
    for i in range(4):
        ky = group * 4 + i
        square = square_xz + of_y_ref[1, ky]
        green_ref[i] = jnp.where(
            square > 0.0, scale_xz * of_y_ref[0, ky] / jnp.maximum(square, 1.0), 0.0
        )


def middle_kernel(part, data_ref, to_kx_ref, from_kx_ref, twist_ref, green_ref, out_ref):
    lane = lax.broadcasted_iota(jnp.int32, (1, 128), 1)
    sign = jnp.where(lane < 64, 1.0, -1.0)
    flat = data_ref.reshape(2, 512, 128)
    both = jnp.concatenate(
        [
            jnp.concatenate([flat[part, pl.ds(c * 2 + i, 128, stride=4), :] for i in range(2)], axis=1)
            for c in range(2)
        ],
        axis=0,
    )
    out = dot3(part_of(to_kx_ref), halves(both))
    cos, sin = twist_ref[0], twist_ref[1]
    reals, imags = [], []
    for i in range(2):
        real = out[:128, i * 128 : (i + 1) * 128]
        imag = out[128:, i * 128 : (i + 1) * 128]
        real, imag = real * cos + imag * sin, imag * cos - real * sin
        real = real * sign + pltpu.roll(real, 64, 1)
        imag = imag * sign + pltpu.roll(imag, 64, 1)
        green = green_ref[part * 2 + i]
        real, imag = real * green, imag * green
        real = real * sign + pltpu.roll(real, 64, 1)
        imag = imag * sign + pltpu.roll(imag, 64, 1)
        real, imag = real * cos - imag * sin, imag * cos + real * sin
        reals.append(real)
        imags.append(imag)
    both = jnp.concatenate(
        [jnp.concatenate(reals, axis=1), jnp.concatenate(imags, axis=1)], axis=0
    )
    out = dot3(part_of(from_kx_ref), halves(both))
    flat = out_ref.reshape(2, 512, 128)
    for c in range(2):
        for i in range(2):
            flat[part, pl.ds(c * 2 + i, 128, stride=4), :] = out[c * 128 : (c + 1) * 128, i * 128 : (i + 1) * 128]


def backward_kernel(data_ref, from_ky_ref, from_kz_ref, out_ref, arrive, leave):
    lane = lax.broadcasted_iota(jnp.int32, (1, 128), 1)
    row = lax.broadcasted_iota(jnp.int32, (8, 128), 0)
    lower = lane < 64
    out = 0.0
    for half in range(2):
        arrive(half)
        flat = data_ref.reshape(2, 512, 128)
        both = jnp.concatenate([flat[half, 0:256], flat[half, 256:512]], axis=1)
        out = out + dot3(
            part_of(from_ky_ref, slice(None), slice(half * 256, half * 256 + 256)), halves(both)
        )
    tiles = [[], []]
    for c in range(2):
        first, second = out[c * 256 : (c + 1) * 256, :128], out[c * 256 : (c + 1) * 256, 128:]
        tiles[0].append(jnp.where(lower, first, pltpu.roll(second, 64, 1)))
        tiles[1].append(jnp.where(lower, pltpu.roll(first, 64, 1), second))
    for x in range(2):
        plane = dot3(halves(jnp.concatenate(tiles[x], axis=1)), part_of(from_kz_ref))
        turned = [plane[:, h * 128 : (h + 1) * 128].T[:8] for h in range(2)]
        for iz in range(2):
            near = plane[:, iz * 128 : (iz + 1) * 128]
            strips = (turned[1 - iz][:, :128], turned[1 - iz][:, 128:])
            rolled = [pltpu.roll(s, 64, 1) for s in strips]
            for iy in range(4):
                after = (iy + 1) % 4
                t = iy // 2
                if iy % 2 == 0:
                    strip = strips[t]
                else:
                    strip = jnp.where(lower, rolled[t], rolled[1 - t])
                out_ref[iz * 4 + iy, x, 0:64, :] = near[iy * 64 : iy * 64 + 64]
                out_ref[iz * 4 + iy, x, 64:72, :] = jnp.where(
                    row < HALO, near[after * 64 : after * 64 + 8], pltpu.roll(strip, HALO, 0)
                )
        leave(x)


WIDTH = 128
UNROLL = 4
ORDER_UP = ((0, 0), (0, 1), (1, 0), (1, 1), (3, 0), (3, 1), (2, 0), (2, 1))
EARLY = 6


def gather_rows(frac_ref, base_ref, rows_x_ref, both_x_ref, grads_y_ref, fold_z_ref):
    ix, iy, iz = block_index()
    rim_row = lax.broadcasted_iota(jnp.int32, (8, 1), 0)
    inside = (rim_row >= 3) & (rim_row < 6)

    def step(c, carry):
        at = pl.ds(pl.multiple_of(c * WIDTH, WIDTH), WIDTH)
        _, sx = spline_weights(frac_ref[0:1, at])
        _, sy = spline_weights(frac_ref[1:2, at])
        wz, sz = spline_weights(frac_ref[2:3, at])
        low_z = base_ref[2:3, at] - iz * CZ
        both_x_ref[c, 0:24] = rows_x_ref[:, at]
        both_x_ref[c, 24:48] = place(sx, base_ref[0:1, at] - ix * CX, 24)
        grads_y_ref[:, at] = place(sy, base_ref[1:2, at] - iy * CY, ROWS)
        high, low = halves(jnp.concatenate([place(wz, low_z, CZ), place(sz, low_z, CZ)], axis=1))
        fold_z_ref[c, 0:128] = high
        fold_z_ref[c, 128:256] = high
        fold_z_ref[c, 256:384] = low
        rim_low = low_z - (CZ - HALO)
        rims = jnp.concatenate([place(wz, rim_low, 8), place(sz, rim_low, 8)], axis=1)
        rims = jnp.where(inside, rims, 0.0)
        rest = rims - rims.astype(BF16).astype(F32)
        zeros = jnp.zeros((104, 2 * WIDTH), F32)
        fold_z_ref[c, 384:512] = jnp.concatenate([rims, rims, rest, zeros], axis=0).astype(BF16)
        return carry

    lax.fori_loop(0, frac_ref.shape[1] // WIDTH, step, 0)


def stage(pot_ref, layers):
    lane = lax.broadcasted_iota(jnp.int32, (1, 128), 1)
    strips = [layer[64:72] for layer in layers]
    blank = [jnp.zeros((128 - 8 * len(layers), 128), F32)] if len(layers) < 16 else []
    turned = jnp.concatenate(strips + blank, axis=0).T[:ROWS]
    for i, layer in enumerate(layers):
        high, low = halves(layer)
        at = pl.ds(i * ROWS, ROWS)
        pot_ref[at, 0:128] = high
        pot_ref[at, 128:256] = low
        pot_ref[at, 256:384] = high
        first, second, third = (pltpu.roll(turned, (128 + 8 * k - 8 * i) % 128, 1) for k in range(3))
        value = jnp.where(lane < 8, first, jnp.where(lane < 16, second, third))
        value = jnp.where(lane < 24, value, 0.0)
        rounded = value.astype(BF16).astype(F32)
        value = jnp.where((lane >= 8) & (lane < 16), value - rounded, rounded)
        pot_ref[at, 384:512] = value.astype(BF16)


def gather_part(cells, pot_ref, both_x_ref, rows_y_ref, grads_y_ref, fold_z_ref, finish):
    def one(c):
        at = pl.ds(pl.multiple_of(c * WIDTH, WIDTH), WIDTH)
        rows_y, grads_y = rows_y_ref[:, at], grads_y_ref[:, at]
        main = dot(pot_ref[0 : len(cells) * ROWS], fold_z_ref[c])
        force_x = force_y = force_z = 0.0
        for i, x in enumerate(cells):
            sum_x = sum_y = sum_z = 0.0
            for y in range(ROWS // 8):
                low = i * ROWS + y * 8
                plain, sloped = main[low : low + 8, :WIDTH], main[low : low + 8, WIDTH:]
                near = rows_y[y * 8 : y * 8 + 8]
                sum_x += plain * near
                sum_y += plain * grads_y[y * 8 : y * 8 + 8]
                sum_z += sloped * near
            rows_x, grads_x = both_x_ref[c, pl.ds(x, 1), :], both_x_ref[c, pl.ds(x + 24, 1), :]
            force_x += grads_x * sum_x
            force_y += rows_x * sum_y
            force_z += rows_x * sum_z
        finish(c, at, force_x, force_y, force_z)

    def step(i, carry):
        for u in range(UNROLL):
            one(i * UNROLL + u)
        return carry

    lax.fori_loop(0, fold_z_ref.shape[0] // UNROLL, step, 0)


def turn_tables(to_kz_ref, to_ky_ref, to_kx_ref, from_kz_ref, from_ky_ref, from_kx_ref):
    row = lax.broadcasted_iota(jnp.int32, (GRID, 1), 0)
    twice = jnp.where(lax.rem(row, GRID // 2) == 0, 1.0, 2.0)
    for part in range(2):
        from_kz_ref[part] = (to_kz_ref[part].T.astype(F32) * twice).astype(BF16)
        from_ky_ref[part] = to_ky_ref[part].T
        from_kx_ref[part] = to_kx_ref[part].T


MESH = pl.DeviceIdType.MESH
INPUTS = ("charges", "fractions", "base_cells")
SMALL = ("counts", "of_y")
NAMES = ("to_kz", "to_ky", "to_kx", "twist", "of_x", "of_z")


FAR = sorted(
    ((a, b) for a in range(4) for b in range(4) if a or b),
    key=lambda o: -(min(o[0], 4 - o[0]) + min(o[1], 4 - o[1])),
)


def drain(ref, sem):
    pltpu.make_async_copy(ref, ref, sem).wait()


def fused_kernel(*refs):
    total = len(INPUTS) + len(SMALL) + len(NAMES)
    hbm, out_ref, refs = refs[:total], refs[total], refs[total + 1 :]
    local, refs = refs[:total], refs[total:]
    (rows_x_ref, rows_y_ref, both_z_ref, strips_ref, both_y_ref, high_ref, low_ref, grid_ref, rim_in_ref, planes_ref,
     send_ref, modes_ref, send2_ref, modes2_ref, blocks_ref, near_ref, far_ref, part_ref, pot_ref,
     both_x_ref, grads_y_ref, fold_z_ref, green_ref, from_kz_ref, from_ky_ref, from_kx_ref,
     load_sem, rim_send, rim_recv, a_send, a_recv, c_send, c_recv, d_send, d_recv,
     b_send, b_recv, e_send, e_recv) = refs
    loads = [pltpu.make_async_copy(h, v, load_sem.at[i]) for i, (h, v) in enumerate(zip(hbm, local))]
    first = len(INPUTS) + len(SMALL)
    for load in loads[:first]:
        load.start()
    charges_ref, frac_ref, base_ref, counts_ref, of_y_ref = local[:first]
    t = dict(zip(NAMES, local[first:]))
    ix, iy, iz = block_index()
    count_x = lax.axis_size("gx")
    block = iz * 4 + iy
    plane = plane_of(iz, iy)
    mine = ix * COLUMN + plane
    after = {"gx": lax.rem(ix + 1, count_x)}
    before = {"gx": lax.rem(ix + count_x - 1, count_x)}
    core, height = lax.rem(iy, 2), lax.div(iy, 2) * 2 + iz
    others = []
    for up, flip in ((2, 0), (2, 1), (1, 0), (1, 1), (3, 0), (3, 1), (0, 1), (0, 0)):
        to = lax.rem(core + flip, 2) * 4 + lax.rem(height + up, 4)
        others.append((to, holder_of(to)))

    barrier = pltpu.get_barrier_semaphore()

    def everyone(action):
        def row(_, steps):
            along, across = lax.rem(steps, 4), lax.rem(lax.div(steps, 4), 4)
            to_x = lax.rem(lax.div(ix, 4) + along, 4) * 4 + lax.rem(lax.rem(ix, 4) + across, 4)
            for to, where in others:
                action(to_x * COLUMN + to, {"gx": to_x, **where})
            return lax.div(steps, 16)

        for part in (FAR[:7], FAR[7:]):
            steps = sum((a + 4 * b) << (4 * i) for i, (a, b) in enumerate(part))
            lax.fori_loop(0, len(part), row, jnp.int32(steps))
        for to, where in others[:-1]:
            action(ix * COLUMN + to, where)

    def greet(to, where):
        pl.semaphore_signal(barrier, inc=1, device_id=where, device_id_type=MESH)

    with jax.named_scope("greet"):
        for a, b in FAR:
            to_x = lax.rem(lax.div(ix, 4) + a, 4) * 4 + lax.rem(lax.rem(ix, 4) + b, 4)
            for _, where in others:
                greet(None, {"gx": to_x, **where})
        for _, where in others[:-1]:
            greet(None, where)
    with jax.named_scope("load"):
        for load in loads[:first]:
            load.wait()
        for load in loads[first:]:
            load.start()
    spread = (rows_x_ref, rows_y_ref, both_z_ref, strips_ref)
    with jax.named_scope("rows"):
        spread_rows(
            counts_ref, charges_ref, frac_ref, base_ref, *spread, both_y_ref, high_ref, low_ref
        )
    with jax.named_scope("spread4"):
        spread_group(4, *spread, high_ref, low_ref, grid_ref)
    def give(to):
        @pl.when(to != plane)
        def _():
            pltpu.make_async_remote_copy(
                src_ref=grid_ref.at[pl.ds(2 * to, 2)], dst_ref=planes_ref.at[block],
                send_sem=a_send.at[to], recv_sem=a_recv.at[block],
                device_id=holder_of(to), device_id_type=MESH,
            ).start()

    def group_at(i):
        return 1 + lax.rem(i + plane, 3)

    with jax.named_scope("spread1"):
        spread_group(group_at(0), *spread, high_ref, low_ref, grid_ref)
    with jax.named_scope("barwait"):
        pl.semaphore_wait(barrier, 127)
    rims = [
        pltpu.make_async_remote_copy(
            src_ref=grid_ref.at[pl.ds(CX + i, n)], dst_ref=rim_in_ref.at[pl.ds(i, n)],
            send_sem=rim_send.at[i], recv_sem=rim_recv.at[i], device_id=after, device_id_type=MESH,
        )
        for i, n in ((0, 2), (2, 1))
    ]
    for rim in rims:
        rim.start()
    give(2 * group_at(0))
    give(2 * group_at(0) + 1)

    def some(i, carry):
        group = group_at(i)
        spread_group(group, *spread, high_ref, low_ref, grid_ref)
        give(2 * group)
        give(2 * group + 1)
        return carry

    with jax.named_scope("spread23"):
        lax.fori_loop(1, 3, some, 0)
    with jax.named_scope("spread0"):
        spread_group(0, *spread, high_ref, low_ref, grid_ref)
    with jax.named_scope("rimwait"):
        rims[0].wait_recv()
    grid_ref[0:2] += rim_in_ref[0:2]
    give(0)
    rims[1].wait_recv()
    grid_ref[2] += rim_in_ref[2]
    give(1)
    planes_ref[pl.ds(block, 1)] = grid_ref[pl.ds(2 * plane, 2)].reshape(1, 2, ROWS, CZ)
    with jax.named_scope("await"):
        for load in loads[first:]:
            load.wait()
        for b in range(COLUMN):
            pl.when(b != block)(functools.partial(drain, planes_ref.at[b], a_recv.at[b]))

    def spray(source, target, send_sem, recv_sem, half):
        def one(to, where):
            pltpu.make_async_remote_copy(
                src_ref=source.at[half, to], dst_ref=target.at[half, mine], send_sem=send_sem.at[half],
                recv_sem=recv_sem.at[half], device_id=where, device_id_type=MESH,
            ).start()

        with jax.named_scope("send"):
            everyone(one)
        target[half, pl.ds(mine, 1)] = source[half, pl.ds(mine, 1)]

    def arrive(target, recv_sem, half):
        with jax.named_scope("arrive"):
            drain(target.at[half, pl.ds(0, 127)], recv_sem.at[half])

    forward_kernel(
        planes_ref, t["to_kz"], t["to_ky"], send_ref,
        functools.partial(spray, send_ref, modes_ref, c_send, c_recv),
    )
    with jax.named_scope("turn"):
        fill_green(t["of_x"], t["of_z"], of_y_ref, green_ref)
        turn_tables(t["to_kz"], t["to_ky"], t["to_kx"], from_kz_ref, from_ky_ref, from_kx_ref)
    for half in range(2):
        arrive(modes_ref, c_recv, half)
        with jax.named_scope("middle"):
            middle_kernel(
                half, modes_ref, t["to_kx"], from_kx_ref, t["twist"], green_ref, send2_ref
            )
        spray(send2_ref, modes2_ref, d_send, d_recv, half)
    with jax.named_scope("gather_rows"):
        gather_rows(frac_ref, base_ref, rows_x_ref, both_x_ref, grads_y_ref, fold_z_ref)
    def give_back(x):
        for slot in range(1, COLUMN if x else EARLY):
            up, flip = ORDER_UP[slot]
            to = lax.rem(core + flip, 2) * 4 + lax.rem(height + up, 4)
            where = holder_of(to)
            source = blocks_ref.at[where["gz"] * 4 + where["gy"]]
            target = near_ref.at[ORDER_UP.index(((4 - up) % 4, flip))]
            if slot < EARLY:
                source, target = source.at[x], target.at[x]
            pltpu.make_async_remote_copy(
                src_ref=source, dst_ref=target, send_sem=b_send.at[slot],
                recv_sem=b_recv.at[ORDER_UP.index(((4 - up) % 4, flip))], device_id=where, device_id_type=MESH,
            ).start()

    backward_kernel(
        modes2_ref, from_ky_ref, from_kz_ref, blocks_ref, functools.partial(arrive, modes2_ref, d_recv),
        give_back,
    )
    near_ref[0] = blocks_ref[block]
    slot_cells = []
    for up, flip in ORDER_UP:
        x = 2 * (lax.rem(core + flip, 2) * 4 + lax.rem(height + up, 4))
        slot_cells += [x, x + 1]

    def slot_of(low_plane):
        up = lax.rem(low_plane - height + 4, 4)
        return jnp.where(up < 2, 2 * up, 10 - 2 * up) + core

    rims_back = []
    for low_plane, layers in ((0, 2), (1, 1)):
        slot = slot_of(low_plane)
        rims_back.append((slot, pltpu.make_async_remote_copy(
            src_ref=near_ref.at[slot, pl.ds(0, layers)], dst_ref=far_ref.at[pl.ds(2 * low_plane, layers)],
            send_sem=e_send.at[low_plane], recv_sem=e_recv.at[low_plane],
            device_id=before, device_id_type=MESH,
        )))
    tools = (both_x_ref, rows_y_ref, grads_y_ref, fold_z_ref)

    def keep(c, at, *forces):
        for d, force in enumerate(forces):
            part_ref[d, :, at] = force

    def add(c, at, *forces):
        for d, force in enumerate(forces):
            part_ref[d, :, at] += force

    def finish(c, at, *forces):
        slot = lax.broadcasted_iota(jnp.int32, (1, WIDTH), 1) + c * WIDTH
        charge = jnp.where(slot < counts_ref[0, 0, 0], charges_ref[:, at], 0.0)
        total = [
            jnp.sum(part_ref[d, :, at] + force, axis=0, keepdims=True) for d, force in enumerate(forces)
        ]
        out_ref[:, at] = -charge * jnp.concatenate(total, axis=0)

    def gather_slots(first, last, more, done):
        layers = [near_ref[slot, i] for slot in range(first, last) for i in range(2)]
        layers += [far_ref[i] for i in range(more)]
        stage(pot_ref, layers)
        cells = slot_cells[2 * first : 2 * last] + [CX + i for i in range(more)]
        gather_part(cells, pot_ref, *tools, done)

    with jax.named_scope("bwait1"):
        drain(near_ref.at[1], b_recv.at[1])
    with jax.named_scope("gather1"):
        gather_slots(0, 2, 0, keep)
    with jax.named_scope("bwait2"):
        for slot in range(2, EARLY):
            drain(near_ref.at[slot], b_recv.at[slot])
        for slot, copy in rims_back:
            pl.when(slot < EARLY)(copy.start)
    with jax.named_scope("gather2"):
        gather_slots(2, EARLY, 0, add)
    with jax.named_scope("bwait3"):
        for slot in range(EARLY, COLUMN):
            drain(near_ref.at[slot], b_recv.at[slot])
        for slot, copy in rims_back:
            pl.when(slot >= EARLY)(copy.start)
    with jax.named_scope("sendwait"):
        for rim in rims:
            rim.wait_send()
        for o in range(COLUMN):
            @pl.when(o != plane)
            def _():
                drain(grid_ref.at[pl.ds(2 * o, 2)], a_send.at[o])

        for half in range(2):
            drain(send_ref.at[half, pl.ds(0, 127)], c_send.at[half])
            drain(send2_ref.at[half, pl.ds(0, 127)], d_send.at[half])
        for slot in range(1, COLUMN):
            drain(blocks_ref.at[slot], b_send.at[slot])

    def rims_home():
        with jax.named_scope("ewait"):
            for _, copy in rims_back:
                copy.wait_recv()

    @pl.when(height < 2)
    def _():
        rims_home()
        gather_slots(EARLY, COLUMN, HALO, finish)

    @pl.when(height >= 2)
    def _():
        gather_slots(EARLY, COLUMN, 0, add)
        rims_home()
        gather_slots(0, 0, HALO, finish)

    for _, copy in rims_back:
        copy.wait_send()


def per_device(charges, fractions, base_cells, counts):
    t = {name: jnp.asarray(value) for name, value in tables().items()}
    arrays = [charges.reshape(1, -1), fractions, base_cells, counts, t["of_y"]]
    arrays += [t[name] for name in NAMES]
    small = len(INPUTS) + len(SMALL)
    atoms = fractions.shape[1]
    dma = pltpu.SemaphoreType.DMA
    scratch = [
        (pltpu.SMEM if len(INPUTS) <= i < small else pltpu.VMEM)(a.shape, a.dtype)
        for i, a in enumerate(arrays)
    ]
    scratch += [
        pltpu.VMEM((24, atoms), F32),
        pltpu.VMEM((ROWS, atoms), F32),
        pltpu.VMEM((2 * CZ, atoms), BF16),
        pltpu.VMEM((160, CZ), F32),
        pltpu.VMEM((2 * ROWS, atoms), BF16),
        pltpu.VMEM((4 * ROWS, atoms), BF16),
        pltpu.VMEM((4 * ROWS, atoms), BF16),
        pltpu.VMEM((20, ROWS, CZ), F32),
        pltpu.VMEM((HALO, ROWS, CZ), F32),
        pltpu.VMEM((COLUMN, 2, ROWS, CZ), F32),
        pltpu.VMEM((2, 128, 4, 128), F32),
        pltpu.VMEM((2, 128, 4, 128), F32),
        pltpu.VMEM((2, 128, 4, 128), F32),
        pltpu.VMEM((2, 128, 4, 128), F32),
        pltpu.VMEM((COLUMN, 2, ROWS, CZ), F32),
        pltpu.VMEM((COLUMN, 2, ROWS, CZ), F32),
        pltpu.VMEM((HALO, ROWS, CZ), F32),
        pltpu.VMEM((3, 8, atoms), F32),
        pltpu.VMEM((2 * EARLY * ROWS, 512), BF16),
        pltpu.VMEM((atoms // WIDTH, 48, WIDTH), F32),
        pltpu.VMEM((ROWS, atoms), F32),
        pltpu.VMEM((atoms // WIDTH, 512, 2 * WIDTH), BF16),
        pltpu.VMEM((4, 128, 128), F32),
        pltpu.VMEM(t["to_kz"].shape, BF16),
        pltpu.VMEM(t["to_ky"].shape, BF16),
        pltpu.VMEM(t["to_kx"].shape, BF16),
        dma((len(arrays),)), dma((HALO,)), dma((HALO,)), dma((COLUMN,)), dma((COLUMN,)), dma((2,)), dma((2,)), dma((2,)), dma((2,)),
        dma((COLUMN,)), dma((COLUMN,)), dma((2,)), dma((2,)),
    ]
    return pl.pallas_call(
        fused_kernel,
        out_shape=jax.ShapeDtypeStruct(fractions.shape, F32),
        in_specs=[pl.BlockSpec(memory_space=pltpu.HBM)] * len(arrays),
        out_specs=pl.BlockSpec(memory_space=pltpu.VMEM),
        scratch_shapes=scratch,
        compiler_params=pltpu.CompilerParams(
            collective_id=0, has_side_effects=True, vmem_limit_bytes=62 << 20
        ),
    )(*arrays)


def solution(mesh):
    split = ("gz", "gy", "gx")
    return jax.shard_map(
        per_device,
        mesh=mesh,
        in_specs=(P(split), P(None, split), P(None, split), P("gz", "gy", "gx")),
        out_specs=P(None, split),
        check_vma=False,
    )
```

```python
import functools

import jax
import jax.numpy as jnp
import numpy as np
from jax import lax
from jax.experimental import pallas as pl
from jax.experimental.pallas import tpu as pltpu
from jax.sharding import PartitionSpec as P

GRID = 256
ORDER = 4
HALO = ORDER - 1
COULOMB = 332.0636
EWALD = 0.7
CX, CY, CZ = 16, 64, 128
ROWS = 72
SPAN = CX + HALO
COLUMN = 8
F32 = jnp.float32
BF16 = jnp.bfloat16
NN = (((1,), (0,)), ((), ()))
NT = (((1,), (1,)), ((), ()))


def split_np(a):
    a = np.asarray(a, np.float32)
    high = a.astype(jnp.bfloat16)
    low = (a - high.astype(np.float32)).astype(jnp.bfloat16)
    return np.stack([high, low])


def tables():
    k = np.arange(GRID)
    half = np.arange(GRID // 2)

    def turn(first, second, length):
        angle = (first[:, None] * second[None, :] % length) * (2.0 * np.pi / length)
        return np.cos(angle), np.sin(angle)

    cos, sin = turn(k, half, GRID)
    to_kz = np.concatenate([cos, -sin], axis=1)
    cos, sin = turn(k, k, GRID)
    real = np.concatenate([cos, sin], axis=1).reshape(64, 2, 2, 512)
    imag = np.concatenate([-sin, cos], axis=1).reshape(64, 2, 2, 512)
    to_ky = np.stack([real, imag], axis=2).swapaxes(0, 1).reshape(512, 512)
    cos, sin = turn(half, half, GRID // 2)
    to_kx = np.concatenate(
        [np.concatenate([cos, sin], axis=1), np.concatenate([-sin, cos], axis=1)], axis=0
    )
    angle = half[:, None] * (2.0 * np.pi / GRID) * np.ones((1, 128))
    upper = np.arange(128)[None, :] >= 64
    twist = np.stack([np.where(upper, np.cos(angle), 1.0), np.where(upper, np.sin(angle), 0.0)])
    signed = np.where(2 * k < GRID, k, k - GRID).astype(np.float64)
    spline = 36.0 / (4.0 + 2.0 * np.cos(k * (2.0 * np.pi / GRID))) ** 2
    spline[GRID // 2] = 0.0
    decay = spline * np.exp(-np.pi**2 * signed**2 / (EWALD**2 * GRID**2))
    lanes = np.arange(128)
    kx = half[:, None] + 128 * (lanes[None, :] // 64)
    of_x = np.stack([decay[kx] * (COULOMB / (np.pi * GRID)), signed[kx] ** 2])
    kz = 64 * np.arange(2)[:, None] + lanes[None, :] % 64
    of_z = np.stack([decay[kz], signed[kz] ** 2], axis=1)
    of_y = np.stack([decay, signed**2])
    return dict(
        to_kz=split_np(to_kz),
        to_ky=split_np(to_ky),
        to_kx=split_np(to_kx),
        twist=twist.astype(np.float32),
        of_x=of_x.astype(np.float32),
        of_y=of_y.astype(np.float32),
        of_z=of_z.astype(np.float32),
    )


def halves(value):
    high = value.astype(BF16)
    return high, (value - high.astype(F32)).astype(BF16)


def dot(a, b, dims=NN):
    return lax.dot_general(a, b, dims, preferred_element_type=F32)


def dot3(a, b):
    return dot(
        jnp.concatenate([a[0], a[1], a[0]], axis=1), jnp.concatenate([b[0], b[0], b[1]], axis=0)
    )


def part_of(ref, *at):
    return ref[(0, *at)], ref[(1, *at)]


def spline_weights(t):
    rest = 1.0 - t
    square = t * t
    cube = square * t
    weights = (
        rest * rest * rest / 6.0,
        (3.0 * cube - 6.0 * square + 4.0) / 6.0,
        (-3.0 * cube + 3.0 * square + 3.0 * t + 1.0) / 6.0,
        cube / 6.0,
    )
    slopes = (-0.5 * rest * rest, 1.5 * square - 2.0 * t, -1.5 * square + t + 0.5, 0.5 * square)
    return weights, slopes


def place(values, lowest, rows):
    offset = lax.broadcasted_iota(jnp.int32, (rows, lowest.shape[1]), 0) - lowest
    out = jnp.where(offset == 3, values[3], 0.0)
    for i in (2, 1, 0):
        out = jnp.where(offset == i, values[i], out)
    return out


def block_index():
    return lax.axis_index("gx"), lax.axis_index("gy"), lax.axis_index("gz")


def plane_of(iz, iy):
    return lax.rem(iy, 2) * 4 + lax.div(iy, 2) * 2 + iz


def holder_of(plane):
    return {"gz": lax.rem(plane, 2), "gy": lax.rem(lax.div(plane, 2), 2) * 2 + lax.div(plane, 4)}


def spread_rows(counts_ref, charges_ref, frac_ref, base_ref, rows_x_ref, rows_y_ref, both_z_ref, strips_ref,
                both_y_ref, high_ref, low_ref):
    ix, iy, iz = block_index()
    width = 512
    rim_row = lax.broadcasted_iota(jnp.int32, (8, 1), 0)
    inside = (rim_row >= 3) & (rim_row < 6)

    for c in range(charges_ref.shape[1] // width):
        at = pl.ds(c * width, width)
        slot = lax.broadcasted_iota(jnp.int32, (1, width), 1) + c * width
        charge = jnp.where(slot < counts_ref[0, 0, 0], charges_ref[:, at], 0.0)
        wx, _ = spline_weights(frac_ref[0:1, at])
        wy, _ = spline_weights(frac_ref[1:2, at])
        wz, _ = spline_weights(frac_ref[2:3, at])
        wz = [w * charge for w in wz]
        low_z = base_ref[2:3, at] - iz * CZ
        rows_x = place(wx, base_ref[0:1, at] - ix * CX, 24)
        rows_x_ref[:, at] = rows_x
        rows_y = place(wy, base_ref[1:2, at] - iy * CY, ROWS)
        rows_y_ref[:, at] = rows_y
        high, low = halves(rows_y)
        both_y_ref[0:ROWS, at] = high
        both_y_ref[ROWS : 2 * ROWS, at] = low
        high, low = halves(place(wz, low_z, CZ))
        both_z_ref[0:CZ, at] = high
        both_z_ref[CZ : 2 * CZ, at] = low
        rim_z = jnp.where(inside, place(wz, low_z - (CZ - HALO), 8), 0.0)
        high, low = halves(jnp.concatenate([rows_x[x : x + 1] * rim_z for x in range(20)], axis=0))
        high_ref[0:160, at] = high
        low_ref[0:160, at] = low
    pad = jnp.zeros((256 - 2 * ROWS, both_y_ref.shape[1]), BF16)
    total = dot(high_ref[0:160], jnp.concatenate([both_y_ref[...], pad], axis=0), NT)
    pad = jnp.zeros((CZ - ROWS, both_y_ref.shape[1]), BF16)
    more = dot(low_ref[0:160], jnp.concatenate([both_y_ref[0:ROWS], pad], axis=0), NT)
    strips_ref[...] = jnp.concatenate(
        [total[:, :ROWS] + total[:, ROWS : 2 * ROWS], jnp.zeros((160, CZ - ROWS), F32)], axis=1
    ) + more


def spread_group(group, rows_x_ref, rows_y_ref, both_z_ref, strips_ref, high_ref, low_ref, out_ref):
    for i in range(4):
        high, low = halves(rows_x_ref[pl.ds(group * 4 + i, 1), :] * rows_y_ref[...])
        high_ref[pl.ds(i * ROWS, ROWS), :] = high
        low_ref[pl.ds(i * ROWS, ROWS), :] = low
    total = dot(high_ref[...], both_z_ref[...], NT)
    total = total[:, :CZ] + total[:, CZ:] + dot(low_ref[...], both_z_ref[0:CZ], NT)
    for i in range(4):
        x = group * 4 + i
        strip = strips_ref[pl.ds(pl.multiple_of(x * 8, 8), 8), :]
        out_ref[x, 0:64, :] = total[i * ROWS : i * ROWS + 64]
        out_ref[x, 64:72, :] = total[i * ROWS + 64 : i * ROWS + 72] + strip


def forward_kernel(data_ref, to_kz_ref, to_ky_ref, out_ref, leave):
    lane = lax.broadcasted_iota(jnp.int32, (1, 128), 1)
    row = lax.broadcasted_iota(jnp.int32, (8, 128), 0)
    lower = lane < 64
    parts = []
    for x in range(2):
        planes = []
        for iz in range(2):
            pieces = []
            for iy in range(4):
                rim = jnp.where(row < HALO, data_ref[iz * 4 + (iy + 3) % 4, x, 64:72, :], 0.0)
                pieces.append(data_ref[iz * 4 + iy, x, 0:8, :] + rim)
                pieces.append(data_ref[iz * 4 + iy, x, 8:64, :])
            planes.append(jnp.concatenate(pieces, axis=0))
        rims = []
        for iz in range(2):
            tiles = [data_ref[iz * 4 + iy, x, 64:72, :] for iy in range(4)]
            turned = [pltpu.roll(tiles[1], 64, 1), pltpu.roll(tiles[3], 64, 1)]
            first = tiles[0] + jnp.where(lower, turned[1], turned[0])
            second = tiles[2] + jnp.where(lower, turned[0], turned[1])
            rims.append(jnp.concatenate([first, second], axis=1))
        rims = jnp.concatenate(rims + [jnp.zeros((112, 256), F32)], axis=0).T
        planes[1] = planes[1] + jnp.where(lane < HALO, pltpu.roll(rims, 125, 1), 0.0)
        planes[0] = planes[0] + jnp.where(lane < HALO, pltpu.roll(rims, 117, 1), 0.0)
        plane = jnp.concatenate(planes, axis=1)
        parts.append(dot3(halves(plane), (to_kz_ref[0], to_kz_ref[1])))
    rows = []
    for c in range(2):
        zero, one = (p[:, c * 128 : (c + 1) * 128] for p in parts)
        first = jnp.where(lower, zero, pltpu.roll(one, 64, 1))
        second = jnp.where(lower, pltpu.roll(zero, 64, 1), one)
        rows.append(jnp.concatenate([first, second], axis=1))
    both = halves(jnp.concatenate(rows, axis=0))
    for half in range(2):
        out = dot3(part_of(to_ky_ref, slice(half * 256, half * 256 + 256)), both)
        flat = out_ref.reshape(2, 512, 128)
        flat[half, 0:256] = out[:, :128]
        flat[half, 256:512] = out[:, 128:]
        leave(half)


def fill_green(of_x_ref, of_z_ref, of_y_ref, green_ref):
    ix, iy, iz = block_index()
    mine = ix * COLUMN + plane_of(iz, iy)
    half, group = mine // 64, mine % 64
    of_z = of_z_ref[half]
    scale_xz = of_x_ref[0] * of_z[0:1]
    square_xz = of_x_ref[1] + of_z[1:2]
    for i in range(4):
        ky = group * 4 + i
        square = square_xz + of_y_ref[1, ky]
        green_ref[i] = jnp.where(
            square > 0.0, scale_xz * of_y_ref[0, ky] / jnp.maximum(square, 1.0), 0.0
        )


def middle_kernel(part, data_ref, to_kx_ref, from_kx_ref, twist_ref, green_ref, out_ref):
    lane = lax.broadcasted_iota(jnp.int32, (1, 128), 1)
    sign = jnp.where(lane < 64, 1.0, -1.0)
    flat = data_ref.reshape(2, 512, 128)
    both = jnp.concatenate(
        [
            jnp.concatenate([flat[part, pl.ds(c * 2 + i, 128, stride=4), :] for i in range(2)], axis=1)
            for c in range(2)
        ],
        axis=0,
    )
    out = dot3(part_of(to_kx_ref), halves(both))
    cos, sin = twist_ref[0], twist_ref[1]
    reals, imags = [], []
    for i in range(2):
        real = out[:128, i * 128 : (i + 1) * 128]
        imag = out[128:, i * 128 : (i + 1) * 128]
        real, imag = real * cos + imag * sin, imag * cos - real * sin
        real = real * sign + pltpu.roll(real, 64, 1)
        imag = imag * sign + pltpu.roll(imag, 64, 1)
        green = green_ref[part * 2 + i]
        real, imag = real * green, imag * green
        real = real * sign + pltpu.roll(real, 64, 1)
        imag = imag * sign + pltpu.roll(imag, 64, 1)
        real, imag = real * cos - imag * sin, imag * cos + real * sin
        reals.append(real)
        imags.append(imag)
    both = jnp.concatenate(
        [jnp.concatenate(reals, axis=1), jnp.concatenate(imags, axis=1)], axis=0
    )
    out = dot3(part_of(from_kx_ref), halves(both))
    flat = out_ref.reshape(2, 512, 128)
    for c in range(2):
        for i in range(2):
            flat[part, pl.ds(c * 2 + i, 128, stride=4), :] = out[c * 128 : (c + 1) * 128, i * 128 : (i + 1) * 128]


def backward_kernel(data_ref, from_ky_ref, from_kz_ref, out_ref, arrive, leave):
    lane = lax.broadcasted_iota(jnp.int32, (1, 128), 1)
    row = lax.broadcasted_iota(jnp.int32, (8, 128), 0)
    lower = lane < 64
    out = 0.0
    for half in range(2):
        arrive(half)
        flat = data_ref.reshape(2, 512, 128)
        both = jnp.concatenate([flat[half, 0:256], flat[half, 256:512]], axis=1)
        out = out + dot3(
            part_of(from_ky_ref, slice(None), slice(half * 256, half * 256 + 256)), halves(both)
        )
    tiles = [[], []]
    for c in range(2):
        first, second = out[c * 256 : (c + 1) * 256, :128], out[c * 256 : (c + 1) * 256, 128:]
        tiles[0].append(jnp.where(lower, first, pltpu.roll(second, 64, 1)))
        tiles[1].append(jnp.where(lower, pltpu.roll(first, 64, 1), second))
    for x in range(2):
        plane = dot3(halves(jnp.concatenate(tiles[x], axis=1)), part_of(from_kz_ref))
        turned = [plane[:, h * 128 : (h + 1) * 128].T[:8] for h in range(2)]
        for iz in range(2):
            near = plane[:, iz * 128 : (iz + 1) * 128]
            strips = (turned[1 - iz][:, :128], turned[1 - iz][:, 128:])
            rolled = [pltpu.roll(s, 64, 1) for s in strips]
            for iy in range(4):
                after = (iy + 1) % 4
                t = iy // 2
                if iy % 2 == 0:
                    strip = strips[t]
                else:
                    strip = jnp.where(lower, rolled[t], rolled[1 - t])
                out_ref[iz * 4 + iy, x, 0:64, :] = near[iy * 64 : iy * 64 + 64]
                out_ref[iz * 4 + iy, x, 64:72, :] = jnp.where(
                    row < HALO, near[after * 64 : after * 64 + 8], pltpu.roll(strip, HALO, 0)
                )
        leave(x)


WIDTH = 128
UNROLL = 16
ORDER_UP = ((0, 0), (0, 1), (1, 0), (1, 1), (3, 0), (3, 1), (2, 0), (2, 1))
EARLY = 6


def gather_rows(frac_ref, base_ref, rows_x_ref, both_x_ref, grads_y_ref, fold_z_ref):
    ix, iy, iz = block_index()
    rim_row = lax.broadcasted_iota(jnp.int32, (8, 1), 0)
    inside = (rim_row >= 3) & (rim_row < 6)

    def step(c, carry):
        at = pl.ds(pl.multiple_of(c * WIDTH, WIDTH), WIDTH)
        _, sx = spline_weights(frac_ref[0:1, at])
        _, sy = spline_weights(frac_ref[1:2, at])
        wz, sz = spline_weights(frac_ref[2:3, at])
        low_z = base_ref[2:3, at] - iz * CZ
        both_x_ref[c, 0:24] = rows_x_ref[:, at]
        both_x_ref[c, 24:48] = place(sx, base_ref[0:1, at] - ix * CX, 24)
        grads_y_ref[:, at] = place(sy, base_ref[1:2, at] - iy * CY, ROWS)
        high, low = halves(jnp.concatenate([place(wz, low_z, CZ), place(sz, low_z, CZ)], axis=1))
        fold_z_ref[c, 0:128] = high
        fold_z_ref[c, 128:256] = high
        fold_z_ref[c, 256:384] = low
        rim_low = low_z - (CZ - HALO)
        rims = jnp.concatenate([place(wz, rim_low, 8), place(sz, rim_low, 8)], axis=1)
        rims = jnp.where(inside, rims, 0.0)
        rest = rims - rims.astype(BF16).astype(F32)
        zeros = jnp.zeros((104, 2 * WIDTH), F32)
        fold_z_ref[c, 384:512] = jnp.concatenate([rims, rims, rest, zeros], axis=0).astype(BF16)
        return carry

    lax.fori_loop(0, frac_ref.shape[1] // WIDTH, step, 0)


def stage(pot_ref, layers):
    lane = lax.broadcasted_iota(jnp.int32, (1, 128), 1)
    strips = [layer[64:72] for layer in layers]
    blank = [jnp.zeros((128 - 8 * len(layers), 128), F32)] if len(layers) < 16 else []
    turned = jnp.concatenate(strips + blank, axis=0).T[:ROWS]
    for i, layer in enumerate(layers):
        high, low = halves(layer)
        at = pl.ds(i * ROWS, ROWS)
        pot_ref[at, 0:128] = high
        pot_ref[at, 128:256] = low
        pot_ref[at, 256:384] = high
        first, second, third = (pltpu.roll(turned, (128 + 8 * k - 8 * i) % 128, 1) for k in range(3))
        value = jnp.where(lane < 8, first, jnp.where(lane < 16, second, third))
        value = jnp.where(lane < 24, value, 0.0)
        rounded = value.astype(BF16).astype(F32)
        value = jnp.where((lane >= 8) & (lane < 16), value - rounded, rounded)
        pot_ref[at, 384:512] = value.astype(BF16)


def gather_part(cells, pot_ref, both_x_ref, rows_y_ref, grads_y_ref, fold_z_ref, finish):
    def one(c):
        at = pl.ds(pl.multiple_of(c * WIDTH, WIDTH), WIDTH)
        rows_y, grads_y = rows_y_ref[:, at], grads_y_ref[:, at]
        main = dot(pot_ref[0 : len(cells) * ROWS], fold_z_ref[c])
        force_x = force_y = force_z = 0.0
        for i, x in enumerate(cells):
            sum_x = sum_y = sum_z = 0.0
            for y in range(ROWS // 8):
                low = i * ROWS + y * 8
                plain, sloped = main[low : low + 8, :WIDTH], main[low : low + 8, WIDTH:]
                near = rows_y[y * 8 : y * 8 + 8]
                sum_x += plain * near
                sum_y += plain * grads_y[y * 8 : y * 8 + 8]
                sum_z += sloped * near
            rows_x, grads_x = both_x_ref[c, pl.ds(x, 1), :], both_x_ref[c, pl.ds(x + 24, 1), :]
            force_x += grads_x * sum_x
            force_y += rows_x * sum_y
            force_z += rows_x * sum_z
        finish(c, at, force_x, force_y, force_z)

    def step(i, carry):
        for u in range(UNROLL):
            one(i * UNROLL + u)
        return carry

    lax.fori_loop(0, fold_z_ref.shape[0] // UNROLL, step, 0)


def turn_tables(to_kz_ref, to_ky_ref, to_kx_ref, from_kz_ref, from_ky_ref, from_kx_ref):
    row = lax.broadcasted_iota(jnp.int32, (GRID, 1), 0)
    twice = jnp.where(lax.rem(row, GRID // 2) == 0, 1.0, 2.0)
    for part in range(2):
        from_kz_ref[part] = (to_kz_ref[part].T.astype(F32) * twice).astype(BF16)
        from_ky_ref[part] = to_ky_ref[part].T
        from_kx_ref[part] = to_kx_ref[part].T


MESH = pl.DeviceIdType.MESH
INPUTS = ("charges", "fractions", "base_cells")
SMALL = ("counts", "of_y")
NAMES = ("to_kz", "to_ky", "to_kx", "twist", "of_x", "of_z")


FAR = sorted(
    ((a, b) for a in range(4) for b in range(4) if a or b),
    key=lambda o: -(min(o[0], 4 - o[0]) + min(o[1], 4 - o[1])),
)


def drain(ref, sem):
    pltpu.make_async_copy(ref, ref, sem).wait()


def fused_kernel(*refs):
    total = len(INPUTS) + len(SMALL) + len(NAMES)
    hbm, out_ref, refs = refs[:total], refs[total], refs[total + 1 :]
    local, refs = refs[:total], refs[total:]
    (rows_x_ref, rows_y_ref, both_z_ref, strips_ref, both_y_ref, high_ref, low_ref, grid_ref, rim_in_ref, planes_ref,
     send_ref, modes_ref, send2_ref, modes2_ref, blocks_ref, near_ref, far_ref, part_ref, pot_ref,
     both_x_ref, grads_y_ref, fold_z_ref, green_ref, from_kz_ref, from_ky_ref, from_kx_ref,
     load_sem, rim_send, rim_recv, a_send, a_recv, c_send, c_recv, d_send, d_recv,
     b_send, b_recv, e_send, e_recv, direct_sem) = refs
    loads = [pltpu.make_async_copy(h, v, load_sem.at[i]) for i, (h, v) in enumerate(zip(hbm, local))]
    first = len(INPUTS) + len(SMALL)
    for load in loads[:first]:
        load.start()
    charges_ref, frac_ref, base_ref, counts_ref, of_y_ref = local[:first]
    t = dict(zip(NAMES, local[first:]))
    ix, iy, iz = block_index()
    count_x = lax.axis_size("gx")
    block = iz * 4 + iy
    plane = plane_of(iz, iy)
    mine = ix * COLUMN + plane
    after = {"gx": lax.rem(ix + 1, count_x)}
    before = {"gx": lax.rem(ix + count_x - 1, count_x)}
    core, height = lax.rem(iy, 2), lax.div(iy, 2) * 2 + iz
    others = []
    for up, flip in ((2, 0), (2, 1), (1, 0), (1, 1), (3, 0), (3, 1), (0, 1), (0, 0)):
        to = lax.rem(core + flip, 2) * 4 + lax.rem(height + up, 4)
        others.append((to, holder_of(to)))

    barrier = pltpu.get_barrier_semaphore()

    def everyone(action):
        def row(_, steps):
            along, across = lax.rem(steps, 4), lax.rem(lax.div(steps, 4), 4)
            to_x = lax.rem(lax.div(ix, 4) + along, 4) * 4 + lax.rem(lax.rem(ix, 4) + across, 4)
            for to, where in others:
                action(to_x * COLUMN + to, {"gx": to_x, **where})
            return lax.div(steps, 16)

        for part in (FAR[:7], FAR[7:]):
            steps = sum((a + 4 * b) << (4 * i) for i, (a, b) in enumerate(part))
            lax.fori_loop(0, len(part), row, jnp.int32(steps))
        for to, where in others[:-1]:
            action(ix * COLUMN + to, where)

    def greet(to, where):
        pl.semaphore_signal(barrier, inc=1, device_id=where, device_id_type=MESH)

    with jax.named_scope("greet"):
        for a, b in FAR:
            to_x = lax.rem(lax.div(ix, 4) + a, 4) * 4 + lax.rem(lax.rem(ix, 4) + b, 4)
            for _, where in others:
                greet(None, {"gx": to_x, **where})
        for _, where in others[:-1]:
            greet(None, where)
    with jax.named_scope("load"):
        for load in loads[:first]:
            load.wait()
        for load in loads[first:]:
            load.start()
    spread = (rows_x_ref, rows_y_ref, both_z_ref, strips_ref)
    with jax.named_scope("rows"):
        spread_rows(
            counts_ref, charges_ref, frac_ref, base_ref, *spread, both_y_ref, high_ref, low_ref
        )
    with jax.named_scope("spread4"):
        spread_group(4, *spread, high_ref, low_ref, grid_ref)
    def give(to):
        @pl.when(to != plane)
        def _():
            pltpu.make_async_remote_copy(
                src_ref=grid_ref.at[pl.ds(2 * to, 2)], dst_ref=planes_ref.at[block],
                send_sem=a_send.at[to], recv_sem=a_recv.at[block],
                device_id=holder_of(to), device_id_type=MESH,
            ).start()

    def give_layer(to, i):
        @pl.when(to != plane)
        def _():
            pltpu.make_async_remote_copy(
                src_ref=grid_ref.at[2 * to + i], dst_ref=planes_ref.at[block, i],
                send_sem=a_send.at[to], recv_sem=a_recv.at[block],
                device_id=holder_of(to), device_id_type=MESH,
            ).start()

    def group_at(i):
        return 1 + lax.rem(i + plane, 3)

    with jax.named_scope("spread1"):
        spread_group(group_at(0), *spread, high_ref, low_ref, grid_ref)
    with jax.named_scope("barwait"):
        pl.semaphore_wait(barrier, 127)
    rims = [
        pltpu.make_async_remote_copy(
            src_ref=grid_ref.at[CX + i], dst_ref=rim_in_ref.at[i],
            send_sem=rim_send.at[i], recv_sem=rim_recv.at[i], device_id=after, device_id_type=MESH,
        )
        for i in range(HALO)
    ]
    for rim in rims:
        rim.start()
    give(2 * group_at(0))
    give(2 * group_at(0) + 1)

    def some(i, carry):
        group = group_at(i)
        spread_group(group, *spread, high_ref, low_ref, grid_ref)
        give(2 * group)
        give(2 * group + 1)
        return carry

    with jax.named_scope("spread23"):
        lax.fori_loop(1, 3, some, 0)
    with jax.named_scope("spread0"):
        spread_group(0, *spread, high_ref, low_ref, grid_ref)
    give_layer(1, 1)
    for i in range(HALO):
        with jax.named_scope("rimwait"):
            rims[i].wait_recv()
        grid_ref[i] += rim_in_ref[i]
        give_layer(i // 2, i % 2)
    planes_ref[pl.ds(block, 1)] = grid_ref[pl.ds(2 * plane, 2)].reshape(1, 2, ROWS, CZ)
    with jax.named_scope("await"):
        for load in loads[first:]:
            load.wait()
        for b in range(COLUMN):
            pl.when(b != block)(functools.partial(drain, planes_ref.at[b], a_recv.at[b]))

    def spray(source, target, send_sem, recv_sem, half):
        def one(to, where):
            pltpu.make_async_remote_copy(
                src_ref=source.at[half, to], dst_ref=target.at[half, mine], send_sem=send_sem.at[half],
                recv_sem=recv_sem.at[half], device_id=where, device_id_type=MESH,
            ).start()

        with jax.named_scope("send"):
            everyone(one)
        target[half, pl.ds(mine, 1)] = source[half, pl.ds(mine, 1)]

    def arrive(target, recv_sem, half):
        with jax.named_scope("arrive"):
            drain(target.at[half, pl.ds(0, 127)], recv_sem.at[half])

    forward_kernel(
        planes_ref, t["to_kz"], t["to_ky"], send_ref,
        functools.partial(spray, send_ref, modes_ref, c_send, c_recv),
    )
    with jax.named_scope("turn"):
        fill_green(t["of_x"], t["of_z"], of_y_ref, green_ref)
        turn_tables(t["to_kz"], t["to_ky"], t["to_kx"], from_kz_ref, from_ky_ref, from_kx_ref)
    for half in range(2):
        arrive(modes_ref, c_recv, half)
        with jax.named_scope("middle"):
            middle_kernel(
                half, modes_ref, t["to_kx"], from_kx_ref, t["twist"], green_ref, send2_ref
            )
        spray(send2_ref, modes2_ref, d_send, d_recv, half)
    with jax.named_scope("gather_rows"):
        gather_rows(frac_ref, base_ref, rows_x_ref, both_x_ref, grads_y_ref, fold_z_ref)
    def give_back(x):
        for slot in range(EARLY, COLUMN) if x is None else range(1, EARLY):
            up, flip = ORDER_UP[slot]
            to = lax.rem(core + flip, 2) * 4 + lax.rem(height + up, 4)
            where = holder_of(to)
            source = blocks_ref.at[where["gz"] * 4 + where["gy"]]
            target = near_ref.at[ORDER_UP.index(((4 - up) % 4, flip))]
            if slot < EARLY:
                source, target = source.at[x], target.at[x]
            pltpu.make_async_remote_copy(
                src_ref=source, dst_ref=target, send_sem=b_send.at[slot],
                recv_sem=b_recv.at[ORDER_UP.index(((4 - up) % 4, flip))], device_id=where, device_id_type=MESH,
            ).start()

    backward_kernel(
        modes2_ref, from_ky_ref, from_kz_ref, blocks_ref, functools.partial(arrive, modes2_ref, d_recv),
        give_back,
    )
    near_ref[0] = blocks_ref[block]
    slot_cells = []
    for up, flip in ORDER_UP:
        x = 2 * (lax.rem(core + flip, 2) * 4 + lax.rem(height + up, 4))
        slot_cells += [x, x + 1]

    def slot_of(low_plane):
        up = lax.rem(low_plane - height + 4, 4)
        return jnp.where(up < 2, 2 * up, 10 - 2 * up) + core

    rims_back = []
    for low_plane, layers in ((0, 2), (1, 1)):
        slot = slot_of(low_plane)
        rims_back.append((slot, pltpu.make_async_remote_copy(
            src_ref=near_ref.at[slot, pl.ds(0, layers)], dst_ref=far_ref.at[pl.ds(2 * low_plane, layers)],
            send_sem=e_send.at[low_plane], recv_sem=e_recv.at[low_plane],
            device_id=before, device_id_type=MESH,
        )))
    tools = (both_x_ref, rows_y_ref, grads_y_ref, fold_z_ref)

    def keep(c, at, *forces):
        for d, force in enumerate(forces):
            part_ref[d, :, at] = force

    def add(c, at, *forces):
        for d, force in enumerate(forces):
            part_ref[d, :, at] += force

    def finish(c, at, *forces):
        slot = lax.broadcasted_iota(jnp.int32, (1, WIDTH), 1) + c * WIDTH
        charge = jnp.where(slot < counts_ref[0, 0, 0], charges_ref[:, at], 0.0)
        total = [
            jnp.sum(part_ref[d, :, at] + force, axis=0, keepdims=True) for d, force in enumerate(forces)
        ]
        out_ref[:, at] = -charge * jnp.concatenate(total, axis=0)

    def gather_slots(first, last, more, done):
        layers = [near_ref[slot, i] for slot in range(first, last) for i in range(2)]
        layers += [far_ref[i] for i in range(more)]
        stage(pot_ref, layers)
        cells = slot_cells[2 * first : 2 * last] + [CX + i for i in range(more)]
        gather_part(cells, pot_ref, *tools, done)

    direct = []
    for low_plane, layers in ((0, 2), (1, 1)):
        for flip in range(2):
            far_z, far_y = low_plane % 2, 2 + flip
            direct.append((low_plane, pltpu.make_async_remote_copy(
                src_ref=blocks_ref.at[far_z * 4 + far_y, pl.ds(0, layers)],
                dst_ref=far_ref.at[pl.ds(2 * low_plane, layers)], send_sem=direct_sem.at[flip],
                recv_sem=e_recv.at[low_plane], device_id={**before, "gz": far_z, "gy": far_y},
                device_id_type=MESH,
            )))

    def give_far():
        for low_plane, copy in direct:
            pl.when(plane == low_plane)(copy.start)
        give_back(None)

    with jax.named_scope("bwait1"):
        drain(near_ref.at[1], b_recv.at[1])
        for slot, copy in rims_back:
            pl.when(slot < 2)(copy.start)
    with jax.named_scope("gather1"):
        gather_slots(0, 2, 0, keep)
        give_far()
    with jax.named_scope("bwait2"):
        for slot in range(2, EARLY):
            drain(near_ref.at[slot], b_recv.at[slot])
        for slot, copy in rims_back:
            pl.when((slot >= 2) & (slot < EARLY))(copy.start)
    with jax.named_scope("gather2"):
        gather_slots(2, EARLY, 0, add)
    with jax.named_scope("bwait3"):
        for slot in range(EARLY, COLUMN):
            drain(near_ref.at[slot], b_recv.at[slot])
    with jax.named_scope("ewait"):
        for _, copy in rims_back:
            copy.wait_recv()
    with jax.named_scope("gather3"):
        gather_slots(EARLY, COLUMN, HALO, finish)
    with jax.named_scope("sendwait"):
        for rim in rims:
            rim.wait_send()
        for o in range(COLUMN):
            @pl.when(o != plane)
            def _():
                drain(grid_ref.at[pl.ds(2 * o, 2)], a_send.at[o])

        for half in range(2):
            drain(send_ref.at[half, pl.ds(0, 127)], c_send.at[half])
            drain(send2_ref.at[half, pl.ds(0, 127)], d_send.at[half])
        for slot in range(1, COLUMN):
            drain(blocks_ref.at[slot], b_send.at[slot])

    for slot, copy in rims_back:
        pl.when(slot < EARLY)(copy.wait_send)
    for low_plane, copy in direct:
        pl.when(plane == low_plane)(copy.wait_send)


def per_device(charges, fractions, base_cells, counts):
    t = {name: jnp.asarray(value) for name, value in tables().items()}
    arrays = [charges.reshape(1, -1), fractions, base_cells, counts, t["of_y"]]
    arrays += [t[name] for name in NAMES]
    small = len(INPUTS) + len(SMALL)
    atoms = fractions.shape[1]
    dma = pltpu.SemaphoreType.DMA
    scratch = [
        (pltpu.SMEM if len(INPUTS) <= i < small else pltpu.VMEM)(a.shape, a.dtype)
        for i, a in enumerate(arrays)
    ]
    scratch += [
        pltpu.VMEM((24, atoms), F32),
        pltpu.VMEM((ROWS, atoms), F32),
        pltpu.VMEM((2 * CZ, atoms), BF16),
        pltpu.VMEM((160, CZ), F32),
        pltpu.VMEM((2 * ROWS, atoms), BF16),
        pltpu.VMEM((4 * ROWS, atoms), BF16),
        pltpu.VMEM((4 * ROWS, atoms), BF16),
        pltpu.VMEM((20, ROWS, CZ), F32),
        pltpu.VMEM((HALO, ROWS, CZ), F32),
        pltpu.VMEM((COLUMN, 2, ROWS, CZ), F32),
        pltpu.VMEM((2, 128, 4, 128), F32),
        pltpu.VMEM((2, 128, 4, 128), F32),
        pltpu.VMEM((2, 128, 4, 128), F32),
        pltpu.VMEM((2, 128, 4, 128), F32),
        pltpu.VMEM((COLUMN, 2, ROWS, CZ), F32),
        pltpu.VMEM((COLUMN, 2, ROWS, CZ), F32),
        pltpu.VMEM((HALO, ROWS, CZ), F32),
        pltpu.VMEM((3, 8, atoms), F32),
        pltpu.VMEM((2 * EARLY * ROWS, 512), BF16),
        pltpu.VMEM((atoms // WIDTH, 48, WIDTH), F32),
        pltpu.VMEM((ROWS, atoms), F32),
        pltpu.VMEM((atoms // WIDTH, 512, 2 * WIDTH), BF16),
        pltpu.VMEM((4, 128, 128), F32),
        pltpu.VMEM(t["to_kz"].shape, BF16),
        pltpu.VMEM(t["to_ky"].shape, BF16),
        pltpu.VMEM(t["to_kx"].shape, BF16),
        dma((len(arrays),)), dma((HALO,)), dma((HALO,)), dma((COLUMN,)), dma((COLUMN,)), dma((2,)), dma((2,)), dma((2,)), dma((2,)),
        dma((COLUMN,)), dma((COLUMN,)), dma((2,)), dma((2,)), dma((2,)),
    ]
    return pl.pallas_call(
        fused_kernel,
        out_shape=jax.ShapeDtypeStruct(fractions.shape, F32),
        in_specs=[pl.BlockSpec(memory_space=pltpu.HBM)] * len(arrays),
        out_specs=pl.BlockSpec(memory_space=pltpu.VMEM),
        scratch_shapes=scratch,
        compiler_params=pltpu.CompilerParams(
            collective_id=0, has_side_effects=True, vmem_limit_bytes=62 << 20
        ),
    )(*arrays)


def solution(mesh):
    split = ("gz", "gy", "gx")
    return jax.shard_map(
        per_device,
        mesh=mesh,
        in_specs=(P(split), P(None, split), P(None, split), P("gz", "gy", "gx")),
        out_specs=P(None, split),
        check_vma=False,
    )
```
